512 devices in a mesh: heads: 16 (over y, core), batch: 32 (over z, x).
Axes of the slice: x: 4, y: 8, z: 8, core: 2. Of those that a mesh axis runs over, the one named last changes fastest.
Arguments:
- queries: bfloat16 [256, 4096], P('batch', 'heads'), may hold values from -6 to 6
- keys_new: bfloat16 [256, 4096], P('batch', 'heads'), may hold values from -6 to 6
- values_new: bfloat16 [256, 4096], P('batch', 'heads'), may hold values from -6 to 6
- out_gate: bfloat16 [256, 4096], P('batch', 'heads'), may hold values from -6 to 6
- decay_logit: float32 [256, 32], P('batch', 'heads'), may hold values from -6 to 6
- beta_logit: float32 [256, 32], P('batch', 'heads'), may hold values from -6 to 6
- decay_rate: float32 [32], P('heads'), may hold values from 0.05 to 2
- state: float32 [256, 32, 128, 128], P('batch', 'heads'), may hold values from -0.6 to 0.6
- norm_gain: float32 [128], replicated, may hold values from 0.1 to 1.9
- out_proj: bfloat16 [4096, 4096], P('heads'), may hold values from -0.09375 to 0.09375
- residual: bfloat16 [256, 4096], P('batch'), may hold values from -40 to 40, as said below
- final_gain: float32 [4096], replicated, may hold values from 0.1 to 1.9
- value_weight: float32 [4096], replicated, may hold values from -0.09375 to 0.09375
- lm_head: bfloat16 [4096, 65536], P(None, ('heads', 'batch')), may hold values from -15 to 15
- sampled: int32 [256], replicated, may hold values from 0 to 65535
Outputs:
- logprob: float32 [256], P('batch')
- value: float32 [256], P('batch')
The draws below stay inside these ranges and needn't reach their ends.
Inputs may be any that keep to these rules, and one draw needn't show every extreme that they name: The residual stream's entries have scales that differ by row and by column (up to tenfold each), so neither rows nor columns share one magnitude.
All inputs are finite; a program needn't handle non-finite values.
Results may differ from the reference program's by a relative error of at most 0.0013.
Values may be sent and summed in bfloat16 or wider, within the bound.
No kernel may reach another device: no remote copies, remote signals or barrier semaphores. Data moves between devices by JAX's collectives and lax.ppermute only.
A program may use at most 64 MiB of HBM per device.

```python
import math
import jax
import jax.numpy as jnp
from jax import lax

D = 4096
H = 32
DK = 128
DV = 128
BATCH = 256
VOCAB = 65536


def draw_residual(key, part):
    first, second, third = jax.random.split(jax.random.fold_in(key, 11), 3)
    base = jnp.clip(jax.random.normal(first, (BATCH, D), jnp.float32), -4.0, 4.0)
    row_scale = jnp.exp(jax.random.uniform(second, (BATCH, 1), jnp.float32) * jnp.log(10.0))
    col_scale = jnp.exp(jax.random.uniform(third, (1, D), jnp.float32) * jnp.log(10.0))
    return (base * row_scale * col_scale * 0.1).astype(jnp.bfloat16)


def draw_lm_head(key, part):
    first = jax.random.fold_in(jax.random.fold_in(key, 23), 0)
    base = jnp.clip(jax.random.normal(first, (D, VOCAB), jnp.float32), -4.0, 4.0) * (3.0 / jnp.sqrt(D * 1.0))
    return base.astype(jnp.bfloat16)


def place_ends(entries, rng, smallest, largest):
    place = [jax.random.randint(jax.random.fold_in(rng, axis), (), 0, length) for axis, length in enumerate(entries.shape)]
    widest = entries.shape.index(max(entries.shape))
    neighbour = place[:widest] + [(place[widest] + 1) % entries.shape[widest]] + place[widest + 1:]
    return entries.at[tuple(place)].set(smallest).at[tuple(neighbour)].set(largest)


def shard_levels(own_key, extent, shards, low, top_value):
    factor_of, own = 1.0, jax.random.fold_in(own_key, 6)
    for dim, parts in shards:
        draws = jnp.exp(jax.random.uniform(jax.random.fold_in(own, dim), (parts,), jnp.float32, low / len(shards), top_value / len(shards)))
        factor_of = factor_of * jnp.repeat(draws, extent[dim] // parts).reshape([-1 if axis == dim else 1 for axis in range(len(extent))])
    return factor_of


def normal_values(key, dims, spread, bound, shards=(), kind=jnp.bfloat16):
    factor_of = shard_levels(key, dims, shards, -0.22, 0.18) if shards else 1.0
    entries = jax.random.normal(key, dims, jnp.float32) * spread * factor_of
    return jnp.minimum(jnp.maximum(entries, -bound), bound).astype(kind)


def setup_inputs(seed: int = 0) -> dict:
    key_list = jax.random.split(jax.random.key(seed), 16)
    return {
        "queries": normal_values(key_list[0], (BATCH, H * DK), 1.0, 6.0, ((0, 32), (1, 16))),
        "keys_new": normal_values(key_list[1], (BATCH, H * DK), 1.0, 6.0, ((0, 32), (1, 16))),
        "values_new": normal_values(key_list[2], (BATCH, H * DV), 1.0, 6.0, ((0, 32), (1, 16))),
        "out_gate": normal_values(key_list[3], (BATCH, H * DV), 1.0, 6.0, ((0, 32), (1, 16))),
        "decay_logit": normal_values(key_list[4], (BATCH, H), 1.5, 6.0, ((0, 32), (1, 16)), jnp.float32),
        "beta_logit": normal_values(key_list[5], (BATCH, H), 1.5, 6.0, ((0, 32), (1, 16)), jnp.float32),
        "decay_rate": jnp.clip(jnp.exp(math.log(2.0) - 3.6888794 * jax.random.uniform(key_list[6], (H,), jnp.float32) ** shard_levels(key_list[6], (H,), ((0, 16),), -0.2, 0.2)), 0.05, 2.0),
        "state": normal_values(key_list[7], (BATCH, H, DK, DV), 0.1, 0.6, ((0, 32), (1, 16)), jnp.float32),
        "norm_gain": jnp.clip(1.0 + 0.18 * jax.random.normal(key_list[8], (DV,), jnp.float32), 0.1, 1.9),
        "out_proj": normal_values(key_list[9], (H * DV, D), (H * DV) ** -0.5, 0.09375, ((0, 16),)),
        "residual": draw_residual(jax.random.fold_in(key_list[15], 71), 0),
        "final_gain": jnp.clip(1.0 + 0.18 * jax.random.normal(key_list[11], (D,), jnp.float32), 0.1, 1.9),
        "value_weight": normal_values(key_list[12], (D,), D ** -0.5, 0.09375, (), jnp.float32),
        "lm_head": draw_lm_head(jax.random.fold_in(key_list[15], 71), 0),
        "sampled": place_ends(jax.random.randint(key_list[14], (BATCH,), 0, VOCAB), jax.random.fold_in(key_list[14], 1), 0, VOCAB - 1).astype(jnp.int32),
    }


epsilon = 1e-06

def head_outputs(queries, keys_new, values_new, out_gate, decay_logit, beta_logit, decay_rate, state, norm_gain):
    rows_here, heads_here = decay_logit.shape
    query_f = queries.astype(jnp.float32).reshape(rows_here, heads_here, -1)
    key_f = keys_new.astype(jnp.float32).reshape(rows_here, heads_here, -1)
    value_f = values_new.astype(jnp.float32).reshape(rows_here, heads_here, -1)
    gate_f = out_gate.astype(jnp.float32).reshape(rows_here, heads_here, -1)
    key_size = query_f.shape[2]
    query_n = query_f / jnp.sqrt(lax.optimization_barrier(jnp.sum(query_f * query_f, axis=2, keepdims=True)) + epsilon)
    query_n = query_n * key_size ** (-0.5)
    key_n = key_f / jnp.sqrt(lax.optimization_barrier(jnp.sum(key_f * key_f, axis=2, keepdims=True)) + epsilon)
    decay = jnp.exp(-decay_rate[None, :] * jax.nn.softplus(decay_logit))
    strength = jax.nn.sigmoid(beta_logit)
    state_query = jnp.einsum('bhk,bhkv->bhv', query_n, state, precision=lax.Precision.HIGHEST)
    state_key = jnp.einsum('bhk,bhkv->bhv', key_n, state, precision=lax.Precision.HIGHEST)
    intersection = lax.optimization_barrier(jnp.sum(query_n * key_n, axis=2, keepdims=True))
    written = value_f - decay[..., None] * state_key
    output = decay[..., None] * state_query + strength[..., None] * intersection * written
    normed = output / jnp.sqrt(lax.optimization_barrier(jnp.mean(output * output, axis=2, keepdims=True)) + epsilon)
    result = normed * norm_gain * jax.nn.silu(gate_f)
    return result.reshape(rows_here, -1).astype(jnp.bfloat16)

def reference(queries, keys_new, values_new, out_gate, decay_logit, beta_logit, decay_rate, state, norm_gain, out_proj, residual, final_gain, value_weight, lm_head, sampled):
    headout = head_outputs(queries, keys_new, values_new, out_gate, decay_logit, beta_logit, decay_rate, state, norm_gain)
    attn = jnp.dot(headout, out_proj, preferred_element_type=jnp.float32)
    hsum = residual.astype(jnp.float32) + attn
    rstd = 1.0 / jnp.sqrt(lax.optimization_barrier(jnp.mean(hsum * hsum, axis=1)) + epsilon)
    value = rstd * lax.optimization_barrier(jnp.sum(hsum * final_gain * value_weight, axis=1))
    normed = (hsum * rstd[:, None] * final_gain).astype(jnp.bfloat16)
    logits = jnp.dot(normed, lm_head, preferred_element_type=jnp.float32)
    top = lax.optimization_barrier(jnp.max(logits, axis=1))
    total = lax.optimization_barrier(jnp.sum(jnp.exp(logits - top[:, None]), axis=1))
    chosen = jnp.take_along_axis(logits, sampled.astype(jnp.int32)[:, None], axis=1)[:, 0]
    logprob = chosen - (top + jnp.log(total))
    return (logprob, value)
```

```python
import jax
import jax.numpy as jnp
from jax import lax
from jax.sharding import Mesh
from jax.sharding import PartitionSpec as P

HEADS = ("heads_0", "heads_1")
BATCH = ("batch_0", "batch_1")
HEADS_BATCH = ("heads_0", "heads_1", "batch_0", "batch_1")


epsilon = 1e-06


def exchange(parts, axis):
    return lax.all_to_all(parts, axis, split_axis=0, concat_axis=0, tiled=True)


def copy_for_each(array, axis):
    size = lax.axis_size(axis)
    return exchange(jnp.broadcast_to(array[None], (size, *array.shape)), axis)


def head_outputs(
    queries, keys_new, values_new, out_gate, decay_logit, beta_logit, decay_rate, state, norm_gain
):
    rows_here, heads_here = decay_logit.shape
    query_f = queries.astype(jnp.float32).reshape(rows_here, heads_here, -1)
    key_f = keys_new.astype(jnp.float32).reshape(rows_here, heads_here, -1)
    value_f = values_new.astype(jnp.float32).reshape(rows_here, heads_here, -1)
    gate_f = out_gate.astype(jnp.float32).reshape(rows_here, heads_here, -1)
    key_size = query_f.shape[2]
    query_n = query_f / jnp.sqrt(jnp.sum(query_f * query_f, axis=2, keepdims=True) + epsilon)
    query_n = query_n * key_size ** (-0.5)
    key_n = key_f / jnp.sqrt(jnp.sum(key_f * key_f, axis=2, keepdims=True) + epsilon)
    decay = jnp.exp(-decay_rate[None, :] * jax.nn.softplus(decay_logit))
    strength = jax.nn.sigmoid(beta_logit)
    state_query = jnp.einsum("bhk,bhkv->bhv", query_n, state, precision=lax.Precision.HIGHEST)
    state_key = jnp.einsum("bhk,bhkv->bhv", key_n, state, precision=lax.Precision.HIGHEST)
    intersection = jnp.sum(query_n * key_n, axis=2, keepdims=True)
    written = value_f - decay[..., None] * state_key
    output = decay[..., None] * state_query + strength[..., None] * intersection * written
    normed = output / jnp.sqrt(jnp.mean(output * output, axis=2, keepdims=True) + epsilon)
    result = normed * norm_gain * jax.nn.silu(gate_f)
    return result.reshape(rows_here, -1).astype(jnp.bfloat16)


def merged(top, total, chosen, axis):
    highest = jnp.max(top, axis=axis, keepdims=True)
    scaled = jnp.sum(total * jnp.exp(top - highest), axis=axis)
    return jnp.squeeze(highest, axis), scaled, jnp.sum(chosen, axis=axis)


def per_device(
    queries,
    keys_new,
    values_new,
    out_gate,
    decay_logit,
    beta_logit,
    decay_rate,
    state,
    norm_gain,
    out_proj,
    residual,
    final_gain,
    value_weight,
    lm_head,
    sampled,
):
    chips, cores = lax.axis_size("heads_0"), lax.axis_size("heads_1")
    groups = lax.axis_size(BATCH)
    chip, core = lax.axis_index("heads_0"), lax.axis_index("heads_1")
    rows_own, width = residual.shape
    rows_core = rows_own // cores
    copies = chips // rows_core
    lanes = 128
    lines = width // lanes
    half = width // copies

    other_head = lax.ppermute(lm_head, "heads_1", [(0, 1), (1, 0)])

    headout = head_outputs(
        queries,
        keys_new,
        values_new,
        out_gate,
        decay_logit,
        beta_logit,
        decay_rate,
        state,
        norm_gain,
    )
    for_owner = headout.reshape(cores, rows_core, 1, -1)
    for_owner = jnp.broadcast_to(for_owner, (cores, rows_core, copies, headout.shape[1]))
    for_owner = for_owner.transpose(1, 2, 0, 3).reshape(chips * cores, -1)
    partial_out = jnp.dot(for_owner, out_proj, preferred_element_type=jnp.float32)
    arrived = exchange(partial_out.reshape(chips * cores, lines, lanes), HEADS)
    row = rows_core * core + chip // copies
    own = lax.dynamic_slice_in_dim(residual, row, 1, 0).astype(jnp.float32).reshape(lines, lanes)
    gain = final_gain.reshape(lines, lanes)
    weight = value_weight.reshape(lines, lanes)
    hsum = own + arrived.sum(axis=0)
    rstd = 1.0 / jnp.sqrt(jnp.sum(hsum * hsum) / width + epsilon)
    value = rstd * jnp.sum(hsum * gain * weight)
    normed = (hsum * rstd * gain).astype(jnp.bfloat16)
    piece = lax.dynamic_slice_in_dim(normed, (chip % copies) * (lines // copies), lines // copies, 0)
    all_groups = copy_for_each(piece, BATCH).reshape(groups, half)
    all_rows = copy_for_each(all_groups, "heads_0").reshape(rows_core, copies, groups, half)

    heads_both = (lm_head, other_head)
    vocab_own = lm_head.shape[1]
    flat = lax.axis_index(HEADS_BATCH)
    firsts = (flat * vocab_own, (flat + (1 - 2 * core) * groups) * vocab_own)
    ids = lax.dynamic_index_in_dim(
        sampled.reshape(groups, cores, rows_core).transpose(1, 2, 0), core, 0, keepdims=False
    ).reshape(-1)
    operand = all_rows.transpose(0, 2, 1, 3).reshape(rows_core * groups, width)
    found = []
    for matrix, first in zip(heads_both, firsts):
        logits = jnp.dot(operand, matrix, preferred_element_type=jnp.float32)
        columns = lax.broadcasted_iota(jnp.int32, logits.shape, 1) + first
        found.append(
            (
                logits,
                jnp.max(logits, axis=1),
                jnp.sum(jnp.where(columns == ids[:, None], logits, 0.0), axis=1),
            )
        )
    top = jnp.maximum(found[0][1], found[1][1])
    total = sum(jnp.sum(jnp.exp(f[0] - top[:, None]), axis=1) for f in found)
    chosen = found[0][2] + found[1][2]
    stats = jnp.stack([top, total, chosen]).reshape(3, rows_core, groups).transpose(2, 0, 1)
    stats = exchange(stats.reshape(groups, 1, 3 * rows_core), BATCH).reshape(groups, 3, rows_core)
    stats = merged(stats[:, 0], stats[:, 1], stats[:, 2], 0)
    packed = jnp.concatenate([*stats, value[None]])
    packed = copy_for_each(packed[None], HEADS).reshape(chips, cores, -1)
    found = packed[..., : 3 * rows_core].reshape(chips, cores, 3, rows_core)
    top, total, chosen = merged(found[:, :, 0], found[:, :, 1], found[:, :, 2], 0)
    logprob = (chosen - (top + jnp.log(total))).reshape(-1)
    values = packed[::copies, :, 3 * rows_core].T.reshape(-1)
    return (logprob, values)


def solution(mesh):
    torus = Mesh(mesh.devices.reshape(8, 2, 8, 4), ("heads_0", "heads_1", "batch_0", "batch_1"))
    return jax.shard_map(
        per_device,
        mesh=torus,
        in_specs=(
            P(BATCH, HEADS),
            P(BATCH, HEADS),
            P(BATCH, HEADS),
            P(BATCH, HEADS),
            P(BATCH, HEADS),
            P(BATCH, HEADS),
            P(HEADS),
            P(BATCH, HEADS, None, None),
            P(),
            P(HEADS, None),
            P(BATCH, None),
            P(),
            P(),
            P(None, HEADS_BATCH),
            P(),
        ),
        out_specs=(P(BATCH), P(BATCH)),
        check_vma=False,
    )
```

```python
import jax
import jax.numpy as jnp
from jax import lax
from jax.sharding import Mesh
from jax.sharding import PartitionSpec as P

HEADS = ("heads_0", "heads_1")
BATCH = ("z_pair", "z_side", "x")
GROUP = ("z_pair", "x")
HEADS_BATCH = ("heads_0", "heads_1", "z_pair", "z_side", "x")
SWAP = [(0, 1), (1, 0)]


epsilon = 1e-06


def exchange(parts, axis):
    return lax.all_to_all(parts, axis, split_axis=0, concat_axis=0, tiled=True)


def copy_for_each(array, axis):
    size = lax.axis_size(axis)
    return exchange(jnp.broadcast_to(array[None], (size, *array.shape)), axis)


def head_outputs(
    queries, keys_new, values_new, out_gate, decay_logit, beta_logit, decay_rate, state, norm_gain
):
    rows_here, heads_here = decay_logit.shape
    query_f = queries.astype(jnp.float32).reshape(rows_here, heads_here, -1)
    key_f = keys_new.astype(jnp.float32).reshape(rows_here, heads_here, -1)
    value_f = values_new.astype(jnp.float32).reshape(rows_here, heads_here, -1)
    gate_f = out_gate.astype(jnp.float32).reshape(rows_here, heads_here, -1)
    key_size = query_f.shape[2]
    query_n = query_f / jnp.sqrt(jnp.sum(query_f * query_f, axis=2, keepdims=True) + epsilon)
    query_n = query_n * key_size ** (-0.5)
    key_n = key_f / jnp.sqrt(jnp.sum(key_f * key_f, axis=2, keepdims=True) + epsilon)
    decay = jnp.exp(-decay_rate[None, :] * jax.nn.softplus(decay_logit))
    strength = jax.nn.sigmoid(beta_logit)
    state_query = jnp.einsum("bhk,bhkv->bhv", query_n, state, precision=lax.Precision.HIGHEST)
    state_key = jnp.einsum("bhk,bhkv->bhv", key_n, state, precision=lax.Precision.HIGHEST)
    intersection = jnp.sum(query_n * key_n, axis=2, keepdims=True)
    written = value_f - decay[..., None] * state_key
    output = decay[..., None] * state_query + strength[..., None] * intersection * written
    normed = output / jnp.sqrt(jnp.mean(output * output, axis=2, keepdims=True) + epsilon)
    result = normed * norm_gain * jax.nn.silu(gate_f)
    return result.reshape(rows_here, -1).astype(jnp.bfloat16)


def merged(top, total, chosen, axis):
    highest = jnp.max(top, axis=axis, keepdims=True)
    scaled = jnp.sum(total * jnp.exp(top - highest), axis=axis)
    return jnp.squeeze(highest, axis), scaled, jnp.sum(chosen, axis=axis)


def per_device(
    queries,
    keys_new,
    values_new,
    out_gate,
    decay_logit,
    beta_logit,
    decay_rate,
    state,
    norm_gain,
    out_proj,
    residual,
    final_gain,
    value_weight,
    lm_head,
    sampled,
):
    chips, cores = lax.axis_size("heads_0"), lax.axis_size("heads_1")
    groups = lax.axis_size(GROUP)
    chip, core = lax.axis_index("heads_0"), lax.axis_index("heads_1")
    side = lax.axis_index("z_side")
    rows_own, width = residual.shape
    rows_core = rows_own // cores
    copies = chips // rows_core
    lanes = 128
    lines = width // lanes
    half = width // copies

    z_head = lax.ppermute(lm_head, "z_side", SWAP)
    core_head = lax.ppermute(lm_head, "heads_1", SWAP)
    both_head = lax.ppermute(z_head, "heads_1", SWAP)

    headout = head_outputs(
        queries,
        keys_new,
        values_new,
        out_gate,
        decay_logit,
        beta_logit,
        decay_rate,
        state,
        norm_gain,
    )
    for_owner = headout.reshape(cores, rows_core, 1, -1)
    for_owner = jnp.broadcast_to(for_owner, (cores, rows_core, copies, headout.shape[1]))
    for_owner = for_owner.transpose(1, 2, 0, 3).reshape(chips * cores, -1)
    partial_out = jnp.dot(for_owner, out_proj, preferred_element_type=jnp.float32)
    arrived = exchange(partial_out.reshape(chips * cores, lines, lanes), HEADS)
    row = rows_core * core + chip // copies
    own = lax.dynamic_slice_in_dim(residual, row, 1, 0).astype(jnp.float32).reshape(lines, lanes)
    gain = final_gain.reshape(lines, lanes)
    weight = value_weight.reshape(lines, lanes)
    hsum = own + arrived.sum(axis=0)
    rstd = 1.0 / jnp.sqrt(jnp.sum(hsum * hsum) / width + epsilon)
    value = rstd * jnp.sum(hsum * gain * weight)
    normed = (hsum * rstd * gain).astype(jnp.bfloat16)
    piece = lax.dynamic_slice_in_dim(normed, (chip % copies) * (lines // copies), lines // copies, 0)
    all_groups = copy_for_each(piece, GROUP).reshape(groups, half)
    all_rows = copy_for_each(all_groups, "heads_0").reshape(rows_core, copies, groups, half)

    vocab_own = lm_head.shape[1]
    flat = lax.axis_index(HEADS_BATCH)
    across = (1 - 2 * core) * lax.axis_size(BATCH)
    along = (1 - 2 * side) * lax.axis_size("x")
    matrices = (lm_head, core_head, z_head, both_head)
    firsts = [(flat + shift) * vocab_own for shift in (0, across, along, across + along)]
    ids = sampled.reshape(-1, lax.axis_size("z_side"), lax.axis_size("x"), cores, rows_core)
    ids = lax.dynamic_index_in_dim(ids, side, 1, keepdims=False)
    ids = lax.dynamic_index_in_dim(ids, core, 2, keepdims=False)
    ids = ids.reshape(groups, rows_core).T.reshape(-1)
    operand = all_rows.transpose(0, 2, 1, 3).reshape(rows_core * groups, width)
    found = []
    for matrix, first in zip(matrices, firsts):
        logits = jnp.dot(operand, matrix, preferred_element_type=jnp.float32)
        columns = lax.broadcasted_iota(jnp.int32, logits.shape, 1) + first
        found.append(
            (
                logits,
                jnp.max(logits, axis=1),
                jnp.sum(jnp.where(columns == ids[:, None], logits, 0.0), axis=1),
            )
        )
    top = jnp.max(jnp.stack([f[1] for f in found]), axis=0)
    total = sum(jnp.sum(jnp.exp(f[0] - top[:, None]), axis=1) for f in found)
    chosen = sum(f[2] for f in found)
    stats = jnp.stack([top, total, chosen]).reshape(3, rows_core, groups).transpose(2, 0, 1)
    stats = exchange(stats.reshape(groups, 1, 3 * rows_core), GROUP).reshape(groups, 3, rows_core)
    stats = merged(stats[:, 0], stats[:, 1], stats[:, 2], 0)
    packed = jnp.concatenate([*stats, value[None]])
    packed = copy_for_each(packed[None], HEADS).reshape(chips, cores, -1)
    found = packed[..., : 3 * rows_core].reshape(chips, cores, 3, rows_core)
    top, total, chosen = merged(found[:, :, 0], found[:, :, 1], found[:, :, 2], 0)
    logprob = (chosen - (top + jnp.log(total))).reshape(-1)
    values = packed[::copies, :, 3 * rows_core].T.reshape(-1)
    return (logprob, values)


def solution(mesh):
    torus = Mesh(
        mesh.devices.reshape(8, 2, 4, 2, 4), ("heads_0", "heads_1", "z_pair", "z_side", "x")
    )
    return jax.shard_map(
        per_device,
        mesh=torus,
        in_specs=(
            P(BATCH, HEADS),
            P(BATCH, HEADS),
            P(BATCH, HEADS),
            P(BATCH, HEADS),
            P(BATCH, HEADS),
            P(BATCH, HEADS),
            P(HEADS),
            P(BATCH, HEADS, None, None),
            P(),
            P(HEADS, None),
            P(BATCH, None),
            P(),
            P(),
            P(None, HEADS_BATCH),
            P(),
        ),
        out_specs=(P(BATCH), P(BATCH)),
        check_vma=False,
    )
```

```python
import jax
import jax.numpy as jnp
from jax import lax
from jax.experimental import pallas as pl
from jax.experimental.pallas import tpu as pltpu
from jax.sharding import Mesh
from jax.sharding import PartitionSpec as P

HEADS = ("heads_0", "heads_1")
BATCH = ("z_pair", "z_side", "x")
GROUP = ("z_pair", "x")
HEADS_BATCH = ("heads_0", "heads_1", "z_pair", "z_side", "x")
SWAP = [(0, 1), (1, 0)]


epsilon = 1e-06


def exchange(parts, axis):
    return lax.all_to_all(parts, axis, split_axis=0, concat_axis=0, tiled=True)


def copy_for_each(array, axis):
    size = lax.axis_size(axis)
    return exchange(jnp.broadcast_to(array[None], (size, *array.shape)), axis)


def any_spec():
    return pl.BlockSpec(memory_space=pl.ANY)


def vmem_spec():
    return pl.BlockSpec(memory_space=pltpu.VMEM)


def smem_spec():
    return pl.BlockSpec(memory_space=pltpu.SMEM)


def as_column(line):
    size = line.shape[1]
    shape = (size, size)
    here = lax.broadcasted_iota(jnp.int32, shape, 0) == lax.broadcasted_iota(jnp.int32, shape, 1)
    return jnp.sum(jnp.where(here, jnp.broadcast_to(line, shape), 0.0), axis=1, keepdims=True)


def heads_kernel(
    first_ref,
    rate_ref,
    *refs,
):
    inputs, out_ref, local, sems = refs[:10], refs[10], refs[11:21], refs[21]
    q_ref, k_ref, v_ref, g_ref, dl_ref, bl_ref, gain_ref, res_ref, state_ref, proj_ref = local
    copies = [pltpu.make_async_copy(inputs[n], local[n], sems.at[n]) for n in range(8)]
    heads = state_ref.shape[1]
    for h in range(heads):
        copies.append(
            pltpu.make_async_copy(inputs[8].at[:, h], state_ref.at[:, h], sems.at[8 + h])
        )
    blocks = 4
    wide = proj_ref.shape[1] // blocks
    for n in range(blocks):
        part = pl.ds(n * wide, wide)
        copies.append(
            pltpu.make_async_copy(
                inputs[9].at[:, part], proj_ref.at[:, part], sems.at[8 + heads + n]
            )
        )
    for copy in copies:
        copy.start()
    for copy in copies[:8]:
        copy.wait()
    rows = q_ref.shape[0]
    size = state_ref.shape[2]
    gain = gain_ref[...]
    queries, keys = [], []
    for h in range(heads):
        lanes = slice(h * size, (h + 1) * size)
        query = q_ref[:, lanes].astype(jnp.float32)
        key = k_ref[:, lanes].astype(jnp.float32)
        query = query / jnp.sqrt(jnp.sum(query * query, axis=1, keepdims=True) + epsilon)
        queries.append(query * size ** (-0.5))
        keys.append(key / jnp.sqrt(jnp.sum(key * key, axis=1, keepdims=True) + epsilon))
    turned = jnp.concatenate(queries + keys, axis=0).T
    parts = []
    for h in range(heads):
        lanes = slice(h * size, (h + 1) * size)
        logit = dl_ref[h : h + 1, :]
        soft = jnp.maximum(logit, 0.0) + jnp.log1p(jnp.exp(-jnp.abs(logit)))
        decay = as_column(jnp.exp(-rate_ref[h] * soft))
        strength = as_column(1.0 / (1.0 + jnp.exp(-bl_ref[h : h + 1, :])))
        inter = jnp.sum(queries[h] * keys[h], axis=1, keepdims=True)
        value = v_ref[:, lanes].astype(jnp.float32)
        gate = g_ref[:, lanes].astype(jnp.float32)
        copies[8 + h].wait()
        by_query, by_key = [], []
        for b in range(rows):
            block = state_ref[b, h]
            at = h * rows + b
            by_query.append(jnp.sum(turned[:, at : at + 1] * block, axis=0, keepdims=True))
            at += heads * rows
            by_key.append(jnp.sum(turned[:, at : at + 1] * block, axis=0, keepdims=True))
        state_query = jnp.concatenate(by_query, axis=0)
        state_key = jnp.concatenate(by_key, axis=0)
        written = value - decay * state_key
        output = decay * state_query + strength * inter * written
        mean = jnp.mean(output * output, axis=1, keepdims=True)
        normed = output / jnp.sqrt(mean + epsilon)
        parts.append(normed * gain * (gate / (1.0 + jnp.exp(-gate))))
    headout = jnp.concatenate(parts, axis=1).astype(jnp.bfloat16)
    first = first_ref[0]
    lines = wide // 128
    cores, halves = 2, out_ref.shape[0] // rows
    for n in range(blocks):
        copies[8 + heads + n].wait()
        part = slice(n * wide, (n + 1) * wide)
        total = jnp.dot(headout, proj_ref[:, part], preferred_element_type=jnp.float32)
        total = total + res_ref[:, part].astype(jnp.float32) * first
        total = total.reshape(rows, lines, 128)
        for row in range(rows):
            for half in range(halves):
                core, r = row // (rows // cores), row % (rows // cores)
                place = (r * halves + half) * cores + core
                out_ref[place, n * lines : (n + 1) * lines, :] = total[row]


def head_partials(
    queries,
    keys_new,
    values_new,
    out_gate,
    decay_logit,
    beta_logit,
    decay_rate,
    state,
    norm_gain,
    out_proj,
    residual,
    first,
    places,
):
    arrays = (
        queries,
        keys_new,
        values_new,
        out_gate,
        decay_logit.T,
        beta_logit.T,
        norm_gain.reshape(1, -1),
        residual,
        state,
        out_proj,
    )
    width = out_proj.shape[1]
    return pl.pallas_call(
        heads_kernel,
        out_shape=jax.ShapeDtypeStruct((places, width // 128, 128), jnp.float32),
        in_specs=[smem_spec(), smem_spec()] + [any_spec() for _ in arrays],
        out_specs=vmem_spec(),
        scratch_shapes=[pltpu.VMEM(a.shape, a.dtype) for a in arrays]
        + [pltpu.SemaphoreType.DMA((8 + state.shape[1] + 4,))],
        cost_estimate=pl.CostEstimate(flops=40000000, bytes_accessed=3500000, transcendentals=0),
        name="heads",
    )(first, decay_rate, *arrays)


def norm_kernel(half_ref, arrived_ref, gain_ref, weight_ref, piece_ref, value_ref, scratch):
    width = gain_ref.size
    hsum = arrived_ref[0]
    for n in range(1, arrived_ref.shape[0]):
        hsum = hsum + arrived_ref[n]
    gain = gain_ref[...]
    squares = jnp.sum(hsum * hsum, axis=(0, 1), keepdims=True)
    terms = jnp.sum(hsum * gain * weight_ref[...], axis=(0, 1), keepdims=True)
    rstd = 1.0 / jnp.sqrt(squares / width + epsilon)
    scratch[...] = hsum * rstd * gain
    lines = piece_ref.shape[1]
    start = pl.multiple_of(half_ref[0] * lines, lines)
    piece = scratch[pl.ds(start, lines), :].astype(jnp.bfloat16)
    for n in range(piece_ref.shape[0]):
        piece_ref[n] = piece
    value_ref[...] = jnp.broadcast_to(rstd * terms, value_ref.shape)


def norm_pieces(arrived, gain, weight, half, copies, lines):
    return pl.pallas_call(
        norm_kernel,
        out_shape=(
            jax.ShapeDtypeStruct((copies, lines, 128), jnp.bfloat16),
            jax.ShapeDtypeStruct((1, 128), jnp.float32),
        ),
        in_specs=[smem_spec(), vmem_spec(), vmem_spec(), vmem_spec()],
        out_specs=(vmem_spec(), vmem_spec()),
        scratch_shapes=[pltpu.VMEM(gain.shape, jnp.float32)],
        cost_estimate=pl.CostEstimate(flops=4000000, bytes_accessed=400000, transcendentals=0),
        name="norm",
    )(half, arrived, gain, weight)


def logits_kernel(firsts_ref, rows_ref, ids_ref, *refs):
    count = 4
    matrices, out_ref, local, sems = refs[:count], refs[count], refs[count + 1], refs[count + 2]
    pieces, groups, deep = rows_ref.shape
    halves = local.shape[1] // deep
    copies = []
    for k in range(halves):
        part = pl.ds(k * deep, deep)
        for n in range(count):
            at = k * count + n
            copies.append(
                pltpu.make_async_copy(
                    matrices[n].at[part], local.at[n, part], sems.at[at]
                )
            )
    for copy in copies:
        copy.start()
    sums = [None] * count
    for k in range(halves):
        part = slice(k * deep, (k + 1) * deep)
        lhs = jnp.concatenate([rows_ref[p] for p in range(k, pieces, halves)], axis=0)
        for n in range(count):
            copies[k * count + n].wait()
            term = jnp.dot(lhs, local[n, part], preferred_element_type=jnp.float32)
            sums[n] = term if k == 0 else sums[n] + term
    top = sums[0]
    for n in range(1, count):
        top = jnp.maximum(top, sums[n])
    top = jnp.max(top, axis=1, keepdims=True)
    ids = ids_ref[...]
    total = jnp.zeros(sums[0].shape, jnp.float32)
    chosen = jnp.zeros(sums[0].shape, jnp.float32)
    for n in range(count):
        total = total + jnp.exp(sums[n] - top)
        columns = lax.broadcasted_iota(jnp.int32, sums[n].shape, 1) + firsts_ref[n]
        chosen = chosen + jnp.where(columns == ids, sums[n], 0.0)
    total = jnp.sum(total, axis=1, keepdims=True)
    chosen = jnp.sum(chosen, axis=1, keepdims=True)
    lane = lax.broadcasted_iota(jnp.int32, (groups, 128), 1)
    packed = jnp.zeros((groups, 128), jnp.float32)
    owned = pieces // halves
    for n, column in enumerate((top, total, chosen)):
        for r in range(owned):
            part = column[r * groups : (r + 1) * groups]
            packed = jnp.where(lane == n * owned + r, part, packed)
    for g in range(groups):
        out_ref[g] = packed[g : g + 1]


def logit_stats(all_rows, matrices, firsts, ids):
    groups = all_rows.shape[1]
    depth = matrices[0].shape[0]
    return pl.pallas_call(
        logits_kernel,
        out_shape=jax.ShapeDtypeStruct((groups, 1, 128), jnp.float32),
        in_specs=[smem_spec(), vmem_spec(), vmem_spec()] + [any_spec() for _ in matrices],
        out_specs=vmem_spec(),
        scratch_shapes=[
            pltpu.VMEM((len(matrices), depth, 128), jnp.bfloat16),
            pltpu.SemaphoreType.DMA((2 * len(matrices),)),
        ],
        cost_estimate=pl.CostEstimate(flops=270000000, bytes_accessed=4700000, transcendentals=0),
        name="logits",
    )(firsts, all_rows, ids, *matrices)


def merged(top, total, chosen, axis):
    highest = jnp.max(top, axis=axis, keepdims=True)
    scaled = jnp.sum(total * jnp.exp(top - highest), axis=axis)
    return jnp.squeeze(highest, axis), scaled, jnp.sum(chosen, axis=axis)


def per_device(
    queries,
    keys_new,
    values_new,
    out_gate,
    decay_logit,
    beta_logit,
    decay_rate,
    state,
    norm_gain,
    out_proj,
    residual,
    final_gain,
    value_weight,
    lm_head,
    sampled,
):
    chips, cores = lax.axis_size("heads_0"), lax.axis_size("heads_1")
    groups = lax.axis_size(GROUP)
    chip, core = lax.axis_index("heads_0"), lax.axis_index("heads_1")
    side = lax.axis_index("z_side")
    rows_own, width = residual.shape
    rows_core = rows_own // cores
    copies = chips // rows_core
    lanes = 128
    lines = width // lanes
    half = width // copies

    z_head = lax.ppermute(lm_head, "z_side", SWAP)
    core_head = lax.ppermute(lm_head, "heads_1", SWAP)
    both_head = lax.ppermute(z_head, "heads_1", SWAP)

    first = jnp.where((chip == 0) & (core == 0), 1.0, 0.0).reshape(1)
    partial_out = head_partials(
        queries,
        keys_new,
        values_new,
        out_gate,
        decay_logit,
        beta_logit,
        decay_rate,
        state,
        norm_gain,
        out_proj,
        residual,
        first,
        chips * cores,
    )
    arrived = exchange(partial_out, HEADS)
    gain = final_gain.reshape(lines, lanes)
    weight = value_weight.reshape(lines, lanes)
    half_here = (chip % copies).astype(jnp.int32).reshape(1)
    pieces, value = norm_pieces(arrived, gain, weight, half_here, groups, lines // copies)
    all_groups = exchange(pieces, GROUP).reshape(groups, half)
    all_rows = copy_for_each(all_groups, "heads_0")

    vocab_own = lm_head.shape[1]
    flat = lax.axis_index(HEADS_BATCH)
    across = (1 - 2 * core) * lax.axis_size(BATCH)
    along = (1 - 2 * side) * lax.axis_size("x")
    matrices = (lm_head, core_head, z_head, both_head)
    firsts = jnp.stack([flat, flat + across, flat + along, flat + across + along]) * vocab_own
    ids = sampled.reshape(-1, lax.axis_size("z_side"), lax.axis_size("x"), cores, rows_core)
    ids = lax.dynamic_index_in_dim(ids, side, 1, keepdims=False)
    ids = lax.dynamic_index_in_dim(ids, core, 2, keepdims=False)
    ids = ids.reshape(groups, rows_core).T.reshape(-1, 1)
    stats = logit_stats(all_rows, matrices, firsts.astype(jnp.int32), ids)
    stats = exchange(stats, GROUP)[:, 0, : 3 * rows_core].reshape(groups, 3, rows_core)
    stats = merged(stats[:, 0], stats[:, 1], stats[:, 2], 0)
    packed = jnp.concatenate([*stats, value[0, :1]])
    packed = copy_for_each(packed[None], HEADS).reshape(chips, cores, -1)
    found = packed[..., : 3 * rows_core].reshape(chips, cores, 3, rows_core)
    top, total, chosen = merged(found[:, :, 0], found[:, :, 1], found[:, :, 2], 0)
    logprob = (chosen - (top + jnp.log(total))).reshape(-1)
    values = packed[::copies, :, 3 * rows_core].T.reshape(-1)
    return (logprob, values)


def solution(mesh):
    torus = Mesh(
        mesh.devices.reshape(8, 2, 4, 2, 4), ("heads_0", "heads_1", "z_pair", "z_side", "x")
    )
    return jax.shard_map(
        per_device,
        mesh=torus,
        in_specs=(
            P(BATCH, HEADS),
            P(BATCH, HEADS),
            P(BATCH, HEADS),
            P(BATCH, HEADS),
            P(BATCH, HEADS),
            P(BATCH, HEADS),
            P(HEADS),
            P(BATCH, HEADS, None, None),
            P(),
            P(HEADS, None),
            P(BATCH, None),
            P(),
            P(),
            P(None, HEADS_BATCH),
            P(),
        ),
        out_specs=(P(BATCH), P(BATCH)),
        check_vma=False,
    )
```

```python
import functools

import jax
import jax.numpy as jnp
from jax import lax
from jax.experimental import pallas as pl
from jax.experimental.pallas import tpu as pltpu
from jax.sharding import Mesh
from jax.sharding import PartitionSpec as P


HEADS = ("heads_0", "heads_1")
BATCH = ("z_pair", "z_side", "x")
GROUP = ("z_pair", "x")
HEADS_BATCH = ("heads_0", "heads_1", "z_pair", "z_side", "x")
SWAP = [(0, 1), (1, 0)]


epsilon = 1e-06


def exchange(parts, axis):
    return lax.all_to_all(parts, axis, split_axis=0, concat_axis=0, tiled=True)


def any_spec():
    return pl.BlockSpec(memory_space=pl.ANY)


def vmem_spec():
    return pl.BlockSpec(memory_space=pltpu.VMEM)


def smem_spec():
    return pl.BlockSpec(memory_space=pltpu.SMEM)


def as_column(line):
    size = line.shape[1]
    shape = (size, size)
    here = lax.broadcasted_iota(jnp.int32, shape, 0) == lax.broadcasted_iota(jnp.int32, shape, 1)
    return jnp.sum(jnp.where(here, jnp.broadcast_to(line, shape), 0.0), axis=1, keepdims=True)


def heads_kernel(
    first_ref,
    rate_ref,
    *refs,
):
    inputs, out_ref, local, sems = refs[:10], refs[10], refs[11:21], refs[21]
    q_ref, k_ref, v_ref, g_ref, dl_ref, bl_ref, gain_ref, res_ref, state_ref, proj_ref = local
    copies = [pltpu.make_async_copy(inputs[n], local[n], sems.at[n]) for n in range(8)]
    heads = state_ref.shape[1]
    for h in range(heads):
        copies.append(
            pltpu.make_async_copy(inputs[8].at[:, h], state_ref.at[:, h], sems.at[8 + h])
        )
    blocks = 4
    wide = proj_ref.shape[1] // blocks
    for n in range(blocks):
        part = pl.ds(n * wide, wide)
        copies.append(
            pltpu.make_async_copy(
                inputs[9].at[:, part], proj_ref.at[:, part], sems.at[8 + heads + n]
            )
        )
    for copy in copies:
        copy.start()
    for copy in copies[:8]:
        copy.wait()
    rows = q_ref.shape[0]
    size = state_ref.shape[2]
    gain = gain_ref[...]
    queries, keys = [], []
    for h in range(heads):
        lanes = slice(h * size, (h + 1) * size)
        query = q_ref[:, lanes].astype(jnp.float32)
        key = k_ref[:, lanes].astype(jnp.float32)
        query = query / jnp.sqrt(jnp.sum(query * query, axis=1, keepdims=True) + epsilon)
        queries.append(query * size ** (-0.5))
        keys.append(key / jnp.sqrt(jnp.sum(key * key, axis=1, keepdims=True) + epsilon))
    turned = jnp.concatenate(queries + keys, axis=0).T
    parts = []
    for h in range(heads):
        lanes = slice(h * size, (h + 1) * size)
        logit = dl_ref[h : h + 1, :]
        soft = jnp.maximum(logit, 0.0) + jnp.log1p(jnp.exp(-jnp.abs(logit)))
        decay = as_column(jnp.exp(-rate_ref[h] * soft))
        strength = as_column(1.0 / (1.0 + jnp.exp(-bl_ref[h : h + 1, :])))
        inter = jnp.sum(queries[h] * keys[h], axis=1, keepdims=True)
        value = v_ref[:, lanes].astype(jnp.float32)
        gate = g_ref[:, lanes].astype(jnp.float32)
        copies[8 + h].wait()
        by_query, by_key = [], []
        for b in range(rows):
            block = state_ref[b, h]
            at = h * rows + b
            by_query.append(jnp.sum(turned[:, at : at + 1] * block, axis=0, keepdims=True))
            at += heads * rows
            by_key.append(jnp.sum(turned[:, at : at + 1] * block, axis=0, keepdims=True))
        state_query = jnp.concatenate(by_query, axis=0)
        state_key = jnp.concatenate(by_key, axis=0)
        written = value - decay * state_key
        output = decay * state_query + strength * inter * written
        mean = jnp.mean(output * output, axis=1, keepdims=True)
        normed = output / jnp.sqrt(mean + epsilon)
        parts.append(normed * gain * (gate / (1.0 + jnp.exp(-gate))))
    headout = jnp.concatenate(parts, axis=1).astype(jnp.bfloat16)
    first = first_ref[0]
    lines = wide // 128
    cores, halves = 2, out_ref.shape[0] // rows
    for n in range(blocks):
        copies[8 + heads + n].wait()
        part = slice(n * wide, (n + 1) * wide)
        total = jnp.dot(headout, proj_ref[:, part], preferred_element_type=jnp.float32)
        total = total + res_ref[:, part].astype(jnp.float32) * first
        total = total.reshape(rows, lines, 128)
        for row in range(rows):
            for half in range(halves):
                core, r = row // (rows // cores), row % (rows // cores)
                place = (r * halves + half) * cores + core
                out_ref[place, n * lines : (n + 1) * lines, :] = total[row]


def head_partials(
    queries,
    keys_new,
    values_new,
    out_gate,
    decay_logit,
    beta_logit,
    decay_rate,
    state,
    norm_gain,
    out_proj,
    residual,
    first,
    places,
):
    arrays = (
        queries,
        keys_new,
        values_new,
        out_gate,
        decay_logit.T,
        beta_logit.T,
        norm_gain.reshape(1, -1),
        residual,
        state,
        out_proj,
    )
    width = out_proj.shape[1]
    return pl.pallas_call(
        heads_kernel,
        out_shape=pltpu.VMEM((places, width // 128, 128), jnp.float32),
        in_specs=[smem_spec(), smem_spec()] + [any_spec() for _ in arrays],
        out_specs=vmem_spec(),
        scratch_shapes=[pltpu.VMEM(a.shape, a.dtype) for a in arrays]
        + [pltpu.SemaphoreType.DMA((8 + state.shape[1] + 4,))],
        cost_estimate=pl.CostEstimate(flops=40000000, bytes_accessed=3500000, transcendentals=0),
        name="heads",
    )(first, decay_rate, *arrays)


def norm_kernel(half_ref, arrived_ref, gain_ref, weight_ref, piece_ref, value_ref, scratch):
    width = gain_ref.size
    hsum = arrived_ref[0]
    for n in range(1, arrived_ref.shape[0]):
        hsum = hsum + arrived_ref[n]
    gain = gain_ref[...]
    squares = jnp.sum(hsum * hsum, axis=(0, 1), keepdims=True)
    terms = jnp.sum(hsum * gain * weight_ref[...], axis=(0, 1), keepdims=True)
    rstd = 1.0 / jnp.sqrt(squares / width + epsilon)
    scratch[...] = hsum * rstd * gain
    lines = piece_ref.shape[1]
    start = pl.multiple_of(half_ref[0] * lines, lines)
    piece = scratch[pl.ds(start, lines), :].astype(jnp.bfloat16)
    for n in range(piece_ref.shape[0]):
        piece_ref[n] = piece
    value_ref[...] = jnp.broadcast_to(rstd * terms, value_ref.shape)


def norm_pieces(arrived, gain, weight, half, copies, lines):
    return pl.pallas_call(
        norm_kernel,
        out_shape=(
            pltpu.VMEM((copies, lines, 128), jnp.bfloat16),
            pltpu.VMEM((1, 128), jnp.float32),
        ),
        in_specs=[smem_spec(), vmem_spec(), vmem_spec(), vmem_spec()],
        out_specs=(vmem_spec(), vmem_spec()),
        scratch_shapes=[pltpu.VMEM(gain.shape, jnp.float32)],
        cost_estimate=pl.CostEstimate(flops=4000000, bytes_accessed=400000, transcendentals=0),
        name="norm",
    )(half, arrived, gain, weight)


def logits_kernel(firsts_ref, rows_ref, ids_ref, *refs):
    count = 4
    matrices, out_ref, local, sems = refs[:count], refs[count], refs[count + 1], refs[count + 2]
    pieces, groups, deep = rows_ref.shape
    halves = local.shape[1] // deep
    copies = []
    for k in range(halves):
        part = pl.ds(k * deep, deep)
        for n in range(count):
            at = k * count + n
            copies.append(
                pltpu.make_async_copy(
                    matrices[n].at[part], local.at[n, part], sems.at[at]
                )
            )
    for copy in copies:
        copy.start()
    sums = [None] * count
    for k in range(halves):
        part = slice(k * deep, (k + 1) * deep)
        lhs = jnp.concatenate([rows_ref[p] for p in range(k, pieces, halves)], axis=0)
        for n in range(count):
            copies[k * count + n].wait()
            term = jnp.dot(lhs, local[n, part], preferred_element_type=jnp.float32)
            sums[n] = term if k == 0 else sums[n] + term
    top = sums[0]
    for n in range(1, count):
        top = jnp.maximum(top, sums[n])
    top = jnp.max(top, axis=1, keepdims=True)
    ids = ids_ref[...]
    total = jnp.zeros(sums[0].shape, jnp.float32)
    chosen = jnp.zeros(sums[0].shape, jnp.float32)
    for n in range(count):
        total = total + jnp.exp(sums[n] - top)
        columns = lax.broadcasted_iota(jnp.int32, sums[n].shape, 1) + firsts_ref[n]
        chosen = chosen + jnp.where(columns == ids, sums[n], 0.0)
    total = jnp.sum(total, axis=1, keepdims=True)
    chosen = jnp.sum(chosen, axis=1, keepdims=True)
    lane = lax.broadcasted_iota(jnp.int32, (groups, 128), 1)
    packed = jnp.zeros((groups, 128), jnp.float32)
    owned = pieces // halves
    for n, column in enumerate((top, total, chosen)):
        for r in range(owned):
            part = column[r * groups : (r + 1) * groups]
            packed = jnp.where(lane == n * owned + r, part, packed)
    for g in range(groups):
        out_ref[g] = packed[g : g + 1]


def logit_stats(all_rows, matrices, firsts, ids):
    groups = all_rows.shape[1]
    depth = matrices[0].shape[0]
    return pl.pallas_call(
        logits_kernel,
        out_shape=pltpu.VMEM((groups, 1, 128), jnp.float32),
        in_specs=[smem_spec(), vmem_spec(), vmem_spec()] + [any_spec() for _ in matrices],
        out_specs=vmem_spec(),
        scratch_shapes=[
            pltpu.VMEM((len(matrices), depth, 128), jnp.bfloat16),
            pltpu.SemaphoreType.DMA((2 * len(matrices),)),
        ],
        cost_estimate=pl.CostEstimate(flops=270000000, bytes_accessed=4700000, transcendentals=0),
        name="logits",
    )(firsts, all_rows, ids, *matrices)


def spread_kernel(groups_ref, out_ref):
    flat = groups_ref[...].astype(jnp.float32)
    flat = flat.reshape(out_ref.shape[1:]).astype(jnp.bfloat16)
    for n in range(out_ref.shape[0]):
        out_ref[n] = flat


def spread(pieces, copies):
    groups, lines, lanes = pieces.shape
    return pl.pallas_call(
        spread_kernel,
        out_shape=pltpu.VMEM((copies, groups, lines * lanes), jnp.bfloat16),
        in_specs=[vmem_spec()],
        out_specs=vmem_spec(),
        cost_estimate=pl.CostEstimate(flops=1000000, bytes_accessed=600000, transcendentals=0),
        name="spread",
    )(pieces)


def shifted(lines, places):
    return pltpu.roll(lines, places % 128, 1)


def merged(lines, keep, owned):
    low = jnp.min(lines, axis=0, keepdims=True)
    top = jnp.max(jnp.where(keep, lines, low), axis=0, keepdims=True)
    weight = jnp.where(keep, jnp.exp(jnp.minimum(lines - top, 0.0)), 0.0)
    total = jnp.sum(shifted(lines, -owned) * weight, axis=0, keepdims=True)
    chosen = jnp.sum(jnp.where(keep, lines, 0.0), axis=0, keepdims=True)
    return top, total, chosen


def group_kernel(owned, stats_ref, value_ref, out_ref):
    lines = stats_ref[...].reshape(stats_ref.shape[0], 128)
    top, total, chosen = merged(lines, jnp.full(lines.shape, True), owned)
    lane = lax.broadcasted_iota(jnp.int32, (1, 128), 1)
    packed = jnp.where(lane < owned, top, shifted(total, owned))
    packed = jnp.where(lane < 2 * owned, packed, chosen)
    packed = jnp.where(lane < 3 * owned, packed, value_ref[...])
    for n in range(out_ref.shape[0]):
        out_ref[n] = packed


def group_stats(stats, value, owned, copies):
    return pl.pallas_call(
        functools.partial(group_kernel, owned),
        out_shape=pltpu.VMEM((copies, 1, 128), jnp.float32),
        in_specs=[vmem_spec(), vmem_spec()],
        out_specs=vmem_spec(),
        name="group",
    )(stats, value)


def final_kernel(owned, cores, stats_ref, logprob_ref, value_ref):
    count = stats_ref.shape[0]
    lines = stats_ref[...].reshape(count, 128)
    place = lax.broadcasted_iota(jnp.int32, lines.shape, 0)
    lane = lax.broadcasted_iota(jnp.int32, lines.shape, 1)
    row = lax.broadcasted_iota(jnp.int32, (1, 128), 1)
    logprob = jnp.zeros((1, 128), jnp.float32)
    for core in range(cores):
        top, total, chosen = merged(lines, place % cores == core, owned)
        total = jnp.where(row < owned, total, 1.0)
        found = shifted(chosen, -2 * owned) - (top + jnp.log(total))
        logprob = jnp.where(row // owned == core, shifted(found, core * owned), logprob)
    values = jnp.broadcast_to(lines[:, 3 * owned : 3 * owned + 1], lines.shape)
    here = place == (lane % owned) * (count // owned) + lane // owned
    value = jnp.sum(jnp.where(here, values, 0.0), axis=0, keepdims=True)
    logprob_ref[...] = logprob[:, : logprob_ref.shape[1]]
    value_ref[...] = value[:, : value_ref.shape[1]]


def final_values(stats, owned, cores):
    rows = owned * cores
    return pl.pallas_call(
        functools.partial(final_kernel, owned, cores),
        out_shape=(
            jax.ShapeDtypeStruct((1, rows), jnp.float32),
            jax.ShapeDtypeStruct((1, rows), jnp.float32),
        ),
        in_specs=[vmem_spec()],
        out_specs=(vmem_spec(), vmem_spec()),
        name="final",
    )(stats)


def per_device(
    queries,
    keys_new,
    values_new,
    out_gate,
    decay_logit,
    beta_logit,
    decay_rate,
    state,
    norm_gain,
    out_proj,
    residual,
    final_gain,
    value_weight,
    lm_head,
    sampled,
):
    chips, cores = lax.axis_size("heads_0"), lax.axis_size("heads_1")
    groups = lax.axis_size(GROUP)
    chip, core = lax.axis_index("heads_0"), lax.axis_index("heads_1")
    side = lax.axis_index("z_side")
    rows_own, width = residual.shape
    rows_core = rows_own // cores
    copies = chips // rows_core
    lanes = 128
    lines = width // lanes

    z_head = lax.ppermute(lm_head, "z_side", SWAP)
    core_head = lax.ppermute(lm_head, "heads_1", SWAP)
    both_head = lax.ppermute(z_head, "heads_1", SWAP)

    first = jnp.where((chip == 0) & (core == 0), 1.0, 0.0).reshape(1)
    partial_out = head_partials(
        queries,
        keys_new,
        values_new,
        out_gate,
        decay_logit,
        beta_logit,
        decay_rate,
        state,
        norm_gain,
        out_proj,
        residual,
        first,
        chips * cores,
    )
    arrived = exchange(partial_out, HEADS)
    gain = final_gain.reshape(lines, lanes)
    weight = value_weight.reshape(lines, lanes)
    half_here = (chip % copies).astype(jnp.int32).reshape(1)
    pieces, value = norm_pieces(arrived, gain, weight, half_here, groups, lines // copies)
    for_chips = spread(exchange(pieces, GROUP), chips)
    all_rows = exchange(for_chips, "heads_0")

    vocab_own = lm_head.shape[1]
    flat = lax.axis_index(HEADS_BATCH)
    across = (1 - 2 * core) * lax.axis_size(BATCH)
    along = (1 - 2 * side) * lax.axis_size("x")
    matrices = (lm_head, core_head, z_head, both_head)
    firsts = jnp.stack([flat, flat + across, flat + along, flat + across + along]) * vocab_own
    ids = sampled.reshape(-1, lax.axis_size("z_side"), lax.axis_size("x"), cores, rows_core)
    ids = lax.dynamic_index_in_dim(ids, side, 1, keepdims=False)
    ids = lax.dynamic_index_in_dim(ids, core, 2, keepdims=False)
    ids = ids.reshape(groups, rows_core).T.reshape(-1, 1)
    stats = logit_stats(all_rows, matrices, firsts.astype(jnp.int32), ids)
    stats = group_stats(exchange(stats, GROUP), value, rows_core, chips * cores)
    logprob, values = final_values(exchange(stats, HEADS), rows_core, cores)
    return (logprob.reshape(-1), values.reshape(-1))


def solution(mesh):
    torus = Mesh(
        mesh.devices.reshape(8, 2, 4, 2, 4), ("heads_0", "heads_1", "z_pair", "z_side", "x")
    )
    return jax.shard_map(
        per_device,
        mesh=torus,
        in_specs=(
            P(BATCH, HEADS),
            P(BATCH, HEADS),
            P(BATCH, HEADS),
            P(BATCH, HEADS),
            P(BATCH, HEADS),
            P(BATCH, HEADS),
            P(HEADS),
            P(BATCH, HEADS, None, None),
            P(),
            P(HEADS, None),
            P(BATCH, None),
            P(),
            P(),
            P(None, HEADS_BATCH),
            P(),
        ),
        out_specs=(P(BATCH), P(BATCH)),
        check_vma=False,
    )
```

```python
import functools

import jax
import jax.numpy as jnp
from jax import lax
from jax.experimental import pallas as pl
from jax.experimental.pallas import tpu as pltpu
from jax.sharding import Mesh
from jax.sharding import PartitionSpec as P


HEADS = ("heads_0", "heads_1")
BATCH = ("z_pair", "z_side", "x")
GROUP = ("z_pair", "x")
GATHER = ("heads_0", "z_pair", "x")
HEADS_BATCH = ("heads_0", "heads_1", "z_pair", "z_side", "x")
SWAP = [(0, 1), (1, 0)]


epsilon = 1e-06


def exchange(parts, axis):
    return lax.all_to_all(parts, axis, split_axis=0, concat_axis=0, tiled=True)


def any_spec():
    return pl.BlockSpec(memory_space=pltpu.HBM)


def room(mebibytes):
    return pltpu.CompilerParams(vmem_limit_bytes=mebibytes * 2**20)


def vmem_spec():
    return pl.BlockSpec(memory_space=pltpu.VMEM)


def smem_spec():
    return pl.BlockSpec(memory_space=pltpu.SMEM)


def as_column(line):
    size = line.shape[1]
    shape = (size, size)
    here = lax.broadcasted_iota(jnp.int32, shape, 0) == lax.broadcasted_iota(jnp.int32, shape, 1)
    return jnp.sum(jnp.where(here, jnp.broadcast_to(line, shape), 0.0), axis=1, keepdims=True)


def heads_kernel(
    first_ref,
    rate_ref,
    *refs,
):
    inputs, out_ref, local, sems = refs[:10], refs[10], refs[11:21], refs[21]
    q_ref, k_ref, v_ref, g_ref, dl_ref, bl_ref, gain_ref, res_ref, state_ref, proj_ref = local
    copies = [pltpu.make_async_copy(inputs[n], local[n], sems.at[n]) for n in range(8)]
    heads = state_ref.shape[1]
    for h in range(heads):
        copies.append(
            pltpu.make_async_copy(inputs[8].at[:, h], state_ref.at[:, h], sems.at[8 + h])
        )
    blocks = 4
    wide = proj_ref.shape[1] // blocks
    for n in range(blocks):
        part = pl.ds(n * wide, wide)
        copies.append(
            pltpu.make_async_copy(
                inputs[9].at[:, part], proj_ref.at[:, part], sems.at[8 + heads + n]
            )
        )
    for copy in copies:
        copy.start()
    for copy in copies[:8]:
        copy.wait()
    rows = q_ref.shape[0]
    size = state_ref.shape[2]
    gain = gain_ref[...]
    queries, keys = [], []
    for h in range(heads):
        lanes = slice(h * size, (h + 1) * size)
        query = q_ref[:, lanes].astype(jnp.float32)
        key = k_ref[:, lanes].astype(jnp.float32)
        query = query / jnp.sqrt(jnp.sum(query * query, axis=1, keepdims=True) + epsilon)
        queries.append(query * size ** (-0.5))
        keys.append(key / jnp.sqrt(jnp.sum(key * key, axis=1, keepdims=True) + epsilon))
    turned = jnp.concatenate(queries + keys, axis=0).T
    parts = []
    for h in range(heads):
        lanes = slice(h * size, (h + 1) * size)
        logit = dl_ref[h : h + 1, :]
        soft = jnp.maximum(logit, 0.0) + jnp.log1p(jnp.exp(-jnp.abs(logit)))
        decay = as_column(jnp.exp(-rate_ref[h] * soft))
        strength = as_column(1.0 / (1.0 + jnp.exp(-bl_ref[h : h + 1, :])))
        inter = jnp.sum(queries[h] * keys[h], axis=1, keepdims=True)
        value = v_ref[:, lanes].astype(jnp.float32)
        gate = g_ref[:, lanes].astype(jnp.float32)
        copies[8 + h].wait()
        by_query, by_key = [], []
        for b in range(rows):
            block = state_ref[b, h]
            at = h * rows + b
            by_query.append(jnp.sum(turned[:, at : at + 1] * block, axis=0, keepdims=True))
            at += heads * rows
            by_key.append(jnp.sum(turned[:, at : at + 1] * block, axis=0, keepdims=True))
        state_query = jnp.concatenate(by_query, axis=0)
        state_key = jnp.concatenate(by_key, axis=0)
        written = value - decay * state_key
        output = decay * state_query + strength * inter * written
        mean = jnp.mean(output * output, axis=1, keepdims=True)
        normed = output / jnp.sqrt(mean + epsilon)
        parts.append(normed * gain * (gate / (1.0 + jnp.exp(-gate))))
    headout = jnp.concatenate(parts, axis=1).astype(jnp.bfloat16)
    first = first_ref[0]
    lines = wide // 128
    cores, halves = 2, out_ref.shape[0] // rows
    for n in range(blocks):
        copies[8 + heads + n].wait()
        part = slice(n * wide, (n + 1) * wide)
        total = jnp.dot(headout, proj_ref[:, part], preferred_element_type=jnp.float32)
        total = total + res_ref[:, part].astype(jnp.float32) * first
        total = total.reshape(rows, lines, 128)
        for row in range(rows):
            for half in range(halves):
                core, r = row // (rows // cores), row % (rows // cores)
                place = (r * halves + half) * cores + core
                out_ref[place, n * lines : (n + 1) * lines, :] = total[row]


def head_partials(
    queries,
    keys_new,
    values_new,
    out_gate,
    decay_logit,
    beta_logit,
    decay_rate,
    state,
    norm_gain,
    out_proj,
    residual,
    first,
    places,
):
    arrays = (
        queries,
        keys_new,
        values_new,
        out_gate,
        decay_logit.T,
        beta_logit.T,
        norm_gain.reshape(1, -1),
        residual,
        state,
        out_proj,
    )
    width = out_proj.shape[1]
    return pl.pallas_call(
        heads_kernel,
        out_shape=pltpu.VMEM((places, width // 128, 128), jnp.float32),
        in_specs=[smem_spec(), smem_spec()] + [any_spec() for _ in arrays],
        out_specs=vmem_spec(),
        scratch_shapes=[pltpu.VMEM(a.shape, a.dtype) for a in arrays]
        + [pltpu.SemaphoreType.DMA((8 + state.shape[1] + 4,))],
        cost_estimate=pl.CostEstimate(flops=40000000, bytes_accessed=3500000, transcendentals=0),
        name="heads",
    )(first, decay_rate, *arrays)


def norm_kernel(half_ref, arrived_ref, gain_ref, weight_ref, piece_ref, value_ref, scratch):
    width = gain_ref.size
    hsum = arrived_ref[0]
    for n in range(1, arrived_ref.shape[0]):
        hsum = hsum + arrived_ref[n]
    gain = gain_ref[...]
    squares = jnp.sum(hsum * hsum, axis=(0, 1), keepdims=True)
    terms = jnp.sum(hsum * gain * weight_ref[...], axis=(0, 1), keepdims=True)
    rstd = 1.0 / jnp.sqrt(squares / width + epsilon)
    scratch[...] = hsum * rstd * gain
    lines = piece_ref.shape[1]
    start = pl.multiple_of(half_ref[0] * lines, lines)
    piece = scratch[pl.ds(start, lines), :].astype(jnp.bfloat16)
    for n in range(piece_ref.shape[0]):
        piece_ref[n] = piece
    value_ref[...] = jnp.broadcast_to(rstd * terms, value_ref.shape)


def norm_pieces(arrived, gain, weight, half, copies, lines):
    return pl.pallas_call(
        norm_kernel,
        out_shape=(
            pltpu.VMEM((copies, lines, 128), jnp.bfloat16),
            pltpu.VMEM((1, 128), jnp.float32),
        ),
        in_specs=[smem_spec(), vmem_spec(), vmem_spec(), vmem_spec()],
        out_specs=(vmem_spec(), vmem_spec()),
        scratch_shapes=[pltpu.VMEM(gain.shape, jnp.float32)],
        cost_estimate=pl.CostEstimate(flops=4000000, bytes_accessed=400000, transcendentals=0),
        compiler_params=room(4),
        name="norm",
    )(half, arrived, gain, weight)


def logits_kernel(firsts_ref, rows_ref, ids_ref, *refs):
    count = 4
    matrices, out_ref, local, flat, sems = refs[:count], *refs[count:]
    pieces, groups, tiles, lanes = rows_ref.shape
    deep = tiles * lanes
    halves = local.shape[1] // deep
    copies = []
    for k in range(halves):
        part = pl.ds(k * deep, deep)
        for n in range(count):
            at = k * count + n
            copies.append(
                pltpu.make_async_copy(
                    matrices[n].at[part], local.at[n, part], sems.at[at]
                )
            )
    for copy in copies:
        copy.start()
    flat[...] = rows_ref[...].reshape(flat.shape).astype(jnp.float32)

    def rows_of(piece):
        start = piece * groups * tiles
        return jnp.concatenate(
            [flat[pl.ds(start + t, groups, stride=tiles), :] for t in range(tiles)], axis=1
        ).astype(jnp.bfloat16)

    sums = [None] * count
    for k in range(halves):
        part = slice(k * deep, (k + 1) * deep)
        lhs = jnp.concatenate([rows_of(p) for p in range(k, pieces, halves)], axis=0)
        for n in range(count):
            copies[k * count + n].wait()
            term = jnp.dot(lhs, local[n, part], preferred_element_type=jnp.float32)
            sums[n] = term if k == 0 else sums[n] + term
    top = sums[0]
    for n in range(1, count):
        top = jnp.maximum(top, sums[n])
    top = jnp.max(top, axis=1, keepdims=True)
    ids = ids_ref[...]
    total = jnp.zeros(sums[0].shape, jnp.float32)
    chosen = jnp.zeros(sums[0].shape, jnp.float32)
    for n in range(count):
        total = total + jnp.exp(sums[n] - top)
        columns = lax.broadcasted_iota(jnp.int32, sums[n].shape, 1) + firsts_ref[n]
        chosen = chosen + jnp.where(columns == ids, sums[n], 0.0)
    total = jnp.sum(total, axis=1, keepdims=True)
    chosen = jnp.sum(chosen, axis=1, keepdims=True)
    lane = lax.broadcasted_iota(jnp.int32, (groups, 128), 1)
    packed = jnp.zeros((groups, 128), jnp.float32)
    owned = pieces // halves
    for n, column in enumerate((top, total, chosen)):
        for r in range(owned):
            part = column[r * groups : (r + 1) * groups]
            packed = jnp.where(lane == n * owned + r, part, packed)
    for g in range(groups):
        out_ref[g] = packed[g : g + 1]


def logit_stats(all_rows, matrices, firsts, ids):
    groups = all_rows.shape[1]
    depth = matrices[0].shape[0]
    return pl.pallas_call(
        logits_kernel,
        out_shape=pltpu.VMEM((groups, 1, 128), jnp.float32),
        in_specs=[smem_spec(), vmem_spec(), vmem_spec()] + [any_spec() for _ in matrices],
        out_specs=vmem_spec(),
        scratch_shapes=[
            pltpu.VMEM((len(matrices), depth, 128), jnp.bfloat16),
            pltpu.VMEM((all_rows.size // 128, 128), jnp.float32),
            pltpu.SemaphoreType.DMA((2 * len(matrices),)),
        ],
        cost_estimate=pl.CostEstimate(flops=270000000, bytes_accessed=4700000, transcendentals=0),
        compiler_params=room(12),
        name="logits",
    )(firsts, all_rows, ids, *matrices)


def shifted(lines, places):
    return pltpu.roll(lines, places % 128, 1)


def merged(lines, keep, owned):
    low = jnp.min(lines, axis=0, keepdims=True)
    top = jnp.max(jnp.where(keep, lines, low), axis=0, keepdims=True)
    weight = jnp.where(keep, jnp.exp(jnp.minimum(lines - top, 0.0)), 0.0)
    total = jnp.sum(shifted(lines, -owned) * weight, axis=0, keepdims=True)
    chosen = jnp.sum(jnp.where(keep, lines, 0.0), axis=0, keepdims=True)
    return top, total, chosen


def group_kernel(owned, stats_ref, value_ref, out_ref):
    lines = stats_ref[...].reshape(stats_ref.shape[0], 128)
    top, total, chosen = merged(lines, jnp.full(lines.shape, True), owned)
    lane = lax.broadcasted_iota(jnp.int32, (1, 128), 1)
    packed = jnp.where(lane < owned, top, shifted(total, owned))
    packed = jnp.where(lane < 2 * owned, packed, chosen)
    packed = jnp.where(lane < 3 * owned, packed, value_ref[...])
    for n in range(out_ref.shape[0]):
        out_ref[n] = packed


def group_stats(stats, value, owned, copies):
    return pl.pallas_call(
        functools.partial(group_kernel, owned),
        out_shape=pltpu.VMEM((copies, 1, 128), jnp.float32),
        in_specs=[vmem_spec(), vmem_spec()],
        out_specs=vmem_spec(),
        compiler_params=room(2),
        name="group",
    )(stats, value)


def final_kernel(owned, cores, stats_ref, logprob_ref, value_ref):
    count = stats_ref.shape[0]
    lines = stats_ref[...].reshape(count, 128)
    place = lax.broadcasted_iota(jnp.int32, lines.shape, 0)
    lane = lax.broadcasted_iota(jnp.int32, lines.shape, 1)
    row = lax.broadcasted_iota(jnp.int32, (1, 128), 1)
    logprob = jnp.zeros((1, 128), jnp.float32)
    for core in range(cores):
        top, total, chosen = merged(lines, place % cores == core, owned)
        total = jnp.where(row < owned, total, 1.0)
        found = shifted(chosen, -2 * owned) - (top + jnp.log(total))
        logprob = jnp.where(row // owned == core, shifted(found, core * owned), logprob)
    values = jnp.broadcast_to(lines[:, 3 * owned : 3 * owned + 1], lines.shape)
    here = place == (lane % owned) * (count // owned) + lane // owned
    value = jnp.sum(jnp.where(here, values, 0.0), axis=0, keepdims=True)
    logprob_ref[...] = logprob[:, : logprob_ref.shape[1]]
    value_ref[...] = value[:, : value_ref.shape[1]]


def final_values(stats, owned, cores):
    rows = owned * cores
    return pl.pallas_call(
        functools.partial(final_kernel, owned, cores),
        out_shape=(
            jax.ShapeDtypeStruct((1, rows), jnp.float32),
            jax.ShapeDtypeStruct((1, rows), jnp.float32),
        ),
        in_specs=[vmem_spec()],
        out_specs=(vmem_spec(), vmem_spec()),
        compiler_params=room(2),
        name="final",
    )(stats)


def per_device(
    queries,
    keys_new,
    values_new,
    out_gate,
    decay_logit,
    beta_logit,
    decay_rate,
    state,
    norm_gain,
    out_proj,
    residual,
    final_gain,
    value_weight,
    lm_head,
    sampled,
):
    chips, cores = lax.axis_size("heads_0"), lax.axis_size("heads_1")
    groups = lax.axis_size(GROUP)
    chip, core = lax.axis_index("heads_0"), lax.axis_index("heads_1")
    side = lax.axis_index("z_side")
    rows_own, width = residual.shape
    rows_core = rows_own // cores
    copies = chips // rows_core
    lanes = 128
    lines = width // lanes

    z_head = lax.ppermute(lm_head, "z_side", SWAP)
    core_head = lax.ppermute(lm_head, "heads_1", SWAP)
    both_head = lax.ppermute(z_head, "heads_1", SWAP)

    first = jnp.where((chip == 0) & (core == 0), 1.0, 0.0).reshape(1)
    partial_out = head_partials(
        queries,
        keys_new,
        values_new,
        out_gate,
        decay_logit,
        beta_logit,
        decay_rate,
        state,
        norm_gain,
        out_proj,
        residual,
        first,
        chips * cores,
    )
    arrived = exchange(partial_out, HEADS)
    gain = final_gain.reshape(lines, lanes)
    weight = value_weight.reshape(lines, lanes)
    half_here = (chip % copies).astype(jnp.int32).reshape(1)
    pieces, value = norm_pieces(arrived, gain, weight, half_here, chips * groups, lines // copies)
    all_rows = exchange(pieces, GATHER)
    all_rows = all_rows.reshape(chips, groups, lines // copies, lanes)

    vocab_own = lm_head.shape[1]
    flat = lax.axis_index(HEADS_BATCH)
    across = (1 - 2 * core) * lax.axis_size(BATCH)
    along = (1 - 2 * side) * lax.axis_size("x")
    matrices = (lm_head, core_head, z_head, both_head)
    firsts = jnp.stack([flat, flat + across, flat + along, flat + across + along]) * vocab_own
    ids = sampled.reshape(-1, lax.axis_size("z_side"), lax.axis_size("x"), cores, rows_core)
    ids = lax.dynamic_index_in_dim(ids, side, 1, keepdims=False)
    ids = lax.dynamic_index_in_dim(ids, core, 2, keepdims=False)
    ids = ids.reshape(groups, rows_core).T.reshape(-1, 1)
    stats = logit_stats(all_rows, matrices, firsts.astype(jnp.int32), ids)
    stats = group_stats(exchange(stats, GROUP), value, rows_core, chips * cores)
    logprob, values = final_values(exchange(stats, HEADS), rows_core, cores)
    return (logprob.reshape(-1), values.reshape(-1))


def solution(mesh):
    torus = Mesh(
        mesh.devices.reshape(8, 2, 4, 2, 4), ("heads_0", "heads_1", "z_pair", "z_side", "x")
    )
    return jax.shard_map(
        per_device,
        mesh=torus,
        in_specs=(
            P(BATCH, HEADS),
            P(BATCH, HEADS),
            P(BATCH, HEADS),
            P(BATCH, HEADS),
            P(BATCH, HEADS),
            P(BATCH, HEADS),
            P(HEADS),
            P(BATCH, HEADS, None, None),
            P(),
            P(HEADS, None),
            P(BATCH, None),
            P(),
            P(),
            P(None, HEADS_BATCH),
            P(),
        ),
        out_specs=(P(BATCH), P(BATCH)),
        check_vma=False,
    )
```

```python
import functools

import jax
import jax.numpy as jnp
from jax import lax
from jax.experimental import pallas as pl
from jax.experimental.pallas import tpu as pltpu
from jax.sharding import Mesh
from jax.sharding import PartitionSpec as P


HEADS = ("heads_0", "heads_1")
BATCH = ("z_pair", "z_side", "x")
GROUP = ("z_pair", "x")
GATHER = ("heads_0", "z_pair", "x")
ROWS = ("heads_0", "heads_1", "z_pair", "x")
HEADS_BATCH = ("heads_0", "heads_1", "z_pair", "z_side", "x")
SWAP = [(0, 1), (1, 0)]


epsilon = 1e-06


def exchange(parts, axis):
    return lax.all_to_all(parts, axis, split_axis=0, concat_axis=0, tiled=True)


def any_spec():
    return pl.BlockSpec(memory_space=pltpu.HBM)


def room(mebibytes):
    return pltpu.CompilerParams(vmem_limit_bytes=mebibytes * 2**20)


def vmem_spec():
    return pl.BlockSpec(memory_space=pltpu.VMEM)


def smem_spec():
    return pl.BlockSpec(memory_space=pltpu.SMEM)


def as_column(line):
    size = line.shape[1]
    shape = (size, size)
    here = lax.broadcasted_iota(jnp.int32, shape, 0) == lax.broadcasted_iota(jnp.int32, shape, 1)
    return jnp.sum(jnp.where(here, jnp.broadcast_to(line, shape), 0.0), axis=1, keepdims=True)


def heads_kernel(
    first_ref,
    rate_ref,
    *refs,
):
    inputs, out_ref, local, sems = refs[:10], refs[10], refs[11:21], refs[21]
    q_ref, k_ref, v_ref, g_ref, dl_ref, bl_ref, gain_ref, res_ref, state_ref, proj_ref = local
    copies = [pltpu.make_async_copy(inputs[n], local[n], sems.at[n]) for n in range(8)]
    heads = state_ref.shape[1]
    for h in range(heads):
        copies.append(
            pltpu.make_async_copy(inputs[8].at[:, h], state_ref.at[:, h], sems.at[8 + h])
        )
    blocks = 4
    wide = proj_ref.shape[1] // blocks
    for n in range(blocks):
        part = pl.ds(n * wide, wide)
        copies.append(
            pltpu.make_async_copy(
                inputs[9].at[:, part], proj_ref.at[:, part], sems.at[8 + heads + n]
            )
        )
    for copy in copies:
        copy.start()
    for copy in copies[:8]:
        copy.wait()
    rows = q_ref.shape[0]
    size = state_ref.shape[2]
    gain = gain_ref[...]
    queries, keys = [], []
    for h in range(heads):
        lanes = slice(h * size, (h + 1) * size)
        query = q_ref[:, lanes].astype(jnp.float32)
        key = k_ref[:, lanes].astype(jnp.float32)
        query = query / jnp.sqrt(jnp.sum(query * query, axis=1, keepdims=True) + epsilon)
        queries.append(query * size ** (-0.5))
        keys.append(key / jnp.sqrt(jnp.sum(key * key, axis=1, keepdims=True) + epsilon))
    turned = jnp.concatenate(queries + keys, axis=0).T
    parts = []
    for h in range(heads):
        lanes = slice(h * size, (h + 1) * size)
        logit = dl_ref[h : h + 1, :]
        soft = jnp.maximum(logit, 0.0) + jnp.log1p(jnp.exp(-jnp.abs(logit)))
        decay = as_column(jnp.exp(-rate_ref[h] * soft))
        strength = as_column(1.0 / (1.0 + jnp.exp(-bl_ref[h : h + 1, :])))
        inter = jnp.sum(queries[h] * keys[h], axis=1, keepdims=True)
        value = v_ref[:, lanes].astype(jnp.float32)
        gate = g_ref[:, lanes].astype(jnp.float32)
        copies[8 + h].wait()
        by_query, by_key = [], []
        for b in range(rows):
            block = state_ref[b, h]
            at = h * rows + b
            by_query.append(jnp.sum(turned[:, at : at + 1] * block, axis=0, keepdims=True))
            at += heads * rows
            by_key.append(jnp.sum(turned[:, at : at + 1] * block, axis=0, keepdims=True))
        state_query = jnp.concatenate(by_query, axis=0)
        state_key = jnp.concatenate(by_key, axis=0)
        written = value - decay * state_key
        output = decay * state_query + strength * inter * written
        mean = jnp.mean(output * output, axis=1, keepdims=True)
        normed = output / jnp.sqrt(mean + epsilon)
        parts.append(normed * gain * (gate / (1.0 + jnp.exp(-gate))))
    headout = jnp.concatenate(parts, axis=1).astype(jnp.bfloat16)
    first = first_ref[0]
    lines = wide // 128
    cores, halves = 2, out_ref.shape[0] // rows
    for n in range(blocks):
        copies[8 + heads + n].wait()
        part = slice(n * wide, (n + 1) * wide)
        total = jnp.dot(headout, proj_ref[:, part], preferred_element_type=jnp.float32)
        total = total + res_ref[:, part].astype(jnp.float32) * first
        total = total.reshape(rows, lines, 128)
        for row in range(rows):
            for half in range(halves):
                core, r = row // (rows // cores), row % (rows // cores)
                place = (r * halves + half) * cores + core
                out_ref[place, n * lines : (n + 1) * lines, :] = total[row]


def head_partials(
    queries,
    keys_new,
    values_new,
    out_gate,
    decay_logit,
    beta_logit,
    decay_rate,
    state,
    norm_gain,
    out_proj,
    residual,
    first,
    places,
):
    arrays = (
        queries,
        keys_new,
        values_new,
        out_gate,
        decay_logit.T,
        beta_logit.T,
        norm_gain.reshape(1, -1),
        residual,
        state,
        out_proj,
    )
    width = out_proj.shape[1]
    return pl.pallas_call(
        heads_kernel,
        out_shape=pltpu.VMEM((places, width // 128, 128), jnp.float32),
        in_specs=[smem_spec(), smem_spec()] + [any_spec() for _ in arrays],
        out_specs=vmem_spec(),
        scratch_shapes=[pltpu.VMEM(a.shape, a.dtype) for a in arrays]
        + [pltpu.SemaphoreType.DMA((8 + state.shape[1] + 4,))],
        cost_estimate=pl.CostEstimate(flops=40000000, bytes_accessed=3500000, transcendentals=0),
        name="heads",
    )(first, decay_rate, *arrays)


def norm_kernel(half_ref, arrived_ref, gain_ref, weight_ref, piece_ref, value_ref, scratch):
    width = gain_ref.size
    hsum = arrived_ref[0]
    for n in range(1, arrived_ref.shape[0]):
        hsum = hsum + arrived_ref[n]
    gain = gain_ref[...]
    squares = jnp.sum(hsum * hsum, axis=(0, 1), keepdims=True)
    terms = jnp.sum(hsum * gain * weight_ref[...], axis=(0, 1), keepdims=True)
    rstd = 1.0 / jnp.sqrt(squares / width + epsilon)
    scratch[...] = hsum * rstd * gain
    lines = piece_ref.shape[1]
    start = pl.multiple_of(half_ref[0] * lines, lines)
    piece = scratch[pl.ds(start, lines), :].astype(jnp.bfloat16)
    for n in range(piece_ref.shape[0]):
        piece_ref[n] = piece
    value_ref[...] = jnp.broadcast_to(rstd * terms, value_ref.shape)


def norm_pieces(arrived, gain, weight, half, copies, lines):
    return pl.pallas_call(
        norm_kernel,
        out_shape=(
            pltpu.VMEM((copies, lines, 128), jnp.bfloat16),
            pltpu.VMEM((1, 128), jnp.float32),
        ),
        in_specs=[smem_spec(), vmem_spec(), vmem_spec(), vmem_spec()],
        out_specs=(vmem_spec(), vmem_spec()),
        scratch_shapes=[pltpu.VMEM(gain.shape, jnp.float32)],
        cost_estimate=pl.CostEstimate(flops=4000000, bytes_accessed=400000, transcendentals=0),
        compiler_params=room(4),
        name="norm",
    )(half, arrived, gain, weight)


def logits_kernel(firsts_ref, rows_ref, ids_ref, value_ref, *refs):
    count = 4
    matrices, out_ref, local, flat, sems = refs[:count], *refs[count:]
    pieces, groups, tiles, lanes = rows_ref.shape
    deep = tiles * lanes
    halves = local.shape[1] // deep
    copies = []
    for k in range(halves):
        part = pl.ds(k * deep, deep)
        for n in range(count):
            at = k * count + n
            copies.append(
                pltpu.make_async_copy(
                    matrices[n].at[part], local.at[n, part], sems.at[at]
                )
            )
    for copy in copies:
        copy.start()
    flat[...] = rows_ref[...].reshape(flat.shape).astype(jnp.float32)

    def rows_of(piece):
        start = piece * groups * tiles
        return jnp.concatenate(
            [flat[pl.ds(start + t, groups, stride=tiles), :] for t in range(tiles)], axis=1
        ).astype(jnp.bfloat16)

    sums = [None] * count
    for k in range(halves):
        part = slice(k * deep, (k + 1) * deep)
        lhs = jnp.concatenate([rows_of(p) for p in range(k, pieces, halves)], axis=0)
        for n in range(count):
            copies[k * count + n].wait()
            term = jnp.dot(lhs, local[n, part], preferred_element_type=jnp.float32)
            sums[n] = term if k == 0 else sums[n] + term
    top = sums[0]
    for n in range(1, count):
        top = jnp.maximum(top, sums[n])
    top = jnp.max(top, axis=1, keepdims=True)
    ids = ids_ref[...]
    total = jnp.zeros(sums[0].shape, jnp.float32)
    chosen = jnp.zeros(sums[0].shape, jnp.float32)
    for n in range(count):
        total = total + jnp.exp(sums[n] - top)
        columns = lax.broadcasted_iota(jnp.int32, sums[n].shape, 1) + firsts_ref[n]
        chosen = chosen + jnp.where(columns == ids, sums[n], 0.0)
    total = jnp.sum(total, axis=1, keepdims=True)
    chosen = jnp.sum(chosen, axis=1, keepdims=True)
    lane = lax.broadcasted_iota(jnp.int32, (groups, 128), 1)
    packed = jnp.broadcast_to(value_ref[...], (groups, 128))
    owned = pieces // halves
    for n, column in enumerate((top, total, chosen)):
        for r in range(owned):
            part = column[r * groups : (r + 1) * groups]
            packed = jnp.where(lane == n * owned + r, part, packed)
    for place in range(out_ref.shape[0]):
        g = place % groups
        out_ref[place] = packed[g : g + 1]


def logit_stats(all_rows, matrices, firsts, ids, value, places):
    groups = all_rows.shape[1]
    depth = matrices[0].shape[0]
    return pl.pallas_call(
        logits_kernel,
        out_shape=pltpu.VMEM((places * groups, 1, 128), jnp.float32),
        in_specs=[smem_spec(), vmem_spec(), vmem_spec(), vmem_spec()]
        + [any_spec() for _ in matrices],
        out_specs=vmem_spec(),
        scratch_shapes=[
            pltpu.VMEM((len(matrices), depth, 128), jnp.bfloat16),
            pltpu.VMEM((all_rows.size // 128, 128), jnp.float32),
            pltpu.SemaphoreType.DMA((2 * len(matrices),)),
        ],
        cost_estimate=pl.CostEstimate(flops=270000000, bytes_accessed=4700000, transcendentals=0),
        compiler_params=room(12),
        name="logits",
    )(firsts, all_rows, ids, value, *matrices)


def shifted(lines, places):
    return pltpu.roll(lines, places % 128, 1)


def merged(lines, keep, owned):
    low = jnp.min(lines, axis=0, keepdims=True)
    top = jnp.max(jnp.where(keep, lines, low), axis=0, keepdims=True)
    weight = jnp.where(keep, jnp.exp(jnp.minimum(lines - top, 0.0)), 0.0)
    total = jnp.sum(shifted(lines, -owned) * weight, axis=0, keepdims=True)
    chosen = jnp.sum(jnp.where(keep, lines, 0.0), axis=0, keepdims=True)
    return top, total, chosen


def final_kernel(owned, cores, groups, group_ref, stats_ref, logprob_ref, value_ref):
    count = stats_ref.shape[0]
    lines = stats_ref[...].reshape(count, 128)
    place = lax.broadcasted_iota(jnp.int32, lines.shape, 0)
    lane = lax.broadcasted_iota(jnp.int32, lines.shape, 1)
    row = lax.broadcasted_iota(jnp.int32, (1, 128), 1)
    logprob = jnp.zeros((1, 128), jnp.float32)
    for core in range(cores):
        top, total, chosen = merged(lines, place // groups % cores == core, owned)
        total = jnp.where(row < owned, total, 1.0)
        found = shifted(chosen, -2 * owned) - (top + jnp.log(total))
        logprob = jnp.where(row // owned == core, shifted(found, core * owned), logprob)
    values = jnp.broadcast_to(lines[:, 3 * owned : 3 * owned + 1], lines.shape)
    source = (lane % owned) * (count // groups // owned) + lane // owned
    here = place == source * groups + group_ref[0]
    value = jnp.sum(jnp.where(here, values, 0.0), axis=0, keepdims=True)
    logprob_ref[...] = logprob[:, : logprob_ref.shape[1]]
    value_ref[...] = value[:, : value_ref.shape[1]]


def final_values(stats, owned, cores, groups, group):
    rows = owned * cores
    return pl.pallas_call(
        functools.partial(final_kernel, owned, cores, groups),
        out_shape=(
            jax.ShapeDtypeStruct((1, rows), jnp.float32),
            jax.ShapeDtypeStruct((1, rows), jnp.float32),
        ),
        in_specs=[smem_spec(), vmem_spec()],
        out_specs=(vmem_spec(), vmem_spec()),
        compiler_params=room(2),
        name="final",
    )(group, stats)


def per_device(
    queries,
    keys_new,
    values_new,
    out_gate,
    decay_logit,
    beta_logit,
    decay_rate,
    state,
    norm_gain,
    out_proj,
    residual,
    final_gain,
    value_weight,
    lm_head,
    sampled,
):
    chips, cores = lax.axis_size("heads_0"), lax.axis_size("heads_1")
    groups = lax.axis_size(GROUP)
    chip, core = lax.axis_index("heads_0"), lax.axis_index("heads_1")
    side = lax.axis_index("z_side")
    rows_own, width = residual.shape
    rows_core = rows_own // cores
    copies = chips // rows_core
    lanes = 128
    lines = width // lanes

    z_head = lax.ppermute(lm_head, "z_side", SWAP)
    core_head = lax.ppermute(lm_head, "heads_1", SWAP)
    both_head = lax.ppermute(z_head, "heads_1", SWAP)

    first = jnp.where((chip == 0) & (core == 0), 1.0, 0.0).reshape(1)
    partial_out = head_partials(
        queries,
        keys_new,
        values_new,
        out_gate,
        decay_logit,
        beta_logit,
        decay_rate,
        state,
        norm_gain,
        out_proj,
        residual,
        first,
        chips * cores,
    )
    arrived = exchange(partial_out, HEADS)
    gain = final_gain.reshape(lines, lanes)
    weight = value_weight.reshape(lines, lanes)
    half_here = (chip % copies).astype(jnp.int32).reshape(1)
    pieces, value = norm_pieces(arrived, gain, weight, half_here, chips * groups, lines // copies)
    all_rows = exchange(pieces, GATHER)
    all_rows = all_rows.reshape(chips, groups, lines // copies, lanes)

    vocab_own = lm_head.shape[1]
    flat = lax.axis_index(HEADS_BATCH)
    across = (1 - 2 * core) * lax.axis_size(BATCH)
    along = (1 - 2 * side) * lax.axis_size("x")
    matrices = (lm_head, core_head, z_head, both_head)
    firsts = jnp.stack([flat, flat + across, flat + along, flat + across + along]) * vocab_own
    ids = sampled.reshape(-1, lax.axis_size("z_side"), lax.axis_size("x"), cores, rows_core)
    ids = lax.dynamic_index_in_dim(ids, side, 1, keepdims=False)
    ids = lax.dynamic_index_in_dim(ids, core, 2, keepdims=False)
    ids = ids.reshape(groups, rows_core).T.reshape(-1, 1)
    stats = logit_stats(all_rows, matrices, firsts.astype(jnp.int32), ids, value, chips * cores)
    group = lax.axis_index(GROUP).astype(jnp.int32).reshape(1)
    logprob, values = final_values(exchange(stats, ROWS), rows_core, cores, groups, group)
    return (logprob.reshape(-1), values.reshape(-1))


def solution(mesh):
    torus = Mesh(
        mesh.devices.reshape(8, 2, 4, 2, 4), ("heads_0", "heads_1", "z_pair", "z_side", "x")
    )
    return jax.shard_map(
        per_device,
        mesh=torus,
        in_specs=(
            P(BATCH, HEADS),
            P(BATCH, HEADS),
            P(BATCH, HEADS),
            P(BATCH, HEADS),
            P(BATCH, HEADS),
            P(BATCH, HEADS),
            P(HEADS),
            P(BATCH, HEADS, None, None),
            P(),
            P(HEADS, None),
            P(BATCH, None),
            P(),
            P(),
            P(None, HEADS_BATCH),
            P(),
        ),
        out_specs=(P(BATCH), P(BATCH)),
        check_vma=False,
    )
```

```python
import functools

import jax
import jax.numpy as jnp
from jax import lax
from jax.experimental import pallas as pl
from jax.experimental.pallas import tpu as pltpu
from jax.sharding import Mesh
from jax.sharding import PartitionSpec as P


HEADS = ("heads_0", "heads_1")
BATCH = ("z_pair", "z_side", "x")
GROUP = ("x", "z_pair")
NEAR = ("z_pair", "heads_0")
HEADS_BATCH = ("heads_0", "heads_1", "z_pair", "z_side", "x")
SWAP = [(0, 1), (1, 0)]


epsilon = 1e-06


def exchange(parts, axis):
    return lax.all_to_all(parts, axis, split_axis=0, concat_axis=0, tiled=True)


def any_spec():
    return pl.BlockSpec(memory_space=pltpu.HBM)


def room(mebibytes):
    return pltpu.CompilerParams(vmem_limit_bytes=mebibytes * 2**20)


def vmem_spec():
    return pl.BlockSpec(memory_space=pltpu.VMEM)


def smem_spec():
    return pl.BlockSpec(memory_space=pltpu.SMEM)


def as_column(line):
    size = line.shape[1]
    shape = (size, size)
    here = lax.broadcasted_iota(jnp.int32, shape, 0) == lax.broadcasted_iota(jnp.int32, shape, 1)
    return jnp.sum(jnp.where(here, jnp.broadcast_to(line, shape), 0.0), axis=1, keepdims=True)


def heads_kernel(
    first_ref,
    rate_ref,
    *refs,
):
    inputs, out_ref, local, sems = refs[:10], refs[10], refs[11:21], refs[21]
    q_ref, k_ref, v_ref, g_ref, dl_ref, bl_ref, gain_ref, res_ref, state_ref, proj_ref = local
    copies = [pltpu.make_async_copy(inputs[n], local[n], sems.at[n]) for n in range(8)]
    heads = state_ref.shape[1]
    for h in range(heads):
        copies.append(
            pltpu.make_async_copy(inputs[8].at[:, h], state_ref.at[:, h], sems.at[8 + h])
        )
    blocks = 4
    wide = proj_ref.shape[1] // blocks
    for n in range(blocks):
        part = pl.ds(n * wide, wide)
        copies.append(
            pltpu.make_async_copy(
                inputs[9].at[:, part], proj_ref.at[:, part], sems.at[8 + heads + n]
            )
        )
    for copy in copies:
        copy.start()
    for copy in copies[:8]:
        copy.wait()
    rows = q_ref.shape[0]
    size = state_ref.shape[2]
    gain = gain_ref[...]
    queries, keys = [], []
    for h in range(heads):
        lanes = slice(h * size, (h + 1) * size)
        query = q_ref[:, lanes].astype(jnp.float32)
        key = k_ref[:, lanes].astype(jnp.float32)
        query = query / jnp.sqrt(jnp.sum(query * query, axis=1, keepdims=True) + epsilon)
        queries.append(query * size ** (-0.5))
        keys.append(key / jnp.sqrt(jnp.sum(key * key, axis=1, keepdims=True) + epsilon))
    turned = jnp.concatenate(queries + keys, axis=0).T
    parts = []
    for h in range(heads):
        lanes = slice(h * size, (h + 1) * size)
        logit = dl_ref[h : h + 1, :]
        soft = jnp.maximum(logit, 0.0) + jnp.log1p(jnp.exp(-jnp.abs(logit)))
        decay = as_column(jnp.exp(-rate_ref[h] * soft))
        strength = as_column(1.0 / (1.0 + jnp.exp(-bl_ref[h : h + 1, :])))
        inter = jnp.sum(queries[h] * keys[h], axis=1, keepdims=True)
        value = v_ref[:, lanes].astype(jnp.float32)
        gate = g_ref[:, lanes].astype(jnp.float32)
        copies[8 + h].wait()
        by_query, by_key = [], []
        for b in range(rows):
            block = state_ref[b, h]
            at = h * rows + b
            by_query.append(jnp.sum(turned[:, at : at + 1] * block, axis=0, keepdims=True))
            at += heads * rows
            by_key.append(jnp.sum(turned[:, at : at + 1] * block, axis=0, keepdims=True))
        state_query = jnp.concatenate(by_query, axis=0)
        state_key = jnp.concatenate(by_key, axis=0)
        written = value - decay * state_key
        output = decay * state_query + strength * inter * written
        mean = jnp.mean(output * output, axis=1, keepdims=True)
        normed = output / jnp.sqrt(mean + epsilon)
        parts.append(normed * gain * (gate / (1.0 + jnp.exp(-gate))))
    headout = jnp.concatenate(parts, axis=1).astype(jnp.bfloat16)
    first = first_ref[0]
    lines = wide // 128
    cores, halves = 2, out_ref.shape[0] // rows
    for n in range(blocks):
        copies[8 + heads + n].wait()
        part = slice(n * wide, (n + 1) * wide)
        total = jnp.dot(headout, proj_ref[:, part], preferred_element_type=jnp.float32)
        total = total + res_ref[:, part].astype(jnp.float32) * first
        total = total.reshape(rows, lines, 128)
        for row in range(rows):
            for half in range(halves):
                core, r = row // (rows // cores), row % (rows // cores)
                place = (r * halves + half) * cores + core
                out_ref[place, n * lines : (n + 1) * lines, :] = total[row]


def head_partials(
    queries,
    keys_new,
    values_new,
    out_gate,
    decay_logit,
    beta_logit,
    decay_rate,
    state,
    norm_gain,
    out_proj,
    residual,
    first,
    places,
):
    arrays = (
        queries,
        keys_new,
        values_new,
        out_gate,
        decay_logit.T,
        beta_logit.T,
        norm_gain.reshape(1, -1),
        residual,
        state,
        out_proj,
    )
    width = out_proj.shape[1]
    return pl.pallas_call(
        heads_kernel,
        out_shape=pltpu.VMEM((places, width // 128, 128), jnp.float32),
        in_specs=[smem_spec(), smem_spec()] + [any_spec() for _ in arrays],
        out_specs=vmem_spec(),
        scratch_shapes=[pltpu.VMEM(a.shape, a.dtype) for a in arrays]
        + [pltpu.SemaphoreType.DMA((8 + state.shape[1] + 4,))],
        cost_estimate=pl.CostEstimate(flops=40000000, bytes_accessed=3500000, transcendentals=0),
        name="heads",
    )(first, decay_rate, *arrays)


def norm_kernel(half_ref, arrived_ref, gain_ref, weight_ref, piece_ref, value_ref, scratch):
    width = gain_ref.size
    hsum = arrived_ref[0]
    for n in range(1, arrived_ref.shape[0]):
        hsum = hsum + arrived_ref[n]
    gain = gain_ref[...]
    squares = jnp.sum(hsum * hsum, axis=(0, 1), keepdims=True)
    terms = jnp.sum(hsum * gain * weight_ref[...], axis=(0, 1), keepdims=True)
    rstd = 1.0 / jnp.sqrt(squares / width + epsilon)
    scratch[...] = hsum * rstd * gain
    lines = piece_ref.shape[1]
    start = pl.multiple_of(half_ref[0] * lines, lines)
    piece = scratch[pl.ds(start, lines), :].astype(jnp.bfloat16)
    for n in range(piece_ref.shape[0]):
        piece_ref[n] = piece
    value_ref[...] = jnp.broadcast_to(rstd * terms, value_ref.shape)


def norm_pieces(arrived, gain, weight, half, copies, lines):
    return pl.pallas_call(
        norm_kernel,
        out_shape=(
            pltpu.VMEM((copies, lines, 128), jnp.bfloat16),
            pltpu.VMEM((1, 128), jnp.float32),
        ),
        in_specs=[smem_spec(), vmem_spec(), vmem_spec(), vmem_spec()],
        out_specs=(vmem_spec(), vmem_spec()),
        scratch_shapes=[pltpu.VMEM(gain.shape, jnp.float32)],
        cost_estimate=pl.CostEstimate(flops=4000000, bytes_accessed=400000, transcendentals=0),
        compiler_params=room(4),
        name="norm",
    )(half, arrived, gain, weight)


def logits_kernel(firsts_ref, rows_ref, ids_ref, *refs):
    count = 4
    matrices, out_ref, local, flat, sems = refs[:count], *refs[count:]
    groups, pieces, tiles, lanes = rows_ref.shape
    deep = tiles * lanes
    halves = local.shape[1] // deep
    copies = []
    for k in range(halves):
        part = pl.ds(k * deep, deep)
        for n in range(count):
            at = k * count + n
            copies.append(
                pltpu.make_async_copy(
                    matrices[n].at[part], local.at[n, part], sems.at[at]
                )
            )
    for copy in copies:
        copy.start()
    flat[...] = rows_ref[...].reshape(flat.shape).astype(jnp.float32)

    def rows_of(piece):
        first, step = piece * tiles, pieces * tiles
        return jnp.concatenate(
            [flat[pl.ds(first + t, groups, stride=step), :] for t in range(tiles)], axis=1
        ).astype(jnp.bfloat16)

    sums = [None] * count
    for k in range(halves):
        part = slice(k * deep, (k + 1) * deep)
        lhs = jnp.concatenate([rows_of(p) for p in range(k, pieces, halves)], axis=0)
        for n in range(count):
            copies[k * count + n].wait()
            term = jnp.dot(lhs, local[n, part], preferred_element_type=jnp.float32)
            sums[n] = term if k == 0 else sums[n] + term
    top = sums[0]
    for n in range(1, count):
        top = jnp.maximum(top, sums[n])
    top = jnp.max(top, axis=1, keepdims=True)
    ids = ids_ref[...]
    total = jnp.zeros(sums[0].shape, jnp.float32)
    chosen = jnp.zeros(sums[0].shape, jnp.float32)
    for n in range(count):
        total = total + jnp.exp(sums[n] - top)
        columns = lax.broadcasted_iota(jnp.int32, sums[n].shape, 1) + firsts_ref[n]
        chosen = chosen + jnp.where(columns == ids, sums[n], 0.0)
    total = jnp.sum(total, axis=1, keepdims=True)
    chosen = jnp.sum(chosen, axis=1, keepdims=True)
    lane = lax.broadcasted_iota(jnp.int32, (groups, 128), 1)
    packed = jnp.zeros((groups, 128), jnp.float32)
    owned = pieces // halves
    for n, column in enumerate((top, total, chosen)):
        for r in range(owned):
            part = column[r * groups : (r + 1) * groups]
            packed = jnp.where(lane == n * owned + r, part, packed)
    for g in range(groups):
        out_ref[g] = packed[g : g + 1]


def logit_stats(all_rows, matrices, firsts, ids):
    groups = all_rows.shape[0]
    depth = matrices[0].shape[0]
    return pl.pallas_call(
        logits_kernel,
        out_shape=pltpu.VMEM((groups, 1, 128), jnp.float32),
        in_specs=[smem_spec(), vmem_spec(), vmem_spec()] + [any_spec() for _ in matrices],
        out_specs=vmem_spec(),
        scratch_shapes=[
            pltpu.VMEM((len(matrices), depth, 128), jnp.bfloat16),
            pltpu.VMEM((all_rows.size // 128, 128), jnp.float32),
            pltpu.SemaphoreType.DMA((2 * len(matrices),)),
        ],
        cost_estimate=pl.CostEstimate(flops=270000000, bytes_accessed=4700000, transcendentals=0),
        compiler_params=room(12),
        name="logits",
    )(firsts, all_rows, ids, *matrices)


def shifted(lines, places):
    return pltpu.roll(lines, places % 128, 1)


def merged(lines, keep, owned):
    low = jnp.min(lines, axis=0, keepdims=True)
    top = jnp.max(jnp.where(keep, lines, low), axis=0, keepdims=True)
    weight = jnp.where(keep, jnp.exp(jnp.minimum(lines - top, 0.0)), 0.0)
    total = jnp.sum(shifted(lines, -owned) * weight, axis=0, keepdims=True)
    chosen = jnp.sum(jnp.where(keep, lines, 0.0), axis=0, keepdims=True)
    return top, total, chosen


def group_kernel(owned, stats_ref, value_ref, out_ref):
    lines = stats_ref[...].reshape(stats_ref.shape[0], 128)
    top, total, chosen = merged(lines, jnp.full(lines.shape, True), owned)
    lane = lax.broadcasted_iota(jnp.int32, (1, 128), 1)
    packed = jnp.where(lane < owned, top, shifted(total, owned))
    packed = jnp.where(lane < 2 * owned, packed, chosen)
    packed = jnp.where(lane < 3 * owned, packed, value_ref[...])
    for n in range(out_ref.shape[0]):
        out_ref[n] = packed


def group_stats(stats, value, owned, copies):
    return pl.pallas_call(
        functools.partial(group_kernel, owned),
        out_shape=pltpu.VMEM((copies, 1, 128), jnp.float32),
        in_specs=[vmem_spec(), vmem_spec()],
        out_specs=vmem_spec(),
        compiler_params=room(2),
        name="group",
    )(stats, value)


def final_kernel(owned, cores, stats_ref, logprob_ref, value_ref):
    count = stats_ref.shape[0]
    lines = stats_ref[...].reshape(count, 128)
    place = lax.broadcasted_iota(jnp.int32, lines.shape, 0)
    lane = lax.broadcasted_iota(jnp.int32, lines.shape, 1)
    row = lax.broadcasted_iota(jnp.int32, (1, 128), 1)
    logprob = jnp.zeros((1, 128), jnp.float32)
    for core in range(cores):
        top, total, chosen = merged(lines, place % cores == core, owned)
        total = jnp.where(row < owned, total, 1.0)
        found = shifted(chosen, -2 * owned) - (top + jnp.log(total))
        logprob = jnp.where(row // owned == core, shifted(found, core * owned), logprob)
    values = jnp.broadcast_to(lines[:, 3 * owned : 3 * owned + 1], lines.shape)
    here = place == (lane % owned) * (count // owned) + lane // owned
    value = jnp.sum(jnp.where(here, values, 0.0), axis=0, keepdims=True)
    logprob_ref[...] = logprob[:, : logprob_ref.shape[1]]
    value_ref[...] = value[:, : value_ref.shape[1]]


def final_values(stats, owned, cores):
    rows = owned * cores
    return pl.pallas_call(
        functools.partial(final_kernel, owned, cores),
        out_shape=(
            jax.ShapeDtypeStruct((1, rows), jnp.float32),
            jax.ShapeDtypeStruct((1, rows), jnp.float32),
        ),
        in_specs=[vmem_spec()],
        out_specs=(vmem_spec(), vmem_spec()),
        compiler_params=room(2),
        name="final",
    )(stats)


def per_device(
    queries,
    keys_new,
    values_new,
    out_gate,
    decay_logit,
    beta_logit,
    decay_rate,
    state,
    norm_gain,
    out_proj,
    residual,
    final_gain,
    value_weight,
    lm_head,
    sampled,
):
    chips, cores = lax.axis_size("heads_0"), lax.axis_size("heads_1")
    groups = lax.axis_size(GROUP)
    chip, core = lax.axis_index("heads_0"), lax.axis_index("heads_1")
    side = lax.axis_index("z_side")
    rows_own, width = residual.shape
    rows_core = rows_own // cores
    copies = chips // rows_core
    lanes = 128
    lines = width // lanes

    z_head = lax.ppermute(lm_head, "z_side", SWAP)
    core_head = lax.ppermute(lm_head, "heads_1", SWAP)
    both_head = lax.ppermute(z_head, "heads_1", SWAP)

    first = jnp.where((chip == 0) & (core == 0), 1.0, 0.0).reshape(1)
    partial_out = head_partials(
        queries,
        keys_new,
        values_new,
        out_gate,
        decay_logit,
        beta_logit,
        decay_rate,
        state,
        norm_gain,
        out_proj,
        residual,
        first,
        chips * cores,
    )
    arrived = exchange(partial_out, HEADS)
    gain = final_gain.reshape(lines, lanes)
    weight = value_weight.reshape(lines, lanes)
    half_here = (chip % copies).astype(jnp.int32).reshape(1)
    near = lax.axis_size(NEAR)
    pieces, value = norm_pieces(arrived, gain, weight, half_here, near, lines // copies)
    near_rows = exchange(pieces, NEAR)
    far = lax.axis_size("x")
    all_rows = exchange(jnp.broadcast_to(near_rows[None], (far, *near_rows.shape)), "x")
    all_rows = all_rows.reshape(groups, chips, lines // copies, lanes)

    vocab_own = lm_head.shape[1]
    flat = lax.axis_index(HEADS_BATCH)
    across = (1 - 2 * core) * lax.axis_size(BATCH)
    along = (1 - 2 * side) * lax.axis_size("x")
    matrices = (lm_head, core_head, z_head, both_head)
    firsts = jnp.stack([flat, flat + across, flat + along, flat + across + along]) * vocab_own
    ids = sampled.reshape(-1, lax.axis_size("z_side"), lax.axis_size("x"), cores, rows_core)
    ids = lax.dynamic_index_in_dim(ids, side, 1, keepdims=False)
    ids = lax.dynamic_index_in_dim(ids, core, 2, keepdims=False)
    ids = ids.transpose(2, 1, 0).reshape(-1, 1)
    stats = logit_stats(all_rows, matrices, firsts.astype(jnp.int32), ids)
    stats = group_stats(exchange(stats, GROUP), value, rows_core, chips * cores)
    logprob, values = final_values(exchange(stats, HEADS), rows_core, cores)
    return (logprob.reshape(-1), values.reshape(-1))


def solution(mesh):
    torus = Mesh(
        mesh.devices.reshape(8, 2, 4, 2, 4), ("heads_0", "heads_1", "z_pair", "z_side", "x")
    )
    return jax.shard_map(
        per_device,
        mesh=torus,
        in_specs=(
            P(BATCH, HEADS),
            P(BATCH, HEADS),
            P(BATCH, HEADS),
            P(BATCH, HEADS),
            P(BATCH, HEADS),
            P(BATCH, HEADS),
            P(HEADS),
            P(BATCH, HEADS, None, None),
            P(),
            P(HEADS, None),
            P(BATCH, None),
            P(),
            P(),
            P(None, HEADS_BATCH),
            P(),
        ),
        out_specs=(P(BATCH), P(BATCH)),
        check_vma=False,
    )
```

```python
import functools

import jax
import jax.numpy as jnp
from jax import lax
from jax.experimental import pallas as pl
from jax.experimental.pallas import tpu as pltpu
from jax.sharding import Mesh
from jax.sharding import PartitionSpec as P


HEADS = ("heads_0", "heads_1")
BATCH = ("z", "x_pair", "x_side")
GROUP = ("x_pair", "z")
NEAR = ("z", "heads_0")
HEADS_BATCH = ("heads_0", "heads_1", "z", "x_pair", "x_side")
SWAP = [(0, 1), (1, 0)]


epsilon = 1e-06


def exchange(parts, axis):
    return lax.all_to_all(parts, axis, split_axis=0, concat_axis=0, tiled=True)


def any_spec():
    return pl.BlockSpec(memory_space=pltpu.HBM)


def room(mebibytes):
    return pltpu.CompilerParams(vmem_limit_bytes=mebibytes * 2**20)


def vmem_spec():
    return pl.BlockSpec(memory_space=pltpu.VMEM)


def smem_spec():
    return pl.BlockSpec(memory_space=pltpu.SMEM)


def as_column(line):
    size = line.shape[1]
    shape = (size, size)
    here = lax.broadcasted_iota(jnp.int32, shape, 0) == lax.broadcasted_iota(jnp.int32, shape, 1)
    return jnp.sum(jnp.where(here, jnp.broadcast_to(line, shape), 0.0), axis=1, keepdims=True)


def heads_kernel(
    first_ref,
    rate_ref,
    *refs,
):
    inputs, out_ref, local, sems = refs[:10], refs[10], refs[11:21], refs[21]
    q_ref, k_ref, v_ref, g_ref, dl_ref, bl_ref, gain_ref, res_ref, state_ref, proj_ref = local
    copies = [pltpu.make_async_copy(inputs[n], local[n], sems.at[n]) for n in range(8)]
    heads = state_ref.shape[1]
    for h in range(heads):
        copies.append(
            pltpu.make_async_copy(inputs[8].at[:, h], state_ref.at[:, h], sems.at[8 + h])
        )
    blocks = 4
    wide = proj_ref.shape[1] // blocks
    for n in range(blocks):
        part = pl.ds(n * wide, wide)
        copies.append(
            pltpu.make_async_copy(
                inputs[9].at[:, part], proj_ref.at[:, part], sems.at[8 + heads + n]
            )
        )
    for copy in copies:
        copy.start()
    for copy in copies[:8]:
        copy.wait()
    rows = q_ref.shape[0]
    size = state_ref.shape[2]
    gain = gain_ref[...]
    queries, keys = [], []
    for h in range(heads):
        lanes = slice(h * size, (h + 1) * size)
        query = q_ref[:, lanes].astype(jnp.float32)
        key = k_ref[:, lanes].astype(jnp.float32)
        query = query / jnp.sqrt(jnp.sum(query * query, axis=1, keepdims=True) + epsilon)
        queries.append(query * size ** (-0.5))
        keys.append(key / jnp.sqrt(jnp.sum(key * key, axis=1, keepdims=True) + epsilon))
    turned = jnp.concatenate(queries + keys, axis=0).T
    parts = []
    for h in range(heads):
        lanes = slice(h * size, (h + 1) * size)
        logit = dl_ref[h : h + 1, :]
        soft = jnp.maximum(logit, 0.0) + jnp.log1p(jnp.exp(-jnp.abs(logit)))
        decay = as_column(jnp.exp(-rate_ref[h] * soft))
        strength = as_column(1.0 / (1.0 + jnp.exp(-bl_ref[h : h + 1, :])))
        inter = jnp.sum(queries[h] * keys[h], axis=1, keepdims=True)
        value = v_ref[:, lanes].astype(jnp.float32)
        gate = g_ref[:, lanes].astype(jnp.float32)
        copies[8 + h].wait()
        by_query, by_key = [], []
        for b in range(rows):
            block = state_ref[b, h]
            at = h * rows + b
            by_query.append(jnp.sum(turned[:, at : at + 1] * block, axis=0, keepdims=True))
            at += heads * rows
            by_key.append(jnp.sum(turned[:, at : at + 1] * block, axis=0, keepdims=True))
        state_query = jnp.concatenate(by_query, axis=0)
        state_key = jnp.concatenate(by_key, axis=0)
        written = value - decay * state_key
        output = decay * state_query + strength * inter * written
        mean = jnp.mean(output * output, axis=1, keepdims=True)
        normed = output / jnp.sqrt(mean + epsilon)
        parts.append(normed * gain * (gate / (1.0 + jnp.exp(-gate))))
    headout = jnp.concatenate(parts, axis=1).astype(jnp.bfloat16)
    first = first_ref[0]
    lines = wide // 128
    cores, halves = 2, out_ref.shape[0] // rows
    for n in range(blocks):
        copies[8 + heads + n].wait()
        part = slice(n * wide, (n + 1) * wide)
        total = jnp.dot(headout, proj_ref[:, part], preferred_element_type=jnp.float32)
        total = total + res_ref[:, part].astype(jnp.float32) * first
        total = total.reshape(rows, lines, 128)
        for row in range(rows):
            for half in range(halves):
                core, r = row // (rows // cores), row % (rows // cores)
                place = (r * halves + half) * cores + core
                out_ref[place, n * lines : (n + 1) * lines, :] = total[row]


def head_partials(
    queries,
    keys_new,
    values_new,
    out_gate,
    decay_logit,
    beta_logit,
    decay_rate,
    state,
    norm_gain,
    out_proj,
    residual,
    first,
    places,
):
    arrays = (
        queries,
        keys_new,
        values_new,
        out_gate,
        decay_logit.T,
        beta_logit.T,
        norm_gain.reshape(1, -1),
        residual,
        state,
        out_proj,
    )
    width = out_proj.shape[1]
    return pl.pallas_call(
        heads_kernel,
        out_shape=pltpu.VMEM((places, width // 128, 128), jnp.float32),
        in_specs=[smem_spec(), smem_spec()] + [any_spec() for _ in arrays],
        out_specs=vmem_spec(),
        scratch_shapes=[pltpu.VMEM(a.shape, a.dtype) for a in arrays]
        + [pltpu.SemaphoreType.DMA((8 + state.shape[1] + 4,))],
        cost_estimate=pl.CostEstimate(flops=40000000, bytes_accessed=3500000, transcendentals=0),
        name="heads",
    )(first, decay_rate, *arrays)


def norm_kernel(half_ref, arrived_ref, gain_ref, weight_ref, piece_ref, value_ref, scratch):
    width = gain_ref.size
    hsum = arrived_ref[0]
    for n in range(1, arrived_ref.shape[0]):
        hsum = hsum + arrived_ref[n]
    gain = gain_ref[...]
    squares = jnp.sum(hsum * hsum, axis=(0, 1), keepdims=True)
    terms = jnp.sum(hsum * gain * weight_ref[...], axis=(0, 1), keepdims=True)
    rstd = 1.0 / jnp.sqrt(squares / width + epsilon)
    scratch[...] = hsum * rstd * gain
    lines = piece_ref.shape[1]
    start = pl.multiple_of(half_ref[0] * lines, lines)
    piece = scratch[pl.ds(start, lines), :].astype(jnp.bfloat16)
    for n in range(piece_ref.shape[0]):
        piece_ref[n] = piece
    value_ref[...] = jnp.broadcast_to(rstd * terms, value_ref.shape)


def norm_pieces(arrived, gain, weight, half, copies, lines):
    return pl.pallas_call(
        norm_kernel,
        out_shape=(
            pltpu.VMEM((copies, lines, 128), jnp.bfloat16),
            pltpu.VMEM((1, 128), jnp.float32),
        ),
        in_specs=[smem_spec(), vmem_spec(), vmem_spec(), vmem_spec()],
        out_specs=(vmem_spec(), vmem_spec()),
        scratch_shapes=[pltpu.VMEM(gain.shape, jnp.float32)],
        cost_estimate=pl.CostEstimate(flops=4000000, bytes_accessed=400000, transcendentals=0),
        compiler_params=room(4),
        name="norm",
    )(half, arrived, gain, weight)


def logits_kernel(groups, firsts_ref, pair_ref, near_ref, far_ref, ids_ref, *refs):
    count = 4
    matrices, out_ref, local, flat, sems = refs[:count], *refs[count:]
    size, (_, tiles, lanes) = near_ref.shape[0] * near_ref.shape[1], near_ref.shape
    pieces = flat.shape[0] // (groups * tiles)
    deep = tiles * lanes
    halves = local.shape[1] // deep
    copies = []
    for k in range(halves):
        part = pl.ds(k * deep, deep)
        for n in range(count):
            at = k * count + n
            copies.append(
                pltpu.make_async_copy(
                    matrices[n].at[part], local.at[n, part], sems.at[at]
                )
            )
    for copy in copies:
        copy.start()
    for start, ref in ((pair_ref[0] * size, near_ref), ((1 - pair_ref[0]) * size, far_ref)):
        part = pl.ds(pl.multiple_of(start, size), size)
        flat[part, :] = ref[...].reshape(size, lanes).astype(jnp.float32)

    def rows_of(piece):
        first, step = piece * tiles, pieces * tiles
        return jnp.concatenate(
            [flat[pl.ds(first + t, groups, stride=step), :] for t in range(tiles)], axis=1
        ).astype(jnp.bfloat16)

    sums = [None] * count
    for k in range(halves):
        part = slice(k * deep, (k + 1) * deep)
        lhs = jnp.concatenate([rows_of(p) for p in range(k, pieces, halves)], axis=0)
        for n in range(count):
            copies[k * count + n].wait()
            term = jnp.dot(lhs, local[n, part], preferred_element_type=jnp.float32)
            sums[n] = term if k == 0 else sums[n] + term
    top = sums[0]
    for n in range(1, count):
        top = jnp.maximum(top, sums[n])
    top = jnp.max(top, axis=1, keepdims=True)
    ids = ids_ref[...]
    total = jnp.zeros(sums[0].shape, jnp.float32)
    chosen = jnp.zeros(sums[0].shape, jnp.float32)
    for n in range(count):
        total = total + jnp.exp(sums[n] - top)
        columns = lax.broadcasted_iota(jnp.int32, sums[n].shape, 1) + firsts_ref[n]
        chosen = chosen + jnp.where(columns == ids, sums[n], 0.0)
    total = jnp.sum(total, axis=1, keepdims=True)
    chosen = jnp.sum(chosen, axis=1, keepdims=True)
    lane = lax.broadcasted_iota(jnp.int32, (groups, 128), 1)
    packed = jnp.zeros((groups, 128), jnp.float32)
    owned = pieces // halves
    for n, column in enumerate((top, total, chosen)):
        for r in range(owned):
            part = column[r * groups : (r + 1) * groups]
            packed = jnp.where(lane == n * owned + r, part, packed)
    for g in range(groups):
        out_ref[g] = packed[g : g + 1]


def logit_stats(near_rows, far_rows, pair, matrices, firsts, ids, groups):
    depth = matrices[0].shape[0]
    return pl.pallas_call(
        functools.partial(logits_kernel, groups),
        out_shape=pltpu.VMEM((groups, 1, 128), jnp.float32),
        in_specs=[smem_spec(), smem_spec(), vmem_spec(), vmem_spec(), vmem_spec()]
        + [any_spec() for _ in matrices],
        out_specs=vmem_spec(),
        scratch_shapes=[
            pltpu.VMEM((len(matrices), depth, 128), jnp.bfloat16),
            pltpu.VMEM((2 * near_rows.size // 128, 128), jnp.float32),
            pltpu.SemaphoreType.DMA((2 * len(matrices),)),
        ],
        cost_estimate=pl.CostEstimate(flops=270000000, bytes_accessed=4700000, transcendentals=0),
        compiler_params=room(12),
        name="logits",
    )(firsts, pair, near_rows, far_rows, ids, *matrices)


def shifted(lines, places):
    return pltpu.roll(lines, places % 128, 1)


def merged(lines, keep, owned):
    low = jnp.min(lines, axis=0, keepdims=True)
    top = jnp.max(jnp.where(keep, lines, low), axis=0, keepdims=True)
    weight = jnp.where(keep, jnp.exp(jnp.minimum(lines - top, 0.0)), 0.0)
    total = jnp.sum(shifted(lines, -owned) * weight, axis=0, keepdims=True)
    chosen = jnp.sum(jnp.where(keep, lines, 0.0), axis=0, keepdims=True)
    return top, total, chosen


def group_kernel(owned, stats_ref, value_ref, out_ref):
    lines = stats_ref[...].reshape(stats_ref.shape[0], 128)
    top, total, chosen = merged(lines, jnp.full(lines.shape, True), owned)
    lane = lax.broadcasted_iota(jnp.int32, (1, 128), 1)
    packed = jnp.where(lane < owned, top, shifted(total, owned))
    packed = jnp.where(lane < 2 * owned, packed, chosen)
    packed = jnp.where(lane < 3 * owned, packed, value_ref[...])
    for n in range(out_ref.shape[0]):
        out_ref[n] = packed


def group_stats(stats, value, owned, copies):
    return pl.pallas_call(
        functools.partial(group_kernel, owned),
        out_shape=pltpu.VMEM((copies, 1, 128), jnp.float32),
        in_specs=[vmem_spec(), vmem_spec()],
        out_specs=vmem_spec(),
        compiler_params=room(2),
        name="group",
    )(stats, value)


def final_kernel(owned, cores, stats_ref, logprob_ref, value_ref):
    count = stats_ref.shape[0]
    lines = stats_ref[...].reshape(count, 128)
    place = lax.broadcasted_iota(jnp.int32, lines.shape, 0)
    lane = lax.broadcasted_iota(jnp.int32, lines.shape, 1)
    row = lax.broadcasted_iota(jnp.int32, (1, 128), 1)
    logprob = jnp.zeros((1, 128), jnp.float32)
    for core in range(cores):
        top, total, chosen = merged(lines, place % cores == core, owned)
        total = jnp.where(row < owned, total, 1.0)
        found = shifted(chosen, -2 * owned) - (top + jnp.log(total))
        logprob = jnp.where(row // owned == core, shifted(found, core * owned), logprob)
    values = jnp.broadcast_to(lines[:, 3 * owned : 3 * owned + 1], lines.shape)
    here = place == (lane % owned) * (count // owned) + lane // owned
    value = jnp.sum(jnp.where(here, values, 0.0), axis=0, keepdims=True)
    logprob_ref[...] = logprob[:, : logprob_ref.shape[1]]
    value_ref[...] = value[:, : value_ref.shape[1]]


def final_values(stats, owned, cores):
    rows = owned * cores
    return pl.pallas_call(
        functools.partial(final_kernel, owned, cores),
        out_shape=(
            jax.ShapeDtypeStruct((1, rows), jnp.float32),
            jax.ShapeDtypeStruct((1, rows), jnp.float32),
        ),
        in_specs=[vmem_spec()],
        out_specs=(vmem_spec(), vmem_spec()),
        compiler_params=room(2),
        name="final",
    )(stats)


def per_device(
    queries,
    keys_new,
    values_new,
    out_gate,
    decay_logit,
    beta_logit,
    decay_rate,
    state,
    norm_gain,
    out_proj,
    residual,
    final_gain,
    value_weight,
    lm_head,
    sampled,
):
    chips, cores = lax.axis_size("heads_0"), lax.axis_size("heads_1")
    groups = lax.axis_size(GROUP)
    chip, core = lax.axis_index("heads_0"), lax.axis_index("heads_1")
    side = lax.axis_index("x_side")
    rows_own, width = residual.shape
    rows_core = rows_own // cores
    copies = chips // rows_core
    lanes = 128
    lines = width // lanes

    x_head = lax.ppermute(lm_head, "x_side", SWAP)
    core_head = lax.ppermute(lm_head, "heads_1", SWAP)
    both_head = lax.ppermute(x_head, "heads_1", SWAP)
    first = jnp.where((chip == 0) & (core == 0), 1.0, 0.0).reshape(1)
    partial_out = head_partials(
        queries,
        keys_new,
        values_new,
        out_gate,
        decay_logit,
        beta_logit,
        decay_rate,
        state,
        norm_gain,
        out_proj,
        residual,
        first,
        chips * cores,
    )
    arrived = exchange(partial_out, HEADS)
    gain = final_gain.reshape(lines, lanes)
    weight = value_weight.reshape(lines, lanes)
    half_here = (chip % copies).astype(jnp.int32).reshape(1)
    near = lax.axis_size(NEAR)
    pieces, value = norm_pieces(arrived, gain, weight, half_here, near, lines // copies)
    near_rows = exchange(pieces, NEAR)
    far_rows = lax.ppermute(near_rows, "x_pair", SWAP)

    vocab_own = lm_head.shape[1]
    flat = lax.axis_index(HEADS_BATCH)
    across = (1 - 2 * core) * lax.axis_size(BATCH)
    along = 1 - 2 * side
    matrices = (lm_head, core_head, x_head, both_head)
    firsts = jnp.stack([flat, flat + across, flat + along, flat + across + along]) * vocab_own
    pair = lax.axis_index("x_pair").astype(jnp.int32).reshape(1)
    ids = sampled.reshape(lax.axis_size("z"), lax.axis_size("x_pair"), -1, cores, rows_core)
    ids = lax.dynamic_index_in_dim(ids, side, 2, keepdims=False)
    ids = lax.dynamic_index_in_dim(ids, core, 2, keepdims=False)
    ids = ids.transpose(2, 1, 0).reshape(-1, 1)
    stats = logit_stats(near_rows, far_rows, pair, matrices, firsts.astype(jnp.int32), ids, groups)
    stats = group_stats(exchange(stats, GROUP), value, rows_core, chips * cores)
    logprob, values = final_values(exchange(stats, HEADS), rows_core, cores)
    return (logprob.reshape(-1), values.reshape(-1))


def solution(mesh):
    torus = Mesh(
        mesh.devices.reshape(8, 2, 8, 2, 2), ("heads_0", "heads_1", "z", "x_pair", "x_side")
    )
    return jax.shard_map(
        per_device,
        mesh=torus,
        in_specs=(
            P(BATCH, HEADS),
            P(BATCH, HEADS),
            P(BATCH, HEADS),
            P(BATCH, HEADS),
            P(BATCH, HEADS),
            P(BATCH, HEADS),
            P(HEADS),
            P(BATCH, HEADS, None, None),
            P(),
            P(HEADS, None),
            P(BATCH, None),
            P(),
            P(),
            P(None, HEADS_BATCH),
            P(),
        ),
        out_specs=(P(BATCH), P(BATCH)),
        check_vma=False,
    )
```

```python
import functools

import jax
import jax.numpy as jnp
from jax import lax
from jax.experimental import pallas as pl
from jax.experimental.pallas import tpu as pltpu
from jax.sharding import Mesh
from jax.sharding import PartitionSpec as P


HEADS = ("heads_0", "heads_1")
BATCH = ("z", "x_pair", "x_side")
GROUP = ("x_pair", "z")
NEAR = ("z", "heads_0")
HEADS_BATCH = ("heads_0", "heads_1", "z", "x_pair", "x_side")
SWAP = [(0, 1), (1, 0)]


epsilon = 1e-06


def exchange(parts, axis):
    return lax.all_to_all(parts, axis, split_axis=0, concat_axis=0, tiled=True)


def any_spec():
    return pl.BlockSpec(memory_space=pltpu.HBM)


def room(mebibytes):
    return pltpu.CompilerParams(vmem_limit_bytes=mebibytes * 2**20)


def vmem_spec():
    return pl.BlockSpec(memory_space=pltpu.VMEM)


def smem_spec():
    return pl.BlockSpec(memory_space=pltpu.SMEM)


def as_column(line):
    size = line.shape[1]
    shape = (size, size)
    here = lax.broadcasted_iota(jnp.int32, shape, 0) == lax.broadcasted_iota(jnp.int32, shape, 1)
    return jnp.sum(jnp.where(here, jnp.broadcast_to(line, shape), 0.0), axis=1, keepdims=True)


def heads_kernel(*refs):
    small = 9
    inputs, out_ref, local = refs[:11], refs[11], refs[12:23]
    done_ref, sems, out_sems = refs[23:]
    q_ref, k_ref, v_ref, g_ref, dl_ref, bl_ref, gain_ref, rate_ref, res_ref = local[:small]
    state_ref, proj_ref = local[small:]
    copies = [pltpu.make_async_copy(inputs[n], local[n], sems.at[n]) for n in range(small)]
    heads = state_ref.shape[1]
    for h in range(heads):
        copies.append(
            pltpu.make_async_copy(
                inputs[small].at[:, h], state_ref.at[:, h], sems.at[small + h]
            )
        )
    blocks = 4
    wide = proj_ref.shape[1] // blocks
    for n in range(blocks):
        part = pl.ds(n * wide, wide)
        copies.append(
            pltpu.make_async_copy(
                inputs[small + 1].at[:, part], proj_ref.at[:, part], sems.at[small + heads + n]
            )
        )
    for copy in copies:
        copy.start()
    for copy in copies[:small]:
        copy.wait()
    rows = q_ref.shape[0]
    size = state_ref.shape[2]
    gain = gain_ref[...]
    queries, keys = [], []
    for h in range(heads):
        lanes = slice(h * size, (h + 1) * size)
        query = q_ref[:, lanes].astype(jnp.float32)
        key = k_ref[:, lanes].astype(jnp.float32)
        query = query / jnp.sqrt(jnp.sum(query * query, axis=1, keepdims=True) + epsilon)
        queries.append(query * size ** (-0.5))
        keys.append(key / jnp.sqrt(jnp.sum(key * key, axis=1, keepdims=True) + epsilon))
    turned = jnp.concatenate(queries + keys, axis=0).T
    parts = []
    for h in range(heads):
        lanes = slice(h * size, (h + 1) * size)
        logit = dl_ref[h : h + 1, :]
        soft = jnp.maximum(logit, 0.0) + jnp.log1p(jnp.exp(-jnp.abs(logit)))
        decay = as_column(jnp.exp(-rate_ref[:, h : h + 1] * soft))
        strength = as_column(1.0 / (1.0 + jnp.exp(-bl_ref[h : h + 1, :])))
        inter = jnp.sum(queries[h] * keys[h], axis=1, keepdims=True)
        value = v_ref[:, lanes].astype(jnp.float32)
        gate = g_ref[:, lanes].astype(jnp.float32)
        copies[small + h].wait()
        by_query, by_key = [], []
        for b in range(rows):
            block = state_ref[b, h]
            at = h * rows + b
            by_query.append(jnp.sum(turned[:, at : at + 1] * block, axis=0, keepdims=True))
            at += heads * rows
            by_key.append(jnp.sum(turned[:, at : at + 1] * block, axis=0, keepdims=True))
        state_query = jnp.concatenate(by_query, axis=0)
        state_key = jnp.concatenate(by_key, axis=0)
        written = value - decay * state_key
        output = decay * state_query + strength * inter * written
        mean = jnp.mean(output * output, axis=1, keepdims=True)
        normed = output / jnp.sqrt(mean + epsilon)
        parts.append(normed * gain * (gate / (1.0 + jnp.exp(-gate))))
    headout = jnp.concatenate(parts, axis=1).astype(jnp.bfloat16)
    chip, core = lax.axis_index("heads_0"), lax.axis_index("heads_1")
    first = jnp.where((chip == 0) & (core == 0), 1.0, 0.0)
    finished = []
    lines = wide // 128
    cores, halves = 2, out_ref.shape[0] // rows
    for n in range(blocks):
        copies[small + heads + n].wait()
        part = slice(n * wide, (n + 1) * wide)
        total = jnp.dot(headout, proj_ref[:, part], preferred_element_type=jnp.float32)
        total = total + res_ref[:, part].astype(jnp.float32) * first
        total = total.reshape(rows, lines, 128)
        for row in range(rows):
            for half in range(halves):
                core, r = row // (rows // cores), row % (rows // cores)
                place = (r * halves + half) * cores + core
                done_ref[place, n * lines : (n + 1) * lines, :] = total[row]
        part = pl.ds(n * lines, lines)
        finished.append(
            pltpu.make_async_copy(done_ref.at[:, part], out_ref.at[:, part], out_sems.at[n])
        )
        finished[-1].start()
    for copy in finished:
        copy.wait()


def head_partials(
    queries,
    keys_new,
    values_new,
    out_gate,
    decay_logit,
    beta_logit,
    decay_rate,
    state,
    norm_gain,
    out_proj,
    residual,
    places,
):
    arrays = (
        queries,
        keys_new,
        values_new,
        out_gate,
        decay_logit.T,
        beta_logit.T,
        norm_gain.reshape(1, -1),
        decay_rate.reshape(1, -1),
        residual,
        state,
        out_proj,
    )
    width = out_proj.shape[1]
    return pl.pallas_call(
        heads_kernel,
        out_shape=jax.ShapeDtypeStruct((places, width // 128, 128), jnp.float32),
        in_specs=[any_spec() for _ in arrays],
        out_specs=any_spec(),
        scratch_shapes=[pltpu.VMEM(a.shape, a.dtype) for a in arrays]
        + [
            pltpu.VMEM((places, width // 128, 128), jnp.float32),
            pltpu.SemaphoreType.DMA((9 + state.shape[1] + 4,)),
            pltpu.SemaphoreType.DMA((4,)),
        ],
        cost_estimate=pl.CostEstimate(flops=40000000, bytes_accessed=3500000, transcendentals=0),
        name="heads",
    )(*arrays)


def norm_kernel(half_ref, arrived_ref, gain_ref, weight_ref, piece_ref, value_ref, scratch):
    width = gain_ref.size
    hsum = arrived_ref[0]
    for n in range(1, arrived_ref.shape[0]):
        hsum = hsum + arrived_ref[n]
    gain = gain_ref[...]
    squares = jnp.sum(hsum * hsum, axis=(0, 1), keepdims=True)
    terms = jnp.sum(hsum * gain * weight_ref[...], axis=(0, 1), keepdims=True)
    rstd = 1.0 / jnp.sqrt(squares / width + epsilon)
    scratch[...] = hsum * rstd * gain
    lines = piece_ref.shape[1]
    start = pl.multiple_of(half_ref[0] * lines, lines)
    piece = scratch[pl.ds(start, lines), :].astype(jnp.bfloat16)
    for n in range(piece_ref.shape[0]):
        piece_ref[n] = piece
    value_ref[...] = jnp.broadcast_to(rstd * terms, value_ref.shape)


def norm_pieces(arrived, gain, weight, half, copies, lines):
    return pl.pallas_call(
        norm_kernel,
        out_shape=(
            pltpu.VMEM((copies, lines, 128), jnp.bfloat16),
            pltpu.VMEM((1, 128), jnp.float32),
        ),
        in_specs=[smem_spec(), vmem_spec(), vmem_spec(), vmem_spec()],
        out_specs=(vmem_spec(), vmem_spec()),
        scratch_shapes=[pltpu.VMEM(gain.shape, jnp.float32)],
        cost_estimate=pl.CostEstimate(flops=4000000, bytes_accessed=400000, transcendentals=0),
        compiler_params=room(4),
        name="norm",
    )(half, arrived, gain, weight)


def logits_kernel(groups, near_ref, far_ref, ids_ref, *refs):
    count = 4
    matrices, out_ref, local, rows, flat, sems = refs[:count], *refs[count:]
    tiles, lanes = near_ref.shape[1:]
    pieces = flat.shape[0] // (groups * tiles)
    deep = tiles * lanes
    halves = local.shape[1] // deep
    pair, core, side = (lax.axis_index(a) for a in ("x_pair", "heads_1", "x_side"))
    flat_place = 0
    for axis in HEADS_BATCH:
        flat_place = flat_place * lax.axis_size(axis) + lax.axis_index(axis)
    across = (1 - 2 * core) * lax.axis_size(BATCH)
    along = 1 - 2 * side
    firsts = [(flat_place + step) * lanes for step in (0, across, along, across + along)]
    moved = [
        pltpu.make_async_copy(near_ref, rows.at[pair], sems.at[halves * count]),
        pltpu.make_async_copy(far_ref, rows.at[1 - pair], sems.at[halves * count + 1]),
    ]
    for copy in moved:
        copy.start()
    copies = []
    for k in range(halves):
        part = pl.ds(k * deep, deep)
        for n in range(count):
            at = k * count + n
            copies.append(
                pltpu.make_async_copy(
                    matrices[n].at[part], local.at[n, part], sems.at[at]
                )
            )
    for copy in copies:
        copy.start()
    for copy in moved:
        copy.wait()
    flat[...] = rows[...].reshape(flat.shape).astype(jnp.float32)

    def rows_of(piece):
        first, step = piece * tiles, pieces * tiles
        return jnp.concatenate(
            [flat[pl.ds(first + t, groups, stride=step), :] for t in range(tiles)], axis=1
        ).astype(jnp.bfloat16)

    sums = [None] * count
    for k in range(halves):
        part = slice(k * deep, (k + 1) * deep)
        lhs = jnp.concatenate([rows_of(p) for p in range(k, pieces, halves)], axis=0)
        for n in range(count):
            copies[k * count + n].wait()
            term = jnp.dot(lhs, local[n, part], preferred_element_type=jnp.float32)
            sums[n] = term if k == 0 else sums[n] + term
    top = sums[0]
    for n in range(1, count):
        top = jnp.maximum(top, sums[n])
    top = jnp.max(top, axis=1, keepdims=True)
    ids = ids_ref[...]
    total = jnp.zeros(sums[0].shape, jnp.float32)
    chosen = jnp.zeros(sums[0].shape, jnp.float32)
    for n in range(count):
        total = total + jnp.exp(sums[n] - top)
        columns = lax.broadcasted_iota(jnp.int32, sums[n].shape, 1) + firsts[n]
        chosen = chosen + jnp.where(columns == ids, sums[n], 0.0)
    total = jnp.sum(total, axis=1, keepdims=True)
    chosen = jnp.sum(chosen, axis=1, keepdims=True)
    lane = lax.broadcasted_iota(jnp.int32, (groups, 128), 1)
    packed = jnp.zeros((groups, 128), jnp.float32)
    owned = pieces // halves
    for n, column in enumerate((top, total, chosen)):
        for r in range(owned):
            part = column[r * groups : (r + 1) * groups]
            packed = jnp.where(lane == n * owned + r, part, packed)
    for g in range(groups):
        out_ref[g] = packed[g : g + 1]


def logit_stats(near_rows, far_rows, matrices, ids, groups):
    depth = matrices[0].shape[0]
    return pl.pallas_call(
        functools.partial(logits_kernel, groups),
        out_shape=pltpu.VMEM((groups, 1, 128), jnp.float32),
        in_specs=[any_spec(), any_spec(), vmem_spec()] + [any_spec() for _ in matrices],
        out_specs=vmem_spec(),
        scratch_shapes=[
            pltpu.VMEM((len(matrices), depth, 128), jnp.bfloat16),
            pltpu.VMEM((2, *near_rows.shape), near_rows.dtype),
            pltpu.VMEM((2 * near_rows.size // 128, 128), jnp.float32),
            pltpu.SemaphoreType.DMA((2 * len(matrices) + 2,)),
        ],
        cost_estimate=pl.CostEstimate(flops=270000000, bytes_accessed=4700000, transcendentals=0),
        compiler_params=room(12),
        name="logits",
    )(near_rows, far_rows, ids, *matrices)


def shifted(lines, places):
    return pltpu.roll(lines, places % 128, 1)


def merged(lines, keep, owned):
    low = jnp.min(lines, axis=0, keepdims=True)
    top = jnp.max(jnp.where(keep, lines, low), axis=0, keepdims=True)
    weight = jnp.where(keep, jnp.exp(jnp.minimum(lines - top, 0.0)), 0.0)
    total = jnp.sum(shifted(lines, -owned) * weight, axis=0, keepdims=True)
    chosen = jnp.sum(jnp.where(keep, lines, 0.0), axis=0, keepdims=True)
    return top, total, chosen


def group_kernel(owned, stats_ref, value_ref, out_ref):
    lines = stats_ref[...].reshape(stats_ref.shape[0], 128)
    top, total, chosen = merged(lines, jnp.full(lines.shape, True), owned)
    lane = lax.broadcasted_iota(jnp.int32, (1, 128), 1)
    packed = jnp.where(lane < owned, top, shifted(total, owned))
    packed = jnp.where(lane < 2 * owned, packed, chosen)
    packed = jnp.where(lane < 3 * owned, packed, value_ref[...])
    for n in range(out_ref.shape[0]):
        out_ref[n] = packed


def group_stats(stats, value, owned, copies):
    return pl.pallas_call(
        functools.partial(group_kernel, owned),
        out_shape=pltpu.VMEM((copies, 1, 128), jnp.float32),
        in_specs=[vmem_spec(), vmem_spec()],
        out_specs=vmem_spec(),
        compiler_params=room(2),
        name="group",
    )(stats, value)


def final_kernel(owned, cores, stats_ref, logprob_ref, value_ref):
    count = stats_ref.shape[0]
    lines = stats_ref[...].reshape(count, 128)
    place = lax.broadcasted_iota(jnp.int32, lines.shape, 0)
    lane = lax.broadcasted_iota(jnp.int32, lines.shape, 1)
    row = lax.broadcasted_iota(jnp.int32, (1, 128), 1)
    logprob = jnp.zeros((1, 128), jnp.float32)
    for core in range(cores):
        top, total, chosen = merged(lines, place % cores == core, owned)
        total = jnp.where(row < owned, total, 1.0)
        found = shifted(chosen, -2 * owned) - (top + jnp.log(total))
        logprob = jnp.where(row // owned == core, shifted(found, core * owned), logprob)
    values = jnp.broadcast_to(lines[:, 3 * owned : 3 * owned + 1], lines.shape)
    here = place == (lane % owned) * (count // owned) + lane // owned
    value = jnp.sum(jnp.where(here, values, 0.0), axis=0, keepdims=True)
    logprob_ref[...] = logprob[:, : logprob_ref.shape[1]]
    value_ref[...] = value[:, : value_ref.shape[1]]


def final_values(stats, owned, cores):
    rows = owned * cores
    return pl.pallas_call(
        functools.partial(final_kernel, owned, cores),
        out_shape=(
            jax.ShapeDtypeStruct((1, rows), jnp.float32),
            jax.ShapeDtypeStruct((1, rows), jnp.float32),
        ),
        in_specs=[vmem_spec()],
        out_specs=(vmem_spec(), vmem_spec()),
        compiler_params=room(2),
        name="final",
    )(stats)


def per_device(
    queries,
    keys_new,
    values_new,
    out_gate,
    decay_logit,
    beta_logit,
    decay_rate,
    state,
    norm_gain,
    out_proj,
    residual,
    final_gain,
    value_weight,
    lm_head,
    sampled,
):
    chips, cores = lax.axis_size("heads_0"), lax.axis_size("heads_1")
    groups = lax.axis_size(GROUP)
    chip, core = lax.axis_index("heads_0"), lax.axis_index("heads_1")
    side = lax.axis_index("x_side")
    rows_own, width = residual.shape
    rows_core = rows_own // cores
    copies = chips // rows_core
    lanes = 128
    lines = width // lanes

    x_head = lax.ppermute(lm_head, "x_side", SWAP)
    core_head = lax.ppermute(lm_head, "heads_1", SWAP)
    both_head = lax.ppermute(x_head, "heads_1", SWAP)
    partial_out = head_partials(
        queries,
        keys_new,
        values_new,
        out_gate,
        decay_logit,
        beta_logit,
        decay_rate,
        state,
        norm_gain,
        out_proj,
        residual,
        chips * cores,
    )
    arrived = exchange(partial_out, HEADS)
    gain = final_gain.reshape(lines, lanes)
    weight = value_weight.reshape(lines, lanes)
    half_here = (chip % copies).astype(jnp.int32).reshape(1)
    near = lax.axis_size(NEAR)
    pieces, value = norm_pieces(arrived, gain, weight, half_here, near, lines // copies)
    near_rows = exchange(pieces, NEAR)
    far_rows = lax.ppermute(near_rows, "x_pair", SWAP)

    matrices = (lm_head, core_head, x_head, both_head)
    ids = sampled.reshape(lax.axis_size("z"), lax.axis_size("x_pair"), -1, cores, rows_core)
    ids = lax.dynamic_index_in_dim(ids, side, 2, keepdims=False)
    ids = lax.dynamic_index_in_dim(ids, core, 2, keepdims=False)
    ids = ids.transpose(2, 1, 0).reshape(-1, 1)
    stats = logit_stats(near_rows, far_rows, matrices, ids, groups)
    stats = group_stats(exchange(stats, GROUP), value, rows_core, chips * cores)
    logprob, values = final_values(exchange(stats, HEADS), rows_core, cores)
    return (logprob.reshape(-1), values.reshape(-1))


def solution(mesh):
    torus = Mesh(
        mesh.devices.reshape(8, 2, 8, 2, 2), ("heads_0", "heads_1", "z", "x_pair", "x_side")
    )
    return jax.shard_map(
        per_device,
        mesh=torus,
        in_specs=(
            P(BATCH, HEADS),
            P(BATCH, HEADS),
            P(BATCH, HEADS),
            P(BATCH, HEADS),
            P(BATCH, HEADS),
            P(BATCH, HEADS),
            P(HEADS),
            P(BATCH, HEADS, None, None),
            P(),
            P(HEADS, None),
            P(BATCH, None),
            P(),
            P(),
            P(None, HEADS_BATCH),
            P(),
        ),
        out_specs=(P(BATCH), P(BATCH)),
        check_vma=False,
    )
```

```python
import functools

import jax
import jax.numpy as jnp
from jax import lax
from jax.experimental import pallas as pl
from jax.experimental.pallas import tpu as pltpu
from jax.sharding import Mesh
from jax.sharding import PartitionSpec as P


HEADS = ("heads_0", "heads_1")
BATCH = ("z", "x_side", "x_pair")
GROUP = ("x_pair", "z")
NEAR = ("z", "heads_0")
HEADS_BATCH = ("heads_0", "heads_1", "z", "x_side", "x_pair")
SWAP = [(0, 1), (1, 0)]


epsilon = 1e-06


def exchange(parts, axis):
    return lax.all_to_all(parts, axis, split_axis=0, concat_axis=0, tiled=True)


def any_spec():
    return pl.BlockSpec(memory_space=pltpu.HBM)


def room(mebibytes):
    return pltpu.CompilerParams(vmem_limit_bytes=mebibytes * 2**20)


def vmem_spec():
    return pl.BlockSpec(memory_space=pltpu.VMEM)


def smem_spec():
    return pl.BlockSpec(memory_space=pltpu.SMEM)


def as_column(line):
    size = line.shape[1]
    shape = (size, size)
    here = lax.broadcasted_iota(jnp.int32, shape, 0) == lax.broadcasted_iota(jnp.int32, shape, 1)
    return jnp.sum(jnp.where(here, jnp.broadcast_to(line, shape), 0.0), axis=1, keepdims=True)


def heads_kernel(*refs):
    small = 9
    inputs, out_ref, local = refs[:11], refs[11], refs[12:23]
    done_ref, sems, out_sems = refs[23:]
    q_ref, k_ref, v_ref, g_ref, dl_ref, bl_ref, gain_ref, rate_ref, res_ref = local[:small]
    state_ref, proj_ref = local[small:]
    copies = [pltpu.make_async_copy(inputs[n], local[n], sems.at[n]) for n in range(small)]
    heads = state_ref.shape[1]
    for h in range(heads):
        copies.append(
            pltpu.make_async_copy(
                inputs[small].at[:, h], state_ref.at[:, h], sems.at[small + h]
            )
        )
    blocks = 4
    wide = proj_ref.shape[1] // blocks
    for n in range(blocks):
        part = pl.ds(n * wide, wide)
        copies.append(
            pltpu.make_async_copy(
                inputs[small + 1].at[:, part], proj_ref.at[:, part], sems.at[small + heads + n]
            )
        )
    for copy in copies:
        copy.start()
    for copy in copies[:small]:
        copy.wait()
    rows = q_ref.shape[0]
    size = state_ref.shape[2]
    gain = gain_ref[...]
    queries, keys = [], []
    for h in range(heads):
        lanes = slice(h * size, (h + 1) * size)
        query = q_ref[:, lanes].astype(jnp.float32)
        key = k_ref[:, lanes].astype(jnp.float32)
        query = query / jnp.sqrt(jnp.sum(query * query, axis=1, keepdims=True) + epsilon)
        queries.append(query * size ** (-0.5))
        keys.append(key / jnp.sqrt(jnp.sum(key * key, axis=1, keepdims=True) + epsilon))
    turned = jnp.concatenate(queries + keys, axis=0).T
    parts = []
    for h in range(heads):
        lanes = slice(h * size, (h + 1) * size)
        logit = dl_ref[h : h + 1, :]
        soft = jnp.maximum(logit, 0.0) + jnp.log1p(jnp.exp(-jnp.abs(logit)))
        decay = as_column(jnp.exp(-rate_ref[:, h : h + 1] * soft))
        strength = as_column(1.0 / (1.0 + jnp.exp(-bl_ref[h : h + 1, :])))
        inter = jnp.sum(queries[h] * keys[h], axis=1, keepdims=True)
        value = v_ref[:, lanes].astype(jnp.float32)
        gate = g_ref[:, lanes].astype(jnp.float32)
        copies[small + h].wait()
        by_query, by_key = [], []
        for b in range(rows):
            block = state_ref[b, h]
            at = h * rows + b
            by_query.append(jnp.sum(turned[:, at : at + 1] * block, axis=0, keepdims=True))
            at += heads * rows
            by_key.append(jnp.sum(turned[:, at : at + 1] * block, axis=0, keepdims=True))
        state_query = jnp.concatenate(by_query, axis=0)
        state_key = jnp.concatenate(by_key, axis=0)
        written = value - decay * state_key
        output = decay * state_query + strength * inter * written
        mean = jnp.mean(output * output, axis=1, keepdims=True)
        normed = output / jnp.sqrt(mean + epsilon)
        parts.append(normed * gain * (gate / (1.0 + jnp.exp(-gate))))
    headout = jnp.concatenate(parts, axis=1).astype(jnp.bfloat16)
    chip, core = lax.axis_index("heads_0"), lax.axis_index("heads_1")
    first = jnp.where((chip == 0) & (core == 0), 1.0, 0.0)
    finished = []
    lines = wide // 128
    cores, halves = 2, out_ref.shape[0] // rows
    for n in range(blocks):
        copies[small + heads + n].wait()
        part = slice(n * wide, (n + 1) * wide)
        total = jnp.dot(headout, proj_ref[:, part], preferred_element_type=jnp.float32)
        total = total + res_ref[:, part].astype(jnp.float32) * first
        total = total.reshape(rows, lines, 128)
        for row in range(rows):
            for half in range(halves):
                core, r = row // (rows // cores), row % (rows // cores)
                place = (r * halves + half) * cores + core
                done_ref[place, n * lines : (n + 1) * lines, :] = total[row]
        part = pl.ds(n * lines, lines)
        finished.append(
            pltpu.make_async_copy(done_ref.at[:, part], out_ref.at[:, part], out_sems.at[n])
        )
        finished[-1].start()
    for copy in finished:
        copy.wait()


def head_partials(
    queries,
    keys_new,
    values_new,
    out_gate,
    decay_logit,
    beta_logit,
    decay_rate,
    state,
    norm_gain,
    out_proj,
    residual,
    places,
):
    arrays = (
        queries,
        keys_new,
        values_new,
        out_gate,
        decay_logit.T,
        beta_logit.T,
        norm_gain.reshape(1, -1),
        decay_rate.reshape(1, -1),
        residual,
        state,
        out_proj,
    )
    width = out_proj.shape[1]
    return pl.pallas_call(
        heads_kernel,
        out_shape=jax.ShapeDtypeStruct((places, width // 128, 128), jnp.float32),
        in_specs=[any_spec() for _ in arrays],
        out_specs=any_spec(),
        scratch_shapes=[pltpu.VMEM(a.shape, a.dtype) for a in arrays]
        + [
            pltpu.VMEM((places, width // 128, 128), jnp.float32),
            pltpu.SemaphoreType.DMA((9 + state.shape[1] + 4,)),
            pltpu.SemaphoreType.DMA((4,)),
        ],
        cost_estimate=pl.CostEstimate(flops=40000000, bytes_accessed=3500000, transcendentals=0),
        name="heads",
    )(*arrays)


def norm_kernel(half_ref, arrived_ref, gain_ref, weight_ref, piece_ref, value_ref, scratch):
    width = gain_ref.size
    hsum = arrived_ref[0]
    for n in range(1, arrived_ref.shape[0]):
        hsum = hsum + arrived_ref[n]
    gain = gain_ref[...]
    squares = jnp.sum(hsum * hsum, axis=(0, 1), keepdims=True)
    terms = jnp.sum(hsum * gain * weight_ref[...], axis=(0, 1), keepdims=True)
    rstd = 1.0 / jnp.sqrt(squares / width + epsilon)
    scratch[...] = hsum * rstd * gain
    lines = piece_ref.shape[1]
    start = pl.multiple_of(half_ref[0] * lines, lines)
    piece = scratch[pl.ds(start, lines), :].astype(jnp.bfloat16)
    for n in range(piece_ref.shape[0]):
        piece_ref[n] = piece
    value_ref[...] = jnp.broadcast_to(rstd * terms, value_ref.shape)


def norm_pieces(arrived, gain, weight, half, copies, lines):
    return pl.pallas_call(
        norm_kernel,
        out_shape=(
            pltpu.VMEM((copies, lines, 128), jnp.bfloat16),
            pltpu.VMEM((1, 128), jnp.float32),
        ),
        in_specs=[smem_spec(), vmem_spec(), vmem_spec(), vmem_spec()],
        out_specs=(vmem_spec(), vmem_spec()),
        scratch_shapes=[pltpu.VMEM(gain.shape, jnp.float32)],
        cost_estimate=pl.CostEstimate(flops=4000000, bytes_accessed=400000, transcendentals=0),
        compiler_params=room(4),
        name="norm",
    )(half, arrived, gain, weight)


def logits_kernel(groups, near_ref, far_ref, ids_ref, *refs):
    count = 4
    matrices, out_ref, local, rows, flat, sems = refs[:count], *refs[count:]
    tiles, lanes = near_ref.shape[1:]
    pieces = flat.shape[0] // (groups * tiles)
    deep = tiles * lanes
    halves = local.shape[1] // deep
    pair, core, side = (lax.axis_index(a) for a in ("x_pair", "heads_1", "x_side"))
    flat_place = 0
    for axis in HEADS_BATCH:
        flat_place = flat_place * lax.axis_size(axis) + lax.axis_index(axis)
    across = (1 - 2 * core) * lax.axis_size(BATCH)
    along = (1 - 2 * side) * lax.axis_size("x_pair")
    firsts = [(flat_place + step) * lanes for step in (0, across, along, across + along)]
    moved = [
        pltpu.make_async_copy(near_ref, rows.at[pair], sems.at[halves * count]),
        pltpu.make_async_copy(far_ref, rows.at[1 - pair], sems.at[halves * count + 1]),
    ]
    for copy in moved:
        copy.start()
    copies = []
    for k in range(halves):
        part = pl.ds(k * deep, deep)
        for n in range(count):
            at = k * count + n
            copies.append(
                pltpu.make_async_copy(
                    matrices[n].at[part], local.at[n, part], sems.at[at]
                )
            )
    for copy in copies:
        copy.start()
    for copy in moved:
        copy.wait()
    flat[...] = rows[...].reshape(flat.shape).astype(jnp.float32)

    def rows_of(piece):
        first, step = piece * tiles, pieces * tiles
        return jnp.concatenate(
            [flat[pl.ds(first + t, groups, stride=step), :] for t in range(tiles)], axis=1
        ).astype(jnp.bfloat16)

    sums = [None] * count
    for k in range(halves):
        part = slice(k * deep, (k + 1) * deep)
        lhs = jnp.concatenate([rows_of(p) for p in range(k, pieces, halves)], axis=0)
        for n in range(count):
            copies[k * count + n].wait()
            term = jnp.dot(lhs, local[n, part], preferred_element_type=jnp.float32)
            sums[n] = term if k == 0 else sums[n] + term
    top = sums[0]
    for n in range(1, count):
        top = jnp.maximum(top, sums[n])
    top = jnp.max(top, axis=1, keepdims=True)
    ids = ids_ref[...]
    total = jnp.zeros(sums[0].shape, jnp.float32)
    chosen = jnp.zeros(sums[0].shape, jnp.float32)
    for n in range(count):
        total = total + jnp.exp(sums[n] - top)
        columns = lax.broadcasted_iota(jnp.int32, sums[n].shape, 1) + firsts[n]
        chosen = chosen + jnp.where(columns == ids, sums[n], 0.0)
    total = jnp.sum(total, axis=1, keepdims=True)
    chosen = jnp.sum(chosen, axis=1, keepdims=True)
    lane = lax.broadcasted_iota(jnp.int32, (groups, 128), 1)
    packed = jnp.zeros((groups, 128), jnp.float32)
    owned = pieces // halves
    for n, column in enumerate((top, total, chosen)):
        for r in range(owned):
            part = column[r * groups : (r + 1) * groups]
            packed = jnp.where(lane == n * owned + r, part, packed)
    for g in range(groups):
        out_ref[g] = packed[g : g + 1]


def logit_stats(near_rows, far_rows, matrices, ids, groups):
    depth = matrices[0].shape[0]
    return pl.pallas_call(
        functools.partial(logits_kernel, groups),
        out_shape=pltpu.VMEM((groups, 1, 128), jnp.float32),
        in_specs=[any_spec(), any_spec(), vmem_spec()] + [any_spec() for _ in matrices],
        out_specs=vmem_spec(),
        scratch_shapes=[
            pltpu.VMEM((len(matrices), depth, 128), jnp.bfloat16),
            pltpu.VMEM((2, *near_rows.shape), near_rows.dtype),
            pltpu.VMEM((2 * near_rows.size // 128, 128), jnp.float32),
            pltpu.SemaphoreType.DMA((2 * len(matrices) + 2,)),
        ],
        cost_estimate=pl.CostEstimate(flops=270000000, bytes_accessed=4700000, transcendentals=0),
        compiler_params=room(12),
        name="logits",
    )(near_rows, far_rows, ids, *matrices)


def shifted(lines, places):
    return pltpu.roll(lines, places % 128, 1)


def merged(lines, keep, owned):
    low = jnp.min(lines, axis=0, keepdims=True)
    top = jnp.max(jnp.where(keep, lines, low), axis=0, keepdims=True)
    weight = jnp.where(keep, jnp.exp(jnp.minimum(lines - top, 0.0)), 0.0)
    total = jnp.sum(shifted(lines, -owned) * weight, axis=0, keepdims=True)
    chosen = jnp.sum(jnp.where(keep, lines, 0.0), axis=0, keepdims=True)
    return top, total, chosen


def group_kernel(owned, stats_ref, value_ref, out_ref):
    lines = stats_ref[...].reshape(stats_ref.shape[0], 128)
    top, total, chosen = merged(lines, jnp.full(lines.shape, True), owned)
    lane = lax.broadcasted_iota(jnp.int32, (1, 128), 1)
    packed = jnp.where(lane < owned, top, shifted(total, owned))
    packed = jnp.where(lane < 2 * owned, packed, chosen)
    packed = jnp.where(lane < 3 * owned, packed, value_ref[...])
    for n in range(out_ref.shape[0]):
        out_ref[n] = packed


def group_stats(stats, value, owned, copies):
    return pl.pallas_call(
        functools.partial(group_kernel, owned),
        out_shape=pltpu.VMEM((copies, 1, 128), jnp.float32),
        in_specs=[vmem_spec(), vmem_spec()],
        out_specs=vmem_spec(),
        compiler_params=room(2),
        name="group",
    )(stats, value)


def final_kernel(owned, cores, stats_ref, logprob_ref, value_ref):
    count = stats_ref.shape[0]
    lines = stats_ref[...].reshape(count, 128)
    place = lax.broadcasted_iota(jnp.int32, lines.shape, 0)
    lane = lax.broadcasted_iota(jnp.int32, lines.shape, 1)
    row = lax.broadcasted_iota(jnp.int32, (1, 128), 1)
    logprob = jnp.zeros((1, 128), jnp.float32)
    for core in range(cores):
        top, total, chosen = merged(lines, place % cores == core, owned)
        total = jnp.where(row < owned, total, 1.0)
        found = shifted(chosen, -2 * owned) - (top + jnp.log(total))
        logprob = jnp.where(row // owned == core, shifted(found, core * owned), logprob)
    values = jnp.broadcast_to(lines[:, 3 * owned : 3 * owned + 1], lines.shape)
    here = place == (lane % owned) * (count // owned) + lane // owned
    value = jnp.sum(jnp.where(here, values, 0.0), axis=0, keepdims=True)
    logprob_ref[...] = logprob[:, : logprob_ref.shape[1]]
    value_ref[...] = value[:, : value_ref.shape[1]]


def final_values(stats, owned, cores):
    rows = owned * cores
    return pl.pallas_call(
        functools.partial(final_kernel, owned, cores),
        out_shape=(
            jax.ShapeDtypeStruct((1, rows), jnp.float32),
            jax.ShapeDtypeStruct((1, rows), jnp.float32),
        ),
        in_specs=[vmem_spec()],
        out_specs=(vmem_spec(), vmem_spec()),
        compiler_params=room(2),
        name="final",
    )(stats)


def per_device(
    queries,
    keys_new,
    values_new,
    out_gate,
    decay_logit,
    beta_logit,
    decay_rate,
    state,
    norm_gain,
    out_proj,
    residual,
    final_gain,
    value_weight,
    lm_head,
    sampled,
):
    chips, cores = lax.axis_size("heads_0"), lax.axis_size("heads_1")
    groups = lax.axis_size(GROUP)
    chip, core = lax.axis_index("heads_0"), lax.axis_index("heads_1")
    side = lax.axis_index("x_side")
    rows_own, width = residual.shape
    rows_core = rows_own // cores
    copies = chips // rows_core
    lanes = 128
    lines = width // lanes

    x_head = lax.ppermute(lm_head, "x_side", SWAP)
    core_head = lax.ppermute(lm_head, "heads_1", SWAP)
    both_head = lax.ppermute(x_head, "heads_1", SWAP)
    partial_out = head_partials(
        queries,
        keys_new,
        values_new,
        out_gate,
        decay_logit,
        beta_logit,
        decay_rate,
        state,
        norm_gain,
        out_proj,
        residual,
        chips * cores,
    )
    arrived = exchange(partial_out, HEADS)
    gain = final_gain.reshape(lines, lanes)
    weight = value_weight.reshape(lines, lanes)
    half_here = (chip % copies).astype(jnp.int32).reshape(1)
    near = lax.axis_size(NEAR)
    pieces, value = norm_pieces(arrived, gain, weight, half_here, near, lines // copies)
    near_rows = exchange(pieces, NEAR)
    far_rows = lax.ppermute(near_rows, "x_pair", SWAP)

    matrices = (lm_head, core_head, x_head, both_head)
    ids = sampled.reshape(lax.axis_size("z"), lax.axis_size("x_side"), -1, cores, rows_core)
    ids = lax.dynamic_index_in_dim(ids, side, 1, keepdims=False)
    ids = lax.dynamic_index_in_dim(ids, core, 2, keepdims=False)
    ids = ids.transpose(2, 1, 0).reshape(-1, 1)
    stats = logit_stats(near_rows, far_rows, matrices, ids, groups)
    stats = group_stats(exchange(stats, GROUP), value, rows_core, chips * cores)
    logprob, values = final_values(exchange(stats, HEADS), rows_core, cores)
    return (logprob.reshape(-1), values.reshape(-1))


def solution(mesh):
    torus = Mesh(
        mesh.devices.reshape(8, 2, 8, 2, 2), ("heads_0", "heads_1", "z", "x_side", "x_pair")
    )
    return jax.shard_map(
        per_device,
        mesh=torus,
        in_specs=(
            P(BATCH, HEADS),
            P(BATCH, HEADS),
            P(BATCH, HEADS),
            P(BATCH, HEADS),
            P(BATCH, HEADS),
            P(BATCH, HEADS),
            P(HEADS),
            P(BATCH, HEADS, None, None),
            P(),
            P(HEADS, None),
            P(BATCH, None),
            P(),
            P(),
            P(None, HEADS_BATCH),
            P(),
        ),
        out_specs=(P(BATCH), P(BATCH)),
        check_vma=False,
    )
```

```python
import functools

import jax
import jax.numpy as jnp
from jax import lax
from jax.experimental import pallas as pl
from jax.experimental.pallas import tpu as pltpu
from jax.sharding import Mesh
from jax.sharding import PartitionSpec as P


HEADS = ("heads_0", "heads_1")
BATCH = ("z", "x_side", "x_pair")
GROUP = ("x_pair", "z")
NEAR = ("z", "heads_0")
CHIPS = ("heads_0", "x_pair", "z")
HEADS_BATCH = ("heads_0", "heads_1", "z", "x_side", "x_pair")
SWAP = [(0, 1), (1, 0)]


epsilon = 1e-06


def exchange(parts, axis):
    return lax.all_to_all(parts, axis, split_axis=0, concat_axis=0, tiled=True)


def any_spec():
    return pl.BlockSpec(memory_space=pltpu.HBM)


def room(mebibytes):
    return pltpu.CompilerParams(vmem_limit_bytes=mebibytes * 2**20)


def vmem_spec():
    return pl.BlockSpec(memory_space=pltpu.VMEM)


def smem_spec():
    return pl.BlockSpec(memory_space=pltpu.SMEM)


def as_column(line):
    size = line.shape[1]
    shape = (size, size)
    here = lax.broadcasted_iota(jnp.int32, shape, 0) == lax.broadcasted_iota(jnp.int32, shape, 1)
    return jnp.sum(jnp.where(here, jnp.broadcast_to(line, shape), 0.0), axis=1, keepdims=True)


def heads_kernel(*refs):
    small = 9
    inputs, out_ref, local = refs[:11], refs[11], refs[12:23]
    done_ref, sems, out_sems = refs[23:]
    q_ref, k_ref, v_ref, g_ref, dl_ref, bl_ref, gain_ref, rate_ref, res_ref = local[:small]
    state_ref, proj_ref = local[small:]
    copies = [pltpu.make_async_copy(inputs[n], local[n], sems.at[n]) for n in range(small)]
    heads = state_ref.shape[1]
    parts = 2
    rows_part = state_ref.shape[0] // parts
    for h in range(heads):
        for n in range(parts):
            part = pl.ds(n * rows_part, rows_part)
            copies.append(
                pltpu.make_async_copy(
                    inputs[small].at[part, h], state_ref.at[part, h], sems.at[len(copies)]
                )
            )
    blocks = 4
    wide = proj_ref.shape[1] // blocks
    deep = proj_ref.shape[0] // parts
    for n in range(blocks):
        for m in range(parts):
            part = (pl.ds(m * deep, deep), pl.ds(n * wide, wide))
            copies.append(
                pltpu.make_async_copy(
                    inputs[small + 1].at[part], proj_ref.at[part], sems.at[len(copies)]
                )
            )
    for copy in copies:
        copy.start()
    for copy in copies[:small]:
        copy.wait()
    rows = q_ref.shape[0]
    size = state_ref.shape[2]
    gain = gain_ref[...]
    queries, keys = [], []
    for h in range(heads):
        lanes = slice(h * size, (h + 1) * size)
        query = q_ref[:, lanes].astype(jnp.float32)
        key = k_ref[:, lanes].astype(jnp.float32)
        query = query / jnp.sqrt(jnp.sum(query * query, axis=1, keepdims=True) + epsilon)
        queries.append(query * size ** (-0.5))
        keys.append(key / jnp.sqrt(jnp.sum(key * key, axis=1, keepdims=True) + epsilon))
    turned = jnp.concatenate(queries + keys, axis=0).T
    pieces = []
    for h in range(heads):
        lanes = slice(h * size, (h + 1) * size)
        logit = dl_ref[h : h + 1, :]
        soft = jnp.maximum(logit, 0.0) + jnp.log1p(jnp.exp(-jnp.abs(logit)))
        decay = as_column(jnp.exp(-rate_ref[:, h : h + 1] * soft))
        strength = as_column(1.0 / (1.0 + jnp.exp(-bl_ref[h : h + 1, :])))
        inter = jnp.sum(queries[h] * keys[h], axis=1, keepdims=True)
        value = v_ref[:, lanes].astype(jnp.float32)
        gate = g_ref[:, lanes].astype(jnp.float32)
        for copy in copies[small + parts * h : small + parts * (h + 1)]:
            copy.wait()
        by_query, by_key = [], []
        for b in range(rows):
            block = state_ref[b, h]
            at = h * rows + b
            by_query.append(jnp.sum(turned[:, at : at + 1] * block, axis=0, keepdims=True))
            at += heads * rows
            by_key.append(jnp.sum(turned[:, at : at + 1] * block, axis=0, keepdims=True))
        state_query = jnp.concatenate(by_query, axis=0)
        state_key = jnp.concatenate(by_key, axis=0)
        written = value - decay * state_key
        output = decay * state_query + strength * inter * written
        mean = jnp.mean(output * output, axis=1, keepdims=True)
        normed = output / jnp.sqrt(mean + epsilon)
        pieces.append(normed * gain * (gate / (1.0 + jnp.exp(-gate))))
    headout = jnp.concatenate(pieces, axis=1).astype(jnp.bfloat16)
    chip, core = lax.axis_index("heads_0"), lax.axis_index("heads_1")
    first = jnp.where((chip == 0) & (core == 0), 1.0, 0.0)
    finished = []
    lines = wide // 128
    cores, halves = 2, out_ref.shape[0] // rows
    for n in range(blocks):
        at = small + parts * (heads + n)
        for copy in copies[at : at + parts]:
            copy.wait()
        part = slice(n * wide, (n + 1) * wide)
        total = jnp.dot(headout, proj_ref[:, part], preferred_element_type=jnp.float32)
        total = total + res_ref[:, part].astype(jnp.float32) * first
        total = total.reshape(rows, lines, 128)
        for row in range(rows):
            for half in range(halves):
                core, r = row // (rows // cores), row % (rows // cores)
                place = (r * halves + half) * cores + core
                done_ref[place, n * lines : (n + 1) * lines, :] = total[row]
        part = pl.ds(n * lines, lines)
        finished.append(
            pltpu.make_async_copy(done_ref.at[:, part], out_ref.at[:, part], out_sems.at[n])
        )
        finished[-1].start()
    for copy in finished:
        copy.wait()


def head_partials(
    queries,
    keys_new,
    values_new,
    out_gate,
    decay_logit,
    beta_logit,
    decay_rate,
    state,
    norm_gain,
    out_proj,
    residual,
    places,
):
    arrays = (
        queries,
        keys_new,
        values_new,
        out_gate,
        decay_logit.T,
        beta_logit.T,
        norm_gain.reshape(1, -1),
        decay_rate.reshape(1, -1),
        residual,
        state,
        out_proj,
    )
    width = out_proj.shape[1]
    return pl.pallas_call(
        heads_kernel,
        out_shape=jax.ShapeDtypeStruct((places, width // 128, 128), jnp.float32),
        in_specs=[any_spec() for _ in arrays],
        out_specs=any_spec(),
        scratch_shapes=[pltpu.VMEM(a.shape, a.dtype) for a in arrays]
        + [
            pltpu.VMEM((places, width // 128, 128), jnp.float32),
            pltpu.SemaphoreType.DMA((9 + 2 * (state.shape[1] + 4),)),
            pltpu.SemaphoreType.DMA((4,)),
        ],
        cost_estimate=pl.CostEstimate(flops=40000000, bytes_accessed=3500000, transcendentals=0),
        compiler_params=room(63),
        name="heads",
    )(*arrays)


def norm_kernel(half_ref, arrived_ref, gain_ref, weight_ref, piece_ref, value_ref, scratch):
    width = gain_ref.size
    hsum = arrived_ref[0]
    for n in range(1, arrived_ref.shape[0]):
        hsum = hsum + arrived_ref[n]
    gain = gain_ref[...]
    squares = jnp.sum(hsum * hsum, axis=(0, 1), keepdims=True)
    terms = jnp.sum(hsum * gain * weight_ref[...], axis=(0, 1), keepdims=True)
    rstd = 1.0 / jnp.sqrt(squares / width + epsilon)
    scratch[...] = hsum * rstd * gain
    lines = piece_ref.shape[1]
    start = pl.multiple_of(half_ref[0] * lines, lines)
    piece = scratch[pl.ds(start, lines), :].astype(jnp.bfloat16)
    for n in range(piece_ref.shape[0]):
        piece_ref[n] = piece
    value_ref[...] = jnp.broadcast_to(rstd * terms, value_ref.shape)


def norm_pieces(arrived, gain, weight, half, copies, lines):
    return pl.pallas_call(
        norm_kernel,
        out_shape=(
            pltpu.VMEM((copies, lines, 128), jnp.bfloat16),
            pltpu.VMEM((1, 128), jnp.float32),
        ),
        in_specs=[smem_spec(), vmem_spec(), vmem_spec(), vmem_spec()],
        out_specs=(vmem_spec(), vmem_spec()),
        scratch_shapes=[pltpu.VMEM(gain.shape, jnp.float32)],
        cost_estimate=pl.CostEstimate(flops=4000000, bytes_accessed=400000, transcendentals=0),
        compiler_params=room(4),
        name="norm",
    )(half, arrived, gain, weight)


def logits_kernel(groups, near_ref, far_ref, ids_ref, value_ref, *refs):
    count = 4
    matrices, out_ref, local, rows, flat, sems = refs[:count], *refs[count:]
    tiles, lanes = near_ref.shape[1:]
    pieces = flat.shape[0] // (groups * tiles)
    deep = tiles * lanes
    halves = local.shape[0] // deep
    pair, core, side = (lax.axis_index(a) for a in ("x_pair", "heads_1", "x_side"))
    flat_place = 0
    for axis in HEADS_BATCH:
        flat_place = flat_place * lax.axis_size(axis) + lax.axis_index(axis)
    across = (1 - 2 * core) * lax.axis_size(BATCH)
    along = (1 - 2 * side) * lax.axis_size("x_pair")
    firsts = [(flat_place + step) * lanes for step in (0, across, along, across + along)]
    moved = [
        pltpu.make_async_copy(near_ref, rows.at[pair], sems.at[halves]),
        pltpu.make_async_copy(far_ref, rows.at[1 - pair], sems.at[halves + 1]),
    ]
    for copy in moved:
        copy.start()
    copies = []
    for k in range(halves):
        part = pl.ds(k * deep, deep)
        copies.append(
            pltpu.make_async_copy(matrices[-1].at[part], local.at[part], sems.at[k])
        )
    for copy in copies:
        copy.start()
    for copy in moved:
        copy.wait()
    flat[...] = rows[...].reshape(flat.shape).astype(jnp.float32)

    def rows_of(piece):
        first, step = piece * tiles, pieces * tiles
        return jnp.concatenate(
            [flat[pl.ds(first + t, groups, stride=step), :] for t in range(tiles)], axis=1
        ).astype(jnp.bfloat16)

    sums = [None] * count
    for k in range(halves):
        part = slice(k * deep, (k + 1) * deep)
        lhs = jnp.concatenate([rows_of(p) for p in range(k, pieces, halves)], axis=0)
        for n in range(count):
            if n == count - 1:
                copies[k].wait()
            matrix = matrices[n] if n < count - 1 else local
            term = jnp.dot(lhs, matrix[part, :], preferred_element_type=jnp.float32)
            sums[n] = term if k == 0 else sums[n] + term
    top = sums[0]
    for n in range(1, count):
        top = jnp.maximum(top, sums[n])
    top = jnp.max(top, axis=1, keepdims=True)
    ids = ids_ref[...]
    total = jnp.zeros(sums[0].shape, jnp.float32)
    chosen = jnp.zeros(sums[0].shape, jnp.float32)
    for n in range(count):
        total = total + jnp.exp(sums[n] - top)
        columns = lax.broadcasted_iota(jnp.int32, sums[n].shape, 1) + firsts[n]
        chosen = chosen + jnp.where(columns == ids, sums[n], 0.0)
    total = jnp.sum(total, axis=1, keepdims=True)
    chosen = jnp.sum(chosen, axis=1, keepdims=True)
    lane = lax.broadcasted_iota(jnp.int32, (groups, 128), 1)
    packed = jnp.broadcast_to(value_ref[...], (groups, 128))
    owned = pieces // halves
    for n, column in enumerate((top, total, chosen)):
        for r in range(owned):
            part = column[r * groups : (r + 1) * groups]
            packed = jnp.where(lane == n * owned + r, part, packed)
    for place in range(out_ref.shape[0]):
        g = place % groups
        out_ref[place] = packed[g : g + 1]


def logit_stats(near_rows, far_rows, matrices, ids, value, groups, chips):
    depth = matrices[0].shape[0]
    return pl.pallas_call(
        functools.partial(logits_kernel, groups),
        out_shape=pltpu.VMEM((chips * groups, 1, 128), jnp.float32),
        in_specs=[any_spec(), any_spec(), vmem_spec(), vmem_spec()]
        + [vmem_spec() for _ in matrices[:-1]]
        + [any_spec()],
        out_specs=vmem_spec(),
        scratch_shapes=[
            pltpu.VMEM((depth, 128), jnp.bfloat16),
            pltpu.VMEM((2, *near_rows.shape), near_rows.dtype),
            pltpu.VMEM((2 * near_rows.size // 128, 128), jnp.float32),
            pltpu.SemaphoreType.DMA((4,)),
        ],
        cost_estimate=pl.CostEstimate(flops=270000000, bytes_accessed=4700000, transcendentals=0),
        compiler_params=room(12),
        name="logits",
    )(near_rows, far_rows, ids, value, *matrices)


def shifted(lines, places):
    return pltpu.roll(lines, places % 128, 1)


def merge_kernel(owned, groups, stats_ref, out_ref):
    count = stats_ref.shape[0]
    lines = stats_ref[...].reshape(count, 128)
    lane = lax.broadcasted_iota(jnp.int32, lines.shape, 1)
    row = lax.broadcasted_iota(jnp.int32, (1, 128), 1)
    top = jnp.max(lines, axis=0, keepdims=True)
    total = jnp.sum(shifted(lines, -owned) * jnp.exp(lines - top), axis=0, keepdims=True)
    chosen = shifted(jnp.sum(lines, axis=0, keepdims=True), -2 * owned)
    logprob = chosen - (top + jnp.log(jnp.where(row < owned, total, 1.0)))
    values = jnp.broadcast_to(lines[:, 3 * owned : 3 * owned + 1], lines.shape)
    here = lax.axis_index("x_pair") * lax.axis_size("z") + lax.axis_index("z")
    source = (lane - owned) * (count // groups // owned) * groups + here
    place = lax.broadcasted_iota(jnp.int32, lines.shape, 0)
    value = jnp.sum(jnp.where(place == source, values, 0.0), axis=0, keepdims=True)
    out_ref[...] = jnp.where(row < owned, logprob, value)


def merge_stats(stats, owned, groups):
    return pl.pallas_call(
        functools.partial(merge_kernel, owned, groups),
        out_shape=pltpu.VMEM((1, 128), jnp.float32),
        in_specs=[vmem_spec()],
        out_specs=vmem_spec(),
        compiler_params=room(2),
        name="merge",
    )(stats)


def final_kernel(owned, own_ref, other_ref, logprob_ref, value_ref):
    own, other = own_ref[...], other_ref[...]
    first = lax.axis_index("heads_1") == 0
    low, high = jnp.where(first, own, other), jnp.where(first, other, own)
    row = lax.broadcasted_iota(jnp.int32, own.shape, 1)
    rows = logprob_ref.shape[1]
    logprob_ref[...] = jnp.where(row < owned, low, shifted(high, owned))[:, :rows]
    value_ref[...] = jnp.where(row < owned, shifted(low, -owned), high)[:, :rows]


def final_values(own, other, owned, rows):
    return pl.pallas_call(
        functools.partial(final_kernel, owned),
        out_shape=(
            jax.ShapeDtypeStruct((1, rows), jnp.float32),
            jax.ShapeDtypeStruct((1, rows), jnp.float32),
        ),
        in_specs=[vmem_spec(), vmem_spec()],
        out_specs=(vmem_spec(), vmem_spec()),
        compiler_params=room(2),
        name="final",
    )(own, other)


def per_device(
    queries,
    keys_new,
    values_new,
    out_gate,
    decay_logit,
    beta_logit,
    decay_rate,
    state,
    norm_gain,
    out_proj,
    residual,
    final_gain,
    value_weight,
    lm_head,
    sampled,
):
    chips, cores = lax.axis_size("heads_0"), lax.axis_size("heads_1")
    groups = lax.axis_size(GROUP)
    chip, core = lax.axis_index("heads_0"), lax.axis_index("heads_1")
    side = lax.axis_index("x_side")
    rows_own, width = residual.shape
    rows_core = rows_own // cores
    copies = chips // rows_core
    lanes = 128
    lines = width // lanes

    x_head = lax.ppermute(lm_head, "x_side", SWAP)
    core_head = lax.ppermute(lm_head, "heads_1", SWAP)
    both_head = lax.ppermute(x_head, "heads_1", SWAP)
    partial_out = head_partials(
        queries,
        keys_new,
        values_new,
        out_gate,
        decay_logit,
        beta_logit,
        decay_rate,
        state,
        norm_gain,
        out_proj,
        residual,
        chips * cores,
    )
    arrived = exchange(partial_out, HEADS)
    gain = final_gain.reshape(lines, lanes)
    weight = value_weight.reshape(lines, lanes)
    half_here = (chip % copies).astype(jnp.int32).reshape(1)
    near = lax.axis_size(NEAR)
    pieces, value = norm_pieces(arrived, gain, weight, half_here, near, lines // copies)
    near_rows = exchange(pieces, NEAR)
    far_rows = lax.ppermute(near_rows, "x_pair", SWAP)

    matrices = (lm_head, core_head, x_head, both_head)
    ids = sampled.reshape(lax.axis_size("z"), lax.axis_size("x_side"), -1, cores, rows_core)
    ids = lax.dynamic_index_in_dim(ids, side, 1, keepdims=False)
    ids = lax.dynamic_index_in_dim(ids, core, 2, keepdims=False)
    ids = ids.transpose(2, 1, 0).reshape(-1, 1)
    stats = logit_stats(near_rows, far_rows, matrices, ids, value, groups, chips)
    own = merge_stats(exchange(stats, CHIPS), rows_core, groups)
    other = lax.ppermute(own, "heads_1", SWAP)
    logprob, values = final_values(own, other, rows_core, rows_own)
    return (logprob.reshape(-1), values.reshape(-1))


def solution(mesh):
    torus = Mesh(
        mesh.devices.reshape(8, 2, 8, 2, 2), ("heads_0", "heads_1", "z", "x_side", "x_pair")
    )
    return jax.shard_map(
        per_device,
        mesh=torus,
        in_specs=(
            P(BATCH, HEADS),
            P(BATCH, HEADS),
            P(BATCH, HEADS),
            P(BATCH, HEADS),
            P(BATCH, HEADS),
            P(BATCH, HEADS),
            P(HEADS),
            P(BATCH, HEADS, None, None),
            P(),
            P(HEADS, None),
            P(BATCH, None),
            P(),
            P(),
            P(None, HEADS_BATCH),
            P(),
        ),
        out_specs=(P(BATCH), P(BATCH)),
        check_vma=False,
    )
```

```python
import functools

import jax
import jax.numpy as jnp
from jax import lax
from jax.experimental import pallas as pl
from jax.experimental.pallas import tpu as pltpu
from jax.sharding import Mesh
from jax.sharding import PartitionSpec as P


HEADS = ("heads_0", "heads_1")
BATCH = ("z", "x_side", "x_pair")
GROUP = ("x_pair", "z")
NEAR = ("z", "heads_0")
HEADS_BATCH = ("heads_0", "heads_1", "z", "x_side", "x_pair")
SWAP = [(0, 1), (1, 0)]


epsilon = 1e-06


def exchange(parts, axis):
    return lax.all_to_all(parts, axis, split_axis=0, concat_axis=0, tiled=True)


def any_spec():
    return pl.BlockSpec(memory_space=pltpu.HBM)


def room(mebibytes):
    return pltpu.CompilerParams(vmem_limit_bytes=mebibytes * 2**20)


def vmem_spec():
    return pl.BlockSpec(memory_space=pltpu.VMEM)


def smem_spec():
    return pl.BlockSpec(memory_space=pltpu.SMEM)


def as_column(line):
    size = line.shape[1]
    shape = (size, size)
    here = lax.broadcasted_iota(jnp.int32, shape, 0) == lax.broadcasted_iota(jnp.int32, shape, 1)
    return jnp.sum(jnp.where(here, jnp.broadcast_to(line, shape), 0.0), axis=1, keepdims=True)


def heads_kernel(*refs):
    small = 9
    inputs, out_ref, local = refs[:11], refs[11], refs[12:23]
    done_ref, sems, out_sems = refs[23:]
    q_ref, k_ref, v_ref, g_ref, dl_ref, bl_ref, gain_ref, rate_ref, res_ref = local[:small]
    state_ref, proj_ref = local[small:]
    copies = [pltpu.make_async_copy(inputs[n], local[n], sems.at[n]) for n in range(small)]
    heads = state_ref.shape[1]
    for h in range(heads):
        copies.append(
            pltpu.make_async_copy(
                inputs[small].at[:, h], state_ref.at[:, h], sems.at[small + h]
            )
        )
    blocks = 4
    wide = proj_ref.shape[1] // blocks
    for n in range(blocks):
        part = pl.ds(n * wide, wide)
        copies.append(
            pltpu.make_async_copy(
                inputs[small + 1].at[:, part], proj_ref.at[:, part], sems.at[small + heads + n]
            )
        )
    for copy in copies:
        copy.start()
    for copy in copies[:small]:
        copy.wait()
    rows = q_ref.shape[0]
    size = state_ref.shape[2]
    gain = gain_ref[...]
    queries, keys = [], []
    for h in range(heads):
        lanes = slice(h * size, (h + 1) * size)
        query = q_ref[:, lanes].astype(jnp.float32)
        key = k_ref[:, lanes].astype(jnp.float32)
        query = query / jnp.sqrt(jnp.sum(query * query, axis=1, keepdims=True) + epsilon)
        queries.append(query * size ** (-0.5))
        keys.append(key / jnp.sqrt(jnp.sum(key * key, axis=1, keepdims=True) + epsilon))
    turned = jnp.concatenate(queries + keys, axis=0).T
    parts = []
    for h in range(heads):
        lanes = slice(h * size, (h + 1) * size)
        logit = dl_ref[h : h + 1, :]
        soft = jnp.maximum(logit, 0.0) + jnp.log1p(jnp.exp(-jnp.abs(logit)))
        decay = as_column(jnp.exp(-rate_ref[:, h : h + 1] * soft))
        strength = as_column(1.0 / (1.0 + jnp.exp(-bl_ref[h : h + 1, :])))
        inter = jnp.sum(queries[h] * keys[h], axis=1, keepdims=True)
        value = v_ref[:, lanes].astype(jnp.float32)
        gate = g_ref[:, lanes].astype(jnp.float32)
        copies[small + h].wait()
        by_query, by_key = [], []
        for b in range(rows):
            block = state_ref[b, h]
            at = h * rows + b
            by_query.append(jnp.sum(turned[:, at : at + 1] * block, axis=0, keepdims=True))
            at += heads * rows
            by_key.append(jnp.sum(turned[:, at : at + 1] * block, axis=0, keepdims=True))
        state_query = jnp.concatenate(by_query, axis=0)
        state_key = jnp.concatenate(by_key, axis=0)
        written = value - decay * state_key
        output = decay * state_query + strength * inter * written
        mean = jnp.mean(output * output, axis=1, keepdims=True)
        normed = output / jnp.sqrt(mean + epsilon)
        parts.append(normed * gain * (gate / (1.0 + jnp.exp(-gate))))
    headout = jnp.concatenate(parts, axis=1).astype(jnp.bfloat16)
    chip, core = lax.axis_index("heads_0"), lax.axis_index("heads_1")
    first = jnp.where((chip == 0) & (core == 0), 1.0, 0.0)
    finished = []
    lines = wide // 128
    cores, halves = 2, out_ref.shape[0] // rows
    for n in range(blocks):
        copies[small + heads + n].wait()
        part = slice(n * wide, (n + 1) * wide)
        total = jnp.dot(headout, proj_ref[:, part], preferred_element_type=jnp.float32)
        total = total + res_ref[:, part].astype(jnp.float32) * first
        total = total.reshape(rows, lines, 128)
        for row in range(rows):
            for half in range(halves):
                core, r = row // (rows // cores), row % (rows // cores)
                place = (r * halves + half) * cores + core
                done_ref[place, n * lines : (n + 1) * lines, :] = total[row]
        part = pl.ds(n * lines, lines)
        finished.append(
            pltpu.make_async_copy(done_ref.at[:, part], out_ref.at[:, part], out_sems.at[n])
        )
        finished[-1].start()
    for copy in finished:
        copy.wait()


def head_partials(
    queries,
    keys_new,
    values_new,
    out_gate,
    decay_logit,
    beta_logit,
    decay_rate,
    state,
    norm_gain,
    out_proj,
    residual,
    places,
):
    arrays = (
        queries,
        keys_new,
        values_new,
        out_gate,
        decay_logit.T,
        beta_logit.T,
        norm_gain.reshape(1, -1),
        decay_rate.reshape(1, -1),
        residual,
        state,
        out_proj,
    )
    width = out_proj.shape[1]
    return pl.pallas_call(
        heads_kernel,
        out_shape=jax.ShapeDtypeStruct((places, width // 128, 128), jnp.float32),
        in_specs=[any_spec() for _ in arrays],
        out_specs=any_spec(),
        scratch_shapes=[pltpu.VMEM(a.shape, a.dtype) for a in arrays]
        + [
            pltpu.VMEM((places, width // 128, 128), jnp.float32),
            pltpu.SemaphoreType.DMA((9 + state.shape[1] + 4,)),
            pltpu.SemaphoreType.DMA((4,)),
        ],
        cost_estimate=pl.CostEstimate(flops=40000000, bytes_accessed=3500000, transcendentals=0),
        name="heads",
    )(*arrays)


def norm_kernel(half_ref, arrived_ref, gain_ref, weight_ref, piece_ref, value_ref, scratch):
    width = gain_ref.size
    hsum = arrived_ref[0]
    for n in range(1, arrived_ref.shape[0]):
        hsum = hsum + arrived_ref[n]
    gain = gain_ref[...]
    squares = jnp.sum(hsum * hsum, axis=(0, 1), keepdims=True)
    terms = jnp.sum(hsum * gain * weight_ref[...], axis=(0, 1), keepdims=True)
    rstd = 1.0 / jnp.sqrt(squares / width + epsilon)
    scratch[...] = hsum * rstd * gain
    lines = piece_ref.shape[1]
    start = pl.multiple_of(half_ref[0] * lines, lines)
    piece = scratch[pl.ds(start, lines), :].astype(jnp.bfloat16)
    for n in range(piece_ref.shape[0]):
        piece_ref[n] = piece
    value_ref[...] = jnp.broadcast_to(rstd * terms, value_ref.shape)


def norm_pieces(arrived, gain, weight, half, copies, lines):
    return pl.pallas_call(
        norm_kernel,
        out_shape=(
            pltpu.VMEM((copies, lines, 128), jnp.bfloat16),
            pltpu.VMEM((1, 128), jnp.float32),
        ),
        in_specs=[smem_spec(), vmem_spec(), vmem_spec(), vmem_spec()],
        out_specs=(vmem_spec(), vmem_spec()),
        scratch_shapes=[pltpu.VMEM(gain.shape, jnp.float32)],
        cost_estimate=pl.CostEstimate(flops=4000000, bytes_accessed=400000, transcendentals=0),
        compiler_params=room(4),
        name="norm",
    )(half, arrived, gain, weight)


def logits_kernel(groups, near_ref, far_ref, ids_ref, *refs):
    count = 4
    matrices, out_ref, local, rows, flat, sems = refs[:count], *refs[count:]
    tiles, lanes = near_ref.shape[1:]
    pieces = flat.shape[0] // (groups * tiles)
    deep = tiles * lanes
    halves = local.shape[0] // deep
    pair, core, side = (lax.axis_index(a) for a in ("x_pair", "heads_1", "x_side"))
    flat_place = 0
    for axis in HEADS_BATCH:
        flat_place = flat_place * lax.axis_size(axis) + lax.axis_index(axis)
    across = (1 - 2 * core) * lax.axis_size(BATCH)
    along = (1 - 2 * side) * lax.axis_size("x_pair")
    firsts = [(flat_place + step) * lanes for step in (0, across, along, across + along)]
    moved = [
        pltpu.make_async_copy(near_ref, rows.at[pair], sems.at[halves]),
        pltpu.make_async_copy(far_ref, rows.at[1 - pair], sems.at[halves + 1]),
    ]
    for copy in moved:
        copy.start()
    copies = []
    for k in range(halves):
        part = pl.ds(k * deep, deep)
        copies.append(
            pltpu.make_async_copy(matrices[-1].at[part], local.at[part], sems.at[k])
        )
    for copy in copies:
        copy.start()
    for copy in moved:
        copy.wait()
    flat[...] = rows[...].reshape(flat.shape).astype(jnp.float32)

    def rows_of(piece):
        first, step = piece * tiles, pieces * tiles
        return jnp.concatenate(
            [flat[pl.ds(first + t, groups, stride=step), :] for t in range(tiles)], axis=1
        ).astype(jnp.bfloat16)

    sums = [None] * count
    for k in range(halves):
        part = slice(k * deep, (k + 1) * deep)
        lhs = jnp.concatenate([rows_of(p) for p in range(k, pieces, halves)], axis=0)
        for n in range(count):
            if n == count - 1:
                copies[k].wait()
            matrix = matrices[n] if n < count - 1 else local
            term = jnp.dot(lhs, matrix[part, :], preferred_element_type=jnp.float32)
            sums[n] = term if k == 0 else sums[n] + term
    top = sums[0]
    for n in range(1, count):
        top = jnp.maximum(top, sums[n])
    top = jnp.max(top, axis=1, keepdims=True)
    ids = ids_ref[...]
    total = jnp.zeros(sums[0].shape, jnp.float32)
    chosen = jnp.zeros(sums[0].shape, jnp.float32)
    for n in range(count):
        total = total + jnp.exp(sums[n] - top)
        columns = lax.broadcasted_iota(jnp.int32, sums[n].shape, 1) + firsts[n]
        chosen = chosen + jnp.where(columns == ids, sums[n], 0.0)
    total = jnp.sum(total, axis=1, keepdims=True)
    chosen = jnp.sum(chosen, axis=1, keepdims=True)
    lane = lax.broadcasted_iota(jnp.int32, (groups, 128), 1)
    packed = jnp.zeros((groups, 128), jnp.float32)
    owned = pieces // halves
    for n, column in enumerate((top, total, chosen)):
        for r in range(owned):
            part = column[r * groups : (r + 1) * groups]
            packed = jnp.where(lane == n * owned + r, part, packed)
    for g in range(groups):
        out_ref[g] = packed[g : g + 1]


def logit_stats(near_rows, far_rows, matrices, ids, groups):
    depth = matrices[0].shape[0]
    return pl.pallas_call(
        functools.partial(logits_kernel, groups),
        out_shape=pltpu.VMEM((groups, 1, 128), jnp.float32),
        in_specs=[any_spec(), any_spec(), vmem_spec()]
        + [vmem_spec() for _ in matrices[:-1]]
        + [any_spec()],
        out_specs=vmem_spec(),
        scratch_shapes=[
            pltpu.VMEM((depth, 128), jnp.bfloat16),
            pltpu.VMEM((2, *near_rows.shape), near_rows.dtype),
            pltpu.VMEM((2 * near_rows.size // 128, 128), jnp.float32),
            pltpu.SemaphoreType.DMA((4,)),
        ],
        cost_estimate=pl.CostEstimate(flops=270000000, bytes_accessed=4700000, transcendentals=0),
        compiler_params=room(12),
        name="logits",
    )(near_rows, far_rows, ids, *matrices)


def shifted(lines, places):
    return pltpu.roll(lines, places % 128, 1)


def merged(lines, keep, owned):
    low = jnp.min(lines, axis=0, keepdims=True)
    top = jnp.max(jnp.where(keep, lines, low), axis=0, keepdims=True)
    weight = jnp.where(keep, jnp.exp(jnp.minimum(lines - top, 0.0)), 0.0)
    total = jnp.sum(shifted(lines, -owned) * weight, axis=0, keepdims=True)
    chosen = jnp.sum(jnp.where(keep, lines, 0.0), axis=0, keepdims=True)
    return top, total, chosen


def group_kernel(owned, stats_ref, value_ref, out_ref):
    lines = stats_ref[...].reshape(stats_ref.shape[0], 128)
    top, total, chosen = merged(lines, jnp.full(lines.shape, True), owned)
    lane = lax.broadcasted_iota(jnp.int32, (1, 128), 1)
    packed = jnp.where(lane < owned, top, shifted(total, owned))
    packed = jnp.where(lane < 2 * owned, packed, chosen)
    packed = jnp.where(lane < 3 * owned, packed, value_ref[...])
    for n in range(out_ref.shape[0]):
        out_ref[n] = packed


def group_stats(stats, value, owned, copies):
    return pl.pallas_call(
        functools.partial(group_kernel, owned),
        out_shape=pltpu.VMEM((copies, 1, 128), jnp.float32),
        in_specs=[vmem_spec(), vmem_spec()],
        out_specs=vmem_spec(),
        compiler_params=room(2),
        name="group",
    )(stats, value)


def final_kernel(owned, cores, stats_ref, logprob_ref, value_ref):
    count = stats_ref.shape[0]
    lines = stats_ref[...].reshape(count, 128)
    place = lax.broadcasted_iota(jnp.int32, lines.shape, 0)
    lane = lax.broadcasted_iota(jnp.int32, lines.shape, 1)
    row = lax.broadcasted_iota(jnp.int32, (1, 128), 1)
    logprob = jnp.zeros((1, 128), jnp.float32)
    for core in range(cores):
        top, total, chosen = merged(lines, place % cores == core, owned)
        total = jnp.where(row < owned, total, 1.0)
        found = shifted(chosen, -2 * owned) - (top + jnp.log(total))
        logprob = jnp.where(row // owned == core, shifted(found, core * owned), logprob)
    values = jnp.broadcast_to(lines[:, 3 * owned : 3 * owned + 1], lines.shape)
    here = place == (lane % owned) * (count // owned) + lane // owned
    value = jnp.sum(jnp.where(here, values, 0.0), axis=0, keepdims=True)
    logprob_ref[...] = logprob[:, : logprob_ref.shape[1]]
    value_ref[...] = value[:, : value_ref.shape[1]]


def final_values(stats, owned, cores):
    rows = owned * cores
    return pl.pallas_call(
        functools.partial(final_kernel, owned, cores),
        out_shape=(
            jax.ShapeDtypeStruct((1, rows), jnp.float32),
            jax.ShapeDtypeStruct((1, rows), jnp.float32),
        ),
        in_specs=[vmem_spec()],
        out_specs=(vmem_spec(), vmem_spec()),
        compiler_params=room(2),
        name="final",
    )(stats)


def per_device(
    queries,
    keys_new,
    values_new,
    out_gate,
    decay_logit,
    beta_logit,
    decay_rate,
    state,
    norm_gain,
    out_proj,
    residual,
    final_gain,
    value_weight,
    lm_head,
    sampled,
):
    chips, cores = lax.axis_size("heads_0"), lax.axis_size("heads_1")
    groups = lax.axis_size(GROUP)
    chip, core = lax.axis_index("heads_0"), lax.axis_index("heads_1")
    side = lax.axis_index("x_side")
    rows_own, width = residual.shape
    rows_core = rows_own // cores
    copies = chips // rows_core
    lanes = 128
    lines = width // lanes

    x_head = lax.ppermute(lm_head, "x_side", SWAP)
    core_head = lax.ppermute(lm_head, "heads_1", SWAP)
    both_head = lax.ppermute(x_head, "heads_1", SWAP)
    partial_out = head_partials(
        queries,
        keys_new,
        values_new,
        out_gate,
        decay_logit,
        beta_logit,
        decay_rate,
        state,
        norm_gain,
        out_proj,
        residual,
        chips * cores,
    )
    arrived = exchange(partial_out, HEADS)
    gain = final_gain.reshape(lines, lanes)
    weight = value_weight.reshape(lines, lanes)
    half_here = (chip % copies).astype(jnp.int32).reshape(1)
    near = lax.axis_size(NEAR)
    pieces, value = norm_pieces(arrived, gain, weight, half_here, near, lines // copies)
    near_rows = exchange(pieces, NEAR)
    far_rows = lax.ppermute(near_rows, "x_pair", SWAP)

    matrices = (lm_head, core_head, x_head, both_head)
    ids = sampled.reshape(lax.axis_size("z"), lax.axis_size("x_side"), -1, cores, rows_core)
    ids = lax.dynamic_index_in_dim(ids, side, 1, keepdims=False)
    ids = lax.dynamic_index_in_dim(ids, core, 2, keepdims=False)
    ids = ids.transpose(2, 1, 0).reshape(-1, 1)
    stats = logit_stats(near_rows, far_rows, matrices, ids, groups)
    stats = group_stats(exchange(stats, GROUP), value, rows_core, chips * cores)
    logprob, values = final_values(exchange(stats, HEADS), rows_core, cores)
    return (logprob.reshape(-1), values.reshape(-1))


def solution(mesh):
    torus = Mesh(
        mesh.devices.reshape(8, 2, 8, 2, 2), ("heads_0", "heads_1", "z", "x_side", "x_pair")
    )
    return jax.shard_map(
        per_device,
        mesh=torus,
        in_specs=(
            P(BATCH, HEADS),
            P(BATCH, HEADS),
            P(BATCH, HEADS),
            P(BATCH, HEADS),
            P(BATCH, HEADS),
            P(BATCH, HEADS),
            P(HEADS),
            P(BATCH, HEADS, None, None),
            P(),
            P(HEADS, None),
            P(BATCH, None),
            P(),
            P(),
            P(None, HEADS_BATCH),
            P(),
        ),
        out_specs=(P(BATCH), P(BATCH)),
        check_vma=False,
    )
```

```python
import functools

import jax
import jax.numpy as jnp
from jax import lax
from jax.experimental import pallas as pl
from jax.experimental.pallas import tpu as pltpu
from jax.sharding import Mesh
from jax.sharding import PartitionSpec as P


HEADS = ("heads_0", "heads_1")
BATCH = ("z", "x_side", "x_pair")
GROUP = ("x_pair", "z")
NEAR = ("heads_0", "z")
HEADS_BATCH = ("heads_0", "heads_1", "z", "x_side", "x_pair")
SWAP = [(0, 1), (1, 0)]


epsilon = 1e-06


def exchange(parts, axis):
    return lax.all_to_all(parts, axis, split_axis=0, concat_axis=0, tiled=True)


def any_spec():
    return pl.BlockSpec(memory_space=pltpu.HBM)


def room(mebibytes):
    return pltpu.CompilerParams(vmem_limit_bytes=mebibytes * 2**20)


def vmem_spec():
    return pl.BlockSpec(memory_space=pltpu.VMEM)


def smem_spec():
    return pl.BlockSpec(memory_space=pltpu.SMEM)


def as_column(line):
    size = line.shape[1]
    shape = (size, size)
    here = lax.broadcasted_iota(jnp.int32, shape, 0) == lax.broadcasted_iota(jnp.int32, shape, 1)
    return jnp.sum(jnp.where(here, jnp.broadcast_to(line, shape), 0.0), axis=1, keepdims=True)


def heads_kernel(*refs):
    small = 9
    inputs, out_ref, local = refs[:11], refs[11], refs[12:23]
    done_ref, sems, out_sems = refs[23:]
    q_ref, k_ref, v_ref, g_ref, dl_ref, bl_ref, gain_ref, rate_ref, res_ref = local[:small]
    state_ref, proj_ref = local[small:]
    copies = [pltpu.make_async_copy(inputs[n], local[n], sems.at[n]) for n in range(small)]
    heads = state_ref.shape[1]
    for h in range(heads):
        copies.append(
            pltpu.make_async_copy(
                inputs[small].at[:, h], state_ref.at[:, h], sems.at[small + h]
            )
        )
    blocks = 4
    wide = proj_ref.shape[1] // blocks
    for n in range(blocks):
        part = pl.ds(n * wide, wide)
        copies.append(
            pltpu.make_async_copy(
                inputs[small + 1].at[:, part], proj_ref.at[:, part], sems.at[small + heads + n]
            )
        )
    for copy in copies:
        copy.start()
    for copy in copies[:small]:
        copy.wait()
    rows = q_ref.shape[0]
    size = state_ref.shape[2]
    gain = gain_ref[...]
    queries, keys = [], []
    for h in range(heads):
        lanes = slice(h * size, (h + 1) * size)
        query = q_ref[:, lanes].astype(jnp.float32)
        key = k_ref[:, lanes].astype(jnp.float32)
        query = query / jnp.sqrt(jnp.sum(query * query, axis=1, keepdims=True) + epsilon)
        queries.append(query * size ** (-0.5))
        keys.append(key / jnp.sqrt(jnp.sum(key * key, axis=1, keepdims=True) + epsilon))
    turned = jnp.concatenate(queries + keys, axis=0).T
    parts = []
    for h in range(heads):
        lanes = slice(h * size, (h + 1) * size)
        logit = dl_ref[h : h + 1, :]
        soft = jnp.maximum(logit, 0.0) + jnp.log1p(jnp.exp(-jnp.abs(logit)))
        decay = as_column(jnp.exp(-rate_ref[:, h : h + 1] * soft))
        strength = as_column(1.0 / (1.0 + jnp.exp(-bl_ref[h : h + 1, :])))
        inter = jnp.sum(queries[h] * keys[h], axis=1, keepdims=True)
        value = v_ref[:, lanes].astype(jnp.float32)
        gate = g_ref[:, lanes].astype(jnp.float32)
        copies[small + h].wait()
        by_query, by_key = [], []
        for b in range(rows):
            block = state_ref[b, h]
            at = h * rows + b
            by_query.append(jnp.sum(turned[:, at : at + 1] * block, axis=0, keepdims=True))
            at += heads * rows
            by_key.append(jnp.sum(turned[:, at : at + 1] * block, axis=0, keepdims=True))
        state_query = jnp.concatenate(by_query, axis=0)
        state_key = jnp.concatenate(by_key, axis=0)
        written = value - decay * state_key
        output = decay * state_query + strength * inter * written
        mean = jnp.mean(output * output, axis=1, keepdims=True)
        normed = output / jnp.sqrt(mean + epsilon)
        parts.append(normed * gain * (gate / (1.0 + jnp.exp(-gate))))
    headout = jnp.concatenate(parts, axis=1).astype(jnp.bfloat16)
    chip, core = lax.axis_index("heads_0"), lax.axis_index("heads_1")
    first = jnp.where((chip == 0) & (core == 0), 1.0, 0.0)
    finished = []
    lines = wide // 128
    cores, halves = 2, out_ref.shape[0] // rows
    for n in range(blocks):
        copies[small + heads + n].wait()
        part = slice(n * wide, (n + 1) * wide)
        total = jnp.dot(headout, proj_ref[:, part], preferred_element_type=jnp.float32)
        total = total + res_ref[:, part].astype(jnp.float32) * first
        total = total.reshape(rows, lines, 128)
        for row in range(rows):
            for half in range(halves):
                core, r = row // (rows // cores), row % (rows // cores)
                place = (r * halves + half) * cores + core
                done_ref[place, n * lines : (n + 1) * lines, :] = total[row]
        part = pl.ds(n * lines, lines)
        finished.append(
            pltpu.make_async_copy(done_ref.at[:, part], out_ref.at[:, part], out_sems.at[n])
        )
        finished[-1].start()
    for copy in finished:
        copy.wait()


def head_partials(
    queries,
    keys_new,
    values_new,
    out_gate,
    decay_logit,
    beta_logit,
    decay_rate,
    state,
    norm_gain,
    out_proj,
    residual,
    places,
):
    arrays = (
        queries,
        keys_new,
        values_new,
        out_gate,
        decay_logit.T,
        beta_logit.T,
        norm_gain.reshape(1, -1),
        decay_rate.reshape(1, -1),
        residual,
        state,
        out_proj,
    )
    width = out_proj.shape[1]
    return pl.pallas_call(
        heads_kernel,
        out_shape=jax.ShapeDtypeStruct((places, width // 128, 128), jnp.float32),
        in_specs=[any_spec() for _ in arrays],
        out_specs=any_spec(),
        scratch_shapes=[pltpu.VMEM(a.shape, a.dtype) for a in arrays]
        + [
            pltpu.VMEM((places, width // 128, 128), jnp.float32),
            pltpu.SemaphoreType.DMA((9 + state.shape[1] + 4,)),
            pltpu.SemaphoreType.DMA((4,)),
        ],
        cost_estimate=pl.CostEstimate(flops=40000000, bytes_accessed=3500000, transcendentals=0),
        name="heads",
    )(*arrays)


def norm_kernel(half_ref, arrived_ref, gain_ref, weight_ref, piece_ref, value_ref, scratch):
    width = gain_ref.size
    hsum = arrived_ref[0]
    for n in range(1, arrived_ref.shape[0]):
        hsum = hsum + arrived_ref[n]
    gain = gain_ref[...]
    squares = jnp.sum(hsum * hsum, axis=(0, 1), keepdims=True)
    terms = jnp.sum(hsum * gain * weight_ref[...], axis=(0, 1), keepdims=True)
    rstd = 1.0 / jnp.sqrt(squares / width + epsilon)
    scratch[...] = hsum * rstd * gain
    lines = piece_ref.shape[1]
    start = pl.multiple_of(half_ref[0] * lines, lines)
    piece = scratch[pl.ds(start, lines), :].astype(jnp.bfloat16)
    for n in range(piece_ref.shape[0]):
        piece_ref[n] = piece
    value_ref[...] = jnp.broadcast_to(rstd * terms, value_ref.shape)


def norm_pieces(arrived, gain, weight, half, copies, lines):
    return pl.pallas_call(
        norm_kernel,
        out_shape=(
            pltpu.VMEM((copies, lines, 128), jnp.bfloat16),
            pltpu.VMEM((1, 128), jnp.float32),
        ),
        in_specs=[smem_spec(), vmem_spec(), vmem_spec(), vmem_spec()],
        out_specs=(vmem_spec(), vmem_spec()),
        scratch_shapes=[pltpu.VMEM(gain.shape, jnp.float32)],
        cost_estimate=pl.CostEstimate(flops=4000000, bytes_accessed=400000, transcendentals=0),
        compiler_params=room(4),
        name="norm",
    )(half, arrived, gain, weight)


def logits_kernel(groups, near_ref, far_ref, ids_ref, *refs):
    count = 4
    matrices, out_ref, local, rows, flat, sems = refs[:count], *refs[count:]
    tiles, lanes = near_ref.shape[1:]
    pieces = flat.shape[0] // (groups * tiles)
    deep = tiles * lanes
    halves = local.shape[0] // deep
    pair, core, side = (lax.axis_index(a) for a in ("x_pair", "heads_1", "x_side"))
    flat_place = 0
    for axis in HEADS_BATCH:
        flat_place = flat_place * lax.axis_size(axis) + lax.axis_index(axis)
    across = (1 - 2 * core) * lax.axis_size(BATCH)
    along = (1 - 2 * side) * lax.axis_size("x_pair")
    firsts = [(flat_place + step) * lanes for step in (0, across, along, across + along)]
    moved = [
        pltpu.make_async_copy(near_ref, rows.at[pair], sems.at[halves]),
        pltpu.make_async_copy(far_ref, rows.at[1 - pair], sems.at[halves + 1]),
    ]
    for copy in moved:
        copy.start()
    copies = []
    for k in range(halves):
        part = pl.ds(k * deep, deep)
        copies.append(
            pltpu.make_async_copy(matrices[-1].at[part], local.at[part], sems.at[k])
        )
    for copy in copies:
        copy.start()
    for copy in moved:
        copy.wait()
    flat[...] = rows[...].reshape(flat.shape).astype(jnp.float32)

    def rows_of(piece):
        each = groups // 2
        lines = []
        for t in range(tiles):
            at = piece * each * tiles + t
            found = [
                flat[pl.ds(at + n * pieces * each * tiles, each, stride=tiles), :] for n in range(2)
            ]
            lines.append(jnp.concatenate(found, axis=0))
        return jnp.concatenate(lines, axis=1).astype(jnp.bfloat16)

    sums = [None] * count
    for k in range(halves):
        part = slice(k * deep, (k + 1) * deep)
        lhs = jnp.concatenate([rows_of(p) for p in range(k, pieces, halves)], axis=0)
        for n in range(count):
            if n == count - 1:
                copies[k].wait()
            matrix = matrices[n] if n < count - 1 else local
            term = jnp.dot(lhs, matrix[part, :], preferred_element_type=jnp.float32)
            sums[n] = term if k == 0 else sums[n] + term
    top = sums[0]
    for n in range(1, count):
        top = jnp.maximum(top, sums[n])
    top = jnp.max(top, axis=1, keepdims=True)
    ids = ids_ref[...]
    total = jnp.zeros(sums[0].shape, jnp.float32)
    chosen = jnp.zeros(sums[0].shape, jnp.float32)
    for n in range(count):
        total = total + jnp.exp(sums[n] - top)
        columns = lax.broadcasted_iota(jnp.int32, sums[n].shape, 1) + firsts[n]
        chosen = chosen + jnp.where(columns == ids, sums[n], 0.0)
    total = jnp.sum(total, axis=1, keepdims=True)
    chosen = jnp.sum(chosen, axis=1, keepdims=True)
    lane = lax.broadcasted_iota(jnp.int32, (groups, 128), 1)
    packed = jnp.zeros((groups, 128), jnp.float32)
    owned = pieces // halves
    for n, column in enumerate((top, total, chosen)):
        for r in range(owned):
            part = column[r * groups : (r + 1) * groups]
            packed = jnp.where(lane == n * owned + r, part, packed)
    for g in range(groups):
        out_ref[g] = packed[g : g + 1]


def logit_stats(near_rows, far_rows, matrices, ids, groups):
    depth = matrices[0].shape[0]
    return pl.pallas_call(
        functools.partial(logits_kernel, groups),
        out_shape=pltpu.VMEM((groups, 1, 128), jnp.float32),
        in_specs=[any_spec(), any_spec(), vmem_spec()]
        + [vmem_spec() for _ in matrices[:-1]]
        + [any_spec()],
        out_specs=vmem_spec(),
        scratch_shapes=[
            pltpu.VMEM((depth, 128), jnp.bfloat16),
            pltpu.VMEM((2, *near_rows.shape), near_rows.dtype),
            pltpu.VMEM((2 * near_rows.size // 128, 128), jnp.float32),
            pltpu.SemaphoreType.DMA((4,)),
        ],
        cost_estimate=pl.CostEstimate(flops=270000000, bytes_accessed=4700000, transcendentals=0),
        compiler_params=room(12),
        name="logits",
    )(near_rows, far_rows, ids, *matrices)


def shifted(lines, places):
    return pltpu.roll(lines, places % 128, 1)


def merged(lines, keep, owned):
    low = jnp.min(lines, axis=0, keepdims=True)
    top = jnp.max(jnp.where(keep, lines, low), axis=0, keepdims=True)
    weight = jnp.where(keep, jnp.exp(jnp.minimum(lines - top, 0.0)), 0.0)
    total = jnp.sum(shifted(lines, -owned) * weight, axis=0, keepdims=True)
    chosen = jnp.sum(jnp.where(keep, lines, 0.0), axis=0, keepdims=True)
    return top, total, chosen


def group_kernel(owned, stats_ref, value_ref, out_ref):
    lines = stats_ref[...].reshape(stats_ref.shape[0], 128)
    top, total, chosen = merged(lines, jnp.full(lines.shape, True), owned)
    lane = lax.broadcasted_iota(jnp.int32, (1, 128), 1)
    packed = jnp.where(lane < owned, top, shifted(total, owned))
    packed = jnp.where(lane < 2 * owned, packed, chosen)
    packed = jnp.where(lane < 3 * owned, packed, value_ref[...])
    for n in range(out_ref.shape[0]):
        out_ref[n] = packed


def group_stats(stats, value, owned, copies):
    return pl.pallas_call(
        functools.partial(group_kernel, owned),
        out_shape=pltpu.VMEM((copies, 1, 128), jnp.float32),
        in_specs=[vmem_spec(), vmem_spec()],
        out_specs=vmem_spec(),
        compiler_params=room(2),
        name="group",
    )(stats, value)


def final_kernel(owned, cores, stats_ref, logprob_ref, value_ref):
    count = stats_ref.shape[0]
    lines = stats_ref[...].reshape(count, 128)
    place = lax.broadcasted_iota(jnp.int32, lines.shape, 0)
    lane = lax.broadcasted_iota(jnp.int32, lines.shape, 1)
    row = lax.broadcasted_iota(jnp.int32, (1, 128), 1)
    logprob = jnp.zeros((1, 128), jnp.float32)
    for core in range(cores):
        top, total, chosen = merged(lines, place % cores == core, owned)
        total = jnp.where(row < owned, total, 1.0)
        found = shifted(chosen, -2 * owned) - (top + jnp.log(total))
        logprob = jnp.where(row // owned == core, shifted(found, core * owned), logprob)
    values = jnp.broadcast_to(lines[:, 3 * owned : 3 * owned + 1], lines.shape)
    here = place == (lane % owned) * (count // owned) + lane // owned
    value = jnp.sum(jnp.where(here, values, 0.0), axis=0, keepdims=True)
    logprob_ref[...] = logprob[:, : logprob_ref.shape[1]]
    value_ref[...] = value[:, : value_ref.shape[1]]


def final_values(stats, owned, cores):
    rows = owned * cores
    return pl.pallas_call(
        functools.partial(final_kernel, owned, cores),
        out_shape=(
            jax.ShapeDtypeStruct((1, rows), jnp.float32),
            jax.ShapeDtypeStruct((1, rows), jnp.float32),
        ),
        in_specs=[vmem_spec()],
        out_specs=(vmem_spec(), vmem_spec()),
        compiler_params=room(2),
        name="final",
    )(stats)


def per_device(
    queries,
    keys_new,
    values_new,
    out_gate,
    decay_logit,
    beta_logit,
    decay_rate,
    state,
    norm_gain,
    out_proj,
    residual,
    final_gain,
    value_weight,
    lm_head,
    sampled,
):
    chips, cores = lax.axis_size("heads_0"), lax.axis_size("heads_1")
    groups = lax.axis_size(GROUP)
    chip, core = lax.axis_index("heads_0"), lax.axis_index("heads_1")
    side = lax.axis_index("x_side")
    rows_own, width = residual.shape
    rows_core = rows_own // cores
    copies = chips // rows_core
    lanes = 128
    lines = width // lanes

    x_head = lax.ppermute(lm_head, "x_side", SWAP)
    core_head = lax.ppermute(lm_head, "heads_1", SWAP)
    both_head = lax.ppermute(x_head, "heads_1", SWAP)
    partial_out = head_partials(
        queries,
        keys_new,
        values_new,
        out_gate,
        decay_logit,
        beta_logit,
        decay_rate,
        state,
        norm_gain,
        out_proj,
        residual,
        chips * cores,
    )
    arrived = exchange(partial_out, HEADS)
    gain = final_gain.reshape(lines, lanes)
    weight = value_weight.reshape(lines, lanes)
    half_here = (chip % copies).astype(jnp.int32).reshape(1)
    near = lax.axis_size(NEAR)
    pieces, value = norm_pieces(arrived, gain, weight, half_here, near, lines // copies)
    near_rows = exchange(pieces, NEAR)
    far_rows = lax.ppermute(near_rows, "x_pair", SWAP)

    matrices = (lm_head, core_head, x_head, both_head)
    ids = sampled.reshape(lax.axis_size("z"), lax.axis_size("x_side"), -1, cores, rows_core)
    ids = lax.dynamic_index_in_dim(ids, side, 1, keepdims=False)
    ids = lax.dynamic_index_in_dim(ids, core, 2, keepdims=False)
    ids = ids.transpose(2, 1, 0).reshape(-1, 1)
    stats = logit_stats(near_rows, far_rows, matrices, ids, groups)
    stats = group_stats(exchange(stats, GROUP), value, rows_core, chips * cores)
    logprob, values = final_values(exchange(stats, HEADS), rows_core, cores)
    return (logprob.reshape(-1), values.reshape(-1))


def solution(mesh):
    torus = Mesh(
        mesh.devices.reshape(8, 2, 8, 2, 2), ("heads_0", "heads_1", "z", "x_side", "x_pair")
    )
    return jax.shard_map(
        per_device,
        mesh=torus,
        in_specs=(
            P(BATCH, HEADS),
            P(BATCH, HEADS),
            P(BATCH, HEADS),
            P(BATCH, HEADS),
            P(BATCH, HEADS),
            P(BATCH, HEADS),
            P(HEADS),
            P(BATCH, HEADS, None, None),
            P(),
            P(HEADS, None),
            P(BATCH, None),
            P(),
            P(),
            P(None, HEADS_BATCH),
            P(),
        ),
        out_specs=(P(BATCH), P(BATCH)),
        check_vma=False,
    )
```

```python
import functools

import jax
import jax.numpy as jnp
from jax import lax
from jax.experimental import pallas as pl
from jax.experimental.pallas import tpu as pltpu
from jax.sharding import Mesh
from jax.sharding import PartitionSpec as P


HEADS = ("heads_0", "heads_1")
BATCH = ("z", "x_side", "x_pair")
GROUP = ("x_pair", "z")
NEAR = ("z", "heads_0")
HEADS_BATCH = ("heads_0", "heads_1", "z", "x_side", "x_pair")
SWAP = [(0, 1), (1, 0)]


epsilon = 1e-06


def exchange(parts, axis):
    return lax.all_to_all(parts, axis, split_axis=0, concat_axis=0, tiled=True)


def any_spec():
    return pl.BlockSpec(memory_space=pltpu.HBM)


def room(mebibytes):
    return pltpu.CompilerParams(vmem_limit_bytes=mebibytes * 2**20)


def vmem_spec():
    return pl.BlockSpec(memory_space=pltpu.VMEM)


def smem_spec():
    return pl.BlockSpec(memory_space=pltpu.SMEM)


def as_column(line):
    size = line.shape[1]
    shape = (size, size)
    here = lax.broadcasted_iota(jnp.int32, shape, 0) == lax.broadcasted_iota(jnp.int32, shape, 1)
    return jnp.sum(jnp.where(here, jnp.broadcast_to(line, shape), 0.0), axis=1, keepdims=True)


def heads_kernel(*refs):
    small = 9
    inputs, out_ref, local = refs[:11], refs[11], refs[12:23]
    done_ref, sems, out_sems = refs[23:]
    q_ref, k_ref, v_ref, g_ref, dl_ref, bl_ref, gain_ref, rate_ref, res_ref = local[:small]
    state_ref, proj_ref = local[small:]
    copies = [pltpu.make_async_copy(inputs[n], local[n], sems.at[n]) for n in range(small)]
    heads = state_ref.shape[1]
    for h in range(heads):
        copies.append(
            pltpu.make_async_copy(
                inputs[small].at[:, h], state_ref.at[:, h], sems.at[small + h]
            )
        )
    blocks = 4
    wide = proj_ref.shape[1] // blocks
    for n in range(blocks):
        part = pl.ds(n * wide, wide)
        copies.append(
            pltpu.make_async_copy(
                inputs[small + 1].at[:, part], proj_ref.at[:, part], sems.at[small + heads + n]
            )
        )
    for copy in copies:
        copy.start()
    for copy in copies[:small]:
        copy.wait()
    rows = q_ref.shape[0]
    size = state_ref.shape[2]
    gain = gain_ref[...]
    queries, keys = [], []
    for h in range(heads):
        lanes = slice(h * size, (h + 1) * size)
        query = q_ref[:, lanes].astype(jnp.float32)
        key = k_ref[:, lanes].astype(jnp.float32)
        query = query / jnp.sqrt(jnp.sum(query * query, axis=1, keepdims=True) + epsilon)
        queries.append(query * size ** (-0.5))
        keys.append(key / jnp.sqrt(jnp.sum(key * key, axis=1, keepdims=True) + epsilon))
    turned = jnp.concatenate(queries + keys, axis=0).T
    parts = []
    for h in range(heads):
        lanes = slice(h * size, (h + 1) * size)
        logit = dl_ref[h : h + 1, :]
        soft = jnp.maximum(logit, 0.0) + jnp.log1p(jnp.exp(-jnp.abs(logit)))
        decay = as_column(jnp.exp(-rate_ref[:, h : h + 1] * soft))
        strength = as_column(1.0 / (1.0 + jnp.exp(-bl_ref[h : h + 1, :])))
        inter = jnp.sum(queries[h] * keys[h], axis=1, keepdims=True)
        value = v_ref[:, lanes].astype(jnp.float32)
        gate = g_ref[:, lanes].astype(jnp.float32)
        copies[small + h].wait()
        by_query, by_key = [], []
        for b in range(rows):
            block = state_ref[b, h]
            at = h * rows + b
            by_query.append(jnp.sum(turned[:, at : at + 1] * block, axis=0, keepdims=True))
            at += heads * rows
            by_key.append(jnp.sum(turned[:, at : at + 1] * block, axis=0, keepdims=True))
        state_query = jnp.concatenate(by_query, axis=0)
        state_key = jnp.concatenate(by_key, axis=0)
        written = value - decay * state_key
        output = decay * state_query + strength * inter * written
        mean = jnp.mean(output * output, axis=1, keepdims=True)
        normed = output / jnp.sqrt(mean + epsilon)
        parts.append(normed * gain * (gate / (1.0 + jnp.exp(-gate))))
    headout = jnp.concatenate(parts, axis=1).astype(jnp.bfloat16)
    chip, core = lax.axis_index("heads_0"), lax.axis_index("heads_1")
    first = jnp.where((chip == 0) & (core == 0), 1.0, 0.0)
    finished = []
    lines = wide // 128
    cores, halves = 2, out_ref.shape[0] // rows
    for n in range(blocks):
        copies[small + heads + n].wait()
        part = slice(n * wide, (n + 1) * wide)
        total = jnp.dot(headout, proj_ref[:, part], preferred_element_type=jnp.float32)
        total = total + res_ref[:, part].astype(jnp.float32) * first
        total = total.reshape(rows, lines, 128)
        for row in range(rows):
            for half in range(halves):
                core, r = row // (rows // cores), row % (rows // cores)
                place = (r * halves + half) * cores + core
                done_ref[place, n * lines : (n + 1) * lines, :] = total[row]
        part = pl.ds(n * lines, lines)
        finished.append(
            pltpu.make_async_copy(done_ref.at[:, part], out_ref.at[:, part], out_sems.at[n])
        )
        finished[-1].start()
    for copy in finished:
        copy.wait()


def head_partials(
    queries,
    keys_new,
    values_new,
    out_gate,
    decay_logit,
    beta_logit,
    decay_rate,
    state,
    norm_gain,
    out_proj,
    residual,
    places,
):
    arrays = (
        queries,
        keys_new,
        values_new,
        out_gate,
        decay_logit.T,
        beta_logit.T,
        norm_gain.reshape(1, -1),
        decay_rate.reshape(1, -1),
        residual,
        state,
        out_proj,
    )
    width = out_proj.shape[1]
    return pl.pallas_call(
        heads_kernel,
        out_shape=jax.ShapeDtypeStruct((places, width // 128, 128), jnp.float32),
        in_specs=[any_spec() for _ in arrays],
        out_specs=any_spec(),
        scratch_shapes=[pltpu.VMEM(a.shape, a.dtype) for a in arrays]
        + [
            pltpu.VMEM((places, width // 128, 128), jnp.float32),
            pltpu.SemaphoreType.DMA((9 + state.shape[1] + 4,)),
            pltpu.SemaphoreType.DMA((4,)),
        ],
        cost_estimate=pl.CostEstimate(flops=40000000, bytes_accessed=3500000, transcendentals=0),
        name="heads",
    )(*arrays)


def norm_kernel(half_ref, arrived_ref, gain_ref, weight_ref, piece_ref, value_ref, scratch):
    width = gain_ref.size
    hsum = arrived_ref[0]
    for n in range(1, arrived_ref.shape[0]):
        hsum = hsum + arrived_ref[n]
    gain = gain_ref[...]
    squares = jnp.sum(hsum * hsum, axis=(0, 1), keepdims=True)
    terms = jnp.sum(hsum * gain * weight_ref[...], axis=(0, 1), keepdims=True)
    rstd = 1.0 / jnp.sqrt(squares / width + epsilon)
    scratch[...] = hsum * rstd * gain
    lines = piece_ref.shape[1]
    start = pl.multiple_of(half_ref[0] * lines, lines)
    piece = scratch[pl.ds(start, lines), :].astype(jnp.bfloat16)
    for n in range(piece_ref.shape[0]):
        piece_ref[n] = piece
    value_ref[...] = jnp.broadcast_to(rstd * terms, value_ref.shape)


def norm_pieces(arrived, gain, weight, half, copies, lines):
    return pl.pallas_call(
        norm_kernel,
        out_shape=(
            pltpu.VMEM((copies, lines, 128), jnp.bfloat16),
            pltpu.VMEM((1, 128), jnp.float32),
        ),
        in_specs=[smem_spec(), vmem_spec(), vmem_spec(), vmem_spec()],
        out_specs=(vmem_spec(), vmem_spec()),
        scratch_shapes=[pltpu.VMEM(gain.shape, jnp.float32)],
        cost_estimate=pl.CostEstimate(flops=4000000, bytes_accessed=400000, transcendentals=0),
        compiler_params=room(4),
        name="norm",
    )(half, arrived, gain, weight)


def logits_kernel(groups, near_ref, far_ref, ids_ref, *refs):
    count = 4
    matrices, out_ref, local, rows, flat, sems = refs[:count], *refs[count:]
    tiles, lanes = near_ref.shape[1:]
    pieces = flat.shape[0] // (groups * tiles)
    deep = tiles * lanes
    halves = local.shape[0] // deep
    pair, core, side = (lax.axis_index(a) for a in ("x_pair", "heads_1", "x_side"))
    flat_place = 0
    for axis in HEADS_BATCH:
        flat_place = flat_place * lax.axis_size(axis) + lax.axis_index(axis)
    across = (1 - 2 * core) * lax.axis_size(BATCH)
    along = (1 - 2 * side) * lax.axis_size("x_pair")
    firsts = [(flat_place + step) * lanes for step in (0, across, along, across + along)]
    moved = [
        pltpu.make_async_copy(near_ref, rows.at[pair], sems.at[halves]),
        pltpu.make_async_copy(far_ref, rows.at[1 - pair], sems.at[halves + 1]),
    ]
    for copy in moved:
        copy.start()
    copies = []
    for k in range(halves):
        part = pl.ds(k * deep, deep)
        copies.append(
            pltpu.make_async_copy(matrices[-1].at[part], local.at[part], sems.at[k])
        )
    for copy in copies:
        copy.start()
    for copy in moved:
        copy.wait()
    flat[...] = rows[...].reshape(flat.shape).astype(jnp.float32)

    def rows_of(piece):
        first, step = piece * tiles, pieces * tiles
        return jnp.concatenate(
            [flat[pl.ds(first + t, groups, stride=step), :] for t in range(tiles)], axis=1
        ).astype(jnp.bfloat16)

    sides = [
        jnp.concatenate([rows_of(p) for p in range(k, pieces, halves)], axis=0)
        for k in range(halves)
    ]
    sums = []
    for n in range(count):
        term = None
        for k in range(halves):
            part = slice(k * deep, (k + 1) * deep)
            if n == count - 1:
                copies[k].wait()
            matrix = matrices[n] if n < count - 1 else local
            found = jnp.dot(sides[k], matrix[part, :], preferred_element_type=jnp.float32)
            term = found if k == 0 else term + found
        sums.append(term)
    top = sums[0]
    for n in range(1, count):
        top = jnp.maximum(top, sums[n])
    top = jnp.max(top, axis=1, keepdims=True)
    ids = ids_ref[...]
    total = jnp.zeros(sums[0].shape, jnp.float32)
    chosen = jnp.zeros(sums[0].shape, jnp.float32)
    for n in range(count):
        total = total + jnp.exp(sums[n] - top)
        columns = lax.broadcasted_iota(jnp.int32, sums[n].shape, 1) + firsts[n]
        chosen = chosen + jnp.where(columns == ids, sums[n], 0.0)
    total = jnp.sum(total, axis=1, keepdims=True)
    chosen = jnp.sum(chosen, axis=1, keepdims=True)
    lane = lax.broadcasted_iota(jnp.int32, (groups, 128), 1)
    packed = jnp.zeros((groups, 128), jnp.float32)
    owned = pieces // halves
    for n, column in enumerate((top, total, chosen)):
        for r in range(owned):
            part = column[r * groups : (r + 1) * groups]
            packed = jnp.where(lane == n * owned + r, part, packed)
    for g in range(groups):
        out_ref[g] = packed[g : g + 1]


def logit_stats(near_rows, far_rows, matrices, ids, groups):
    depth = matrices[0].shape[0]
    return pl.pallas_call(
        functools.partial(logits_kernel, groups),
        out_shape=pltpu.VMEM((groups, 1, 128), jnp.float32),
        in_specs=[any_spec(), any_spec(), vmem_spec()]
        + [vmem_spec() for _ in matrices[:-1]]
        + [any_spec()],
        out_specs=vmem_spec(),
        scratch_shapes=[
            pltpu.VMEM((depth, 128), jnp.bfloat16),
            pltpu.VMEM((2, *near_rows.shape), near_rows.dtype),
            pltpu.VMEM((2 * near_rows.size // 128, 128), jnp.float32),
            pltpu.SemaphoreType.DMA((4,)),
        ],
        cost_estimate=pl.CostEstimate(flops=270000000, bytes_accessed=4700000, transcendentals=0),
        compiler_params=room(12),
        name="logits",
    )(near_rows, far_rows, ids, *matrices)


def shifted(lines, places):
    return pltpu.roll(lines, places % 128, 1)


def merged(lines, keep, owned):
    low = jnp.min(lines, axis=0, keepdims=True)
    top = jnp.max(jnp.where(keep, lines, low), axis=0, keepdims=True)
    weight = jnp.where(keep, jnp.exp(jnp.minimum(lines - top, 0.0)), 0.0)
    total = jnp.sum(shifted(lines, -owned) * weight, axis=0, keepdims=True)
    chosen = jnp.sum(jnp.where(keep, lines, 0.0), axis=0, keepdims=True)
    return top, total, chosen


def group_kernel(owned, stats_ref, value_ref, out_ref):
    lines = stats_ref[...].reshape(stats_ref.shape[0], 128)
    top, total, chosen = merged(lines, jnp.full(lines.shape, True), owned)
    lane = lax.broadcasted_iota(jnp.int32, (1, 128), 1)
    packed = jnp.where(lane < owned, top, shifted(total, owned))
    packed = jnp.where(lane < 2 * owned, packed, chosen)
    packed = jnp.where(lane < 3 * owned, packed, value_ref[...])
    for n in range(out_ref.shape[0]):
        out_ref[n] = packed


def group_stats(stats, value, owned, copies):
    return pl.pallas_call(
        functools.partial(group_kernel, owned),
        out_shape=pltpu.VMEM((copies, 1, 128), jnp.float32),
        in_specs=[vmem_spec(), vmem_spec()],
        out_specs=vmem_spec(),
        compiler_params=room(2),
        name="group",
    )(stats, value)


def final_kernel(owned, cores, stats_ref, logprob_ref, value_ref):
    count = stats_ref.shape[0]
    lines = stats_ref[...].reshape(count, 128)
    place = lax.broadcasted_iota(jnp.int32, lines.shape, 0)
    lane = lax.broadcasted_iota(jnp.int32, lines.shape, 1)
    row = lax.broadcasted_iota(jnp.int32, (1, 128), 1)
    logprob = jnp.zeros((1, 128), jnp.float32)
    for core in range(cores):
        top, total, chosen = merged(lines, place % cores == core, owned)
        total = jnp.where(row < owned, total, 1.0)
        found = shifted(chosen, -2 * owned) - (top + jnp.log(total))
        logprob = jnp.where(row // owned == core, shifted(found, core * owned), logprob)
    values = jnp.broadcast_to(lines[:, 3 * owned : 3 * owned + 1], lines.shape)
    here = place == (lane % owned) * (count // owned) + lane // owned
    value = jnp.sum(jnp.where(here, values, 0.0), axis=0, keepdims=True)
    logprob_ref[...] = logprob[:, : logprob_ref.shape[1]]
    value_ref[...] = value[:, : value_ref.shape[1]]


def final_values(stats, owned, cores):
    rows = owned * cores
    return pl.pallas_call(
        functools.partial(final_kernel, owned, cores),
        out_shape=(
            jax.ShapeDtypeStruct((1, rows), jnp.float32),
            jax.ShapeDtypeStruct((1, rows), jnp.float32),
        ),
        in_specs=[vmem_spec()],
        out_specs=(vmem_spec(), vmem_spec()),
        compiler_params=room(2),
        name="final",
    )(stats)


def per_device(
    queries,
    keys_new,
    values_new,
    out_gate,
    decay_logit,
    beta_logit,
    decay_rate,
    state,
    norm_gain,
    out_proj,
    residual,
    final_gain,
    value_weight,
    lm_head,
    sampled,
):
    chips, cores = lax.axis_size("heads_0"), lax.axis_size("heads_1")
    groups = lax.axis_size(GROUP)
    chip, core = lax.axis_index("heads_0"), lax.axis_index("heads_1")
    side = lax.axis_index("x_side")
    rows_own, width = residual.shape
    rows_core = rows_own // cores
    copies = chips // rows_core
    lanes = 128
    lines = width // lanes

    x_head = lax.ppermute(lm_head, "x_side", SWAP)
    core_head = lax.ppermute(lm_head, "heads_1", SWAP)
    both_head = lax.ppermute(x_head, "heads_1", SWAP)
    partial_out = head_partials(
        queries,
        keys_new,
        values_new,
        out_gate,
        decay_logit,
        beta_logit,
        decay_rate,
        state,
        norm_gain,
        out_proj,
        residual,
        chips * cores,
    )
    arrived = exchange(partial_out, HEADS)
    gain = final_gain.reshape(lines, lanes)
    weight = value_weight.reshape(lines, lanes)
    half_here = (chip % copies).astype(jnp.int32).reshape(1)
    near = lax.axis_size(NEAR)
    pieces, value = norm_pieces(arrived, gain, weight, half_here, near, lines // copies)
    near_rows = exchange(pieces, NEAR)
    far_rows = lax.ppermute(near_rows, "x_pair", SWAP)

    matrices = (lm_head, core_head, x_head, both_head)
    ids = sampled.reshape(lax.axis_size("z"), lax.axis_size("x_side"), -1, cores, rows_core)
    ids = lax.dynamic_index_in_dim(ids, side, 1, keepdims=False)
    ids = lax.dynamic_index_in_dim(ids, core, 2, keepdims=False)
    ids = ids.transpose(2, 1, 0).reshape(-1, 1)
    stats = logit_stats(near_rows, far_rows, matrices, ids, groups)
    stats = group_stats(exchange(stats, GROUP), value, rows_core, chips * cores)
    logprob, values = final_values(exchange(stats, HEADS), rows_core, cores)
    return (logprob.reshape(-1), values.reshape(-1))


def solution(mesh):
    torus = Mesh(
        mesh.devices.reshape(8, 2, 8, 2, 2), ("heads_0", "heads_1", "z", "x_side", "x_pair")
    )
    return jax.shard_map(
        per_device,
        mesh=torus,
        in_specs=(
            P(BATCH, HEADS),
            P(BATCH, HEADS),
            P(BATCH, HEADS),
            P(BATCH, HEADS),
            P(BATCH, HEADS),
            P(BATCH, HEADS),
            P(HEADS),
            P(BATCH, HEADS, None, None),
            P(),
            P(HEADS, None),
            P(BATCH, None),
            P(),
            P(),
            P(None, HEADS_BATCH),
            P(),
        ),
        out_specs=(P(BATCH), P(BATCH)),
        check_vma=False,
    )
```
